16 devices in a mesh: tp: 2 (over z), dp: 8 (over y, x, core).
Axes of the slice: x: 2, y: 2, z: 2, core: 2. Of those that a mesh axis runs over, the one named last changes fastest.
Arguments:
- w_in: float32 [1, 1280, 8960], P(None, None, 'tp')
- w_out: float32 [1, 6400, 1280], P(None, 'tp')
- g_in: float32 [8, 1, 1280, 8960], P('dp', None, None, 'tp')
- g_out: float32 [8, 1, 6400, 1280], P('dp', None, 'tp')
- m_in: bfloat16 [1, 1280, 8960], P(None, 'dp', 'tp')
- m_out: bfloat16 [1, 6400, 1280], P(None, 'tp', 'dp')
- r_in: float32 [1, 1280], P(None, 'dp')
- c_in: float32 [1, 8960], P(None, 'tp')
- r_out: float32 [1, 6400], P(None, 'tp')
- c_out: float32 [1, 1280], P(None, 'dp')
- learn_rate: float32 [], replicated
- weight_decay: float32 [], replicated
- beta_two: float32 [], replicated
Outputs:
- output 1: float32 [1, 1280, 8960], P(None, None, 'tp')
- output 2: float32 [1, 6400, 1280], P(None, 'tp')
- output 3: bfloat16 [1, 1280, 8960], P(None, 'dp', 'tp')
- output 4: bfloat16 [1, 6400, 1280], P(None, 'tp', 'dp')
- output 5: float32 [1, 1280], P(None, 'dp')
- output 6: float32 [1, 8960], P(None, 'tp')
- output 7: float32 [1, 6400], P(None, 'tp')
- output 8: float32 [1, 1280], P(None, 'dp')
All inputs are finite; a program needn't handle non-finite values.
Results may differ from the reference program's by a relative error of at most 0.00121538.
Values sent between devices are 32-bit elements.
A program may use at most 1 GiB of HBM per device.

```python
import math
import jax
import jax.numpy as jnp

LAYERS = 1
D = 1280
MLP = 5120
DP = 8

FIN = MLP + 3 * D
FOUT = MLP + D


def axis_scales(key, count):
    key_ramp, key_noise = jax.random.split(key)
    ramp_slope = jax.random.uniform(key_ramp, (LAYERS, 1), jnp.float32, 0.6, 1.0)
    ramp_vals = jnp.linspace(-1.0, 1.0, count, dtype=jnp.float32)[None, :]
    noise_vals = jax.random.normal(key_noise, (LAYERS, count), jnp.float32)
    return jnp.exp(ramp_slope * ramp_vals + 0.3 * noise_vals)


def draw_matrix(key, n_rows, n_cols):
    key_list = jax.random.split(key, 7)
    row_scale = axis_scales(key_list[0], n_rows)
    col_scale = axis_scales(key_list[1], n_cols)
    noise_rep = jax.random.normal(key_list[2], (DP, LAYERS, n_rows, n_cols), jnp.float32)
    grad_rep = noise_rep * (row_scale[:, :, None] * col_scale[:, None, :] / math.sqrt(DP))
    grad_sum = jnp.sum(grad_rep, axis=0)
    grad_sq = grad_sum * grad_sum
    row_noise = jax.random.normal(key_list[3], (LAYERS, n_rows), jnp.float32)
    col_noise = jax.random.normal(key_list[4], (LAYERS, n_cols), jnp.float32)
    row_old = 0.25 * jnp.mean(grad_sq, axis=2) * jnp.exp(0.5 * row_noise)
    col_old = 0.25 * jnp.mean(grad_sq, axis=1) * jnp.exp(0.5 * col_noise)
    weight = jax.random.normal(key_list[5], (LAYERS, n_rows, n_cols), jnp.float32) * n_rows ** -0.5
    moment = (0.1 * jax.random.normal(key_list[6], (LAYERS, n_rows, n_cols), jnp.float32)).astype(jnp.bfloat16)
    return weight, grad_rep, moment, row_old, col_old


def setup_inputs(seed: int = 0) -> dict:
    key_list = jax.random.split(jax.random.key(seed), 5)
    w_in, g_in, m_in, r_in, c_in = draw_matrix(key_list[0], D, FIN)
    w_out, g_out, m_out, r_out, c_out = draw_matrix(key_list[1], FOUT, D)
    learn_rate = jax.random.uniform(key_list[2], (), jnp.float32, 0.25, 0.75) * D ** -0.5
    weight_decay = jax.random.uniform(key_list[3], (), jnp.float32, 0.15, 0.45) * D ** 0.5
    beta_two = jax.random.uniform(key_list[4], (), jnp.float32, 0.8, 0.9)
    return dict(w_in=w_in, w_out=w_out, g_in=g_in, g_out=g_out, m_in=m_in, m_out=m_out, r_in=r_in, c_in=c_in, r_out=r_out, c_out=c_out, learn_rate=learn_rate, weight_decay=weight_decay, beta_two=beta_two)


def adafactor_matrix(weight, grad_rep, moment, row_old, col_old, learn_rate, weight_decay, beta_two):
    grad_sum = jnp.sum(grad_rep, axis=0)
    grad_sq = grad_sum * grad_sum + 1e-30
    row_new = beta_two * row_old + (1.0 - beta_two) * jnp.mean(grad_sq, axis=2)
    col_new = beta_two * col_old + (1.0 - beta_two) * jnp.mean(grad_sq, axis=1)
    row_avg = jnp.mean(row_new, axis=1)
    second = row_new[:, :, None] * col_new[:, None, :] / row_avg[:, None, None]
    update = grad_sum / jnp.sqrt(second)
    rms_val = jnp.sqrt(jnp.mean(update * update, axis=(1, 2)))
    update = update / jnp.maximum(1.0, rms_val)[:, None, None]
    mom_new = (0.9 * moment.astype(jnp.float32) + 0.1 * update).astype(jnp.bfloat16)
    w_new = weight - learn_rate * mom_new.astype(jnp.float32) - learn_rate * weight_decay * weight
    return w_new, mom_new, row_new, col_new


def reference(w_in, w_out, g_in, g_out, m_in, m_out, r_in, c_in, r_out, c_out, learn_rate, weight_decay, beta_two):
    in_result = adafactor_matrix(w_in, g_in, m_in, r_in, c_in, learn_rate, weight_decay, beta_two)
    out_result = adafactor_matrix(w_out, g_out, m_out, r_out, c_out, learn_rate, weight_decay, beta_two)
    return (in_result[0], out_result[0], in_result[1], out_result[1], in_result[2], in_result[3], out_result[2], out_result[3])
```

```python
import functools

import jax
import jax.numpy as jnp
from jax import lax
from jax.experimental import pallas as pl
from jax.experimental.pallas import tpu as pltpu
from jax.sharding import PartitionSpec as P

F32 = jnp.float32
BF16 = jnp.bfloat16
MESH = pl.DeviceIdType.MESH
LANE, SUB, SUB2, PART, QUAD, WIDTH = 128, 8, 16, 32, 4, 160
NO = None

D = 1280
ROWS_IN, COLS_IN = WIDTH, 4480
ROWS_OUT, COLS_OUT = 800, 640
RAW_OUT = 3200
STEPS = 10
M_IN = ROWS_IN // STEPS // 2
M_OUT = ROWS_OUT // STEPS // 2
RAW_STEP = RAW_OUT // STEPS
TILES_OUT = RAW_OUT // LANE

GRANT = 24 << 20

N_RED = 11
N_GAT = 18
(OWN, DSS, DSR, A1S, A1R, B1S, B1R, A2S, A2R, B2S, B2R) = range(N_RED)
(OXS, OXR, OYS, OYR, OPS, OPR, FXS, FXR, FYS, FYR, PXS, PXR, PYS, PYR, PDS, PDR, _U0, _U1) = range(N_GAT)


def lanes(shape):
    return lax.broadcasted_iota(jnp.int32, shape, 1)


def aligned(value, by):
    return pl.multiple_of(value, by)


def pad_lanes(row):
    return jnp.concatenate([row, jnp.zeros((1, LANE - row.shape[1]), F32)], axis=1)


def row_to_col(row):
    return jnp.broadcast_to(row, (LANE, LANE)).T


def main_kernel(n_tp, n_dp, rows_all_in, cols_all_in, rows_all_out, cols_all_out,
                w_in, w_out, g_in, g_out, m_in, m_out, r_in, c_in, r_out, c_out, lr_ref, wd_ref, b2_ref,
                win, wpk, m_in_new, m_out_new, r_in_new, c_in_new, r_out_new, c_out_new,
                own_in, raw, packed, gs_in, gs_out, w_cols, ai_out, ai_in, bj_in, vec_x, vec_y,
                col_acc, row_acc, row_peer, col_acc_out, col_peer_out, sv_in, sv_out,
                tot1_in, tot2_in, tot1_out, tot2_out,
                red_sem, gat_sem, load_sem, sv_send, sv_recv, zv_sem, tot_send, tot_recv):
    tp = lax.axis_index('tp')
    q = lax.axis_index('dp')
    me = tp * n_dp + q
    p, c = q // 2, q % 2
    y, x = p // 2, p % 2
    p_x, p_y, p_d = 2 * y + (1 - x), 2 * (1 - y) + x, 2 * (1 - y) + (1 - x)
    to_x = {'dp': 2 * p_x + c}
    to_y = {'dp': 2 * p_y + c}
    to_core = {'dp': 2 * p + (1 - c)}
    to_z = {'tp': 1 - tp}
    n_all = n_tp * n_dp
    j = q % QUAD
    lr, wd, b2 = lr_ref[0], wd_ref[0], b2_ref[0]

    barrier = pltpu.get_barrier_semaphore()

    def greet(d, _):
        other = lax.rem(me + d, n_all)
        pl.semaphore_signal(barrier, inc=1, device_id={'tp': other // n_dp, 'dp': lax.rem(other, n_dp)}, device_id_type=MESH)
        return 0

    lax.fori_loop(1, n_all, greet, 0)
    pl.semaphore_wait(barrier, n_all - 1)

    def rcopy(src, dst, send, recv, dev):
        return pltpu.make_async_remote_copy(src_ref=src, dst_ref=dst, send_sem=send, recv_sem=recv, device_id=dev, device_id_type=MESH)

    def spans(m, t):
        base = aligned(2 * m * t, SUB)
        return pl.ds(base, 2 * m), pl.ds(base, m), pl.ds(aligned(base + m, SUB), m)

    def first_copies(ph, w, m, t):
        _, ra, rb = spans(m, t)
        a = rcopy(w.at[pl.ds(0, 2), 1 - x, ra], w.at[2, pl.ds(0, 2), ra], red_sem.at[ph, A1S, t], red_sem.at[ph, A1R, t], to_x)
        b = rcopy(w.at[1 - y, pl.ds(0, 2), rb], w.at[2, pl.ds(0, 2), rb], red_sem.at[ph, B1S, t], red_sem.at[ph, B1R, t], to_y)
        return a, b

    def second_copies(ph, w, m, t):
        _, ra, rb = spans(m, t)
        a = rcopy(w.at[1 - y, x, ra], w.at[3, 0, ra], red_sem.at[ph, A2S, t], red_sem.at[ph, A2R, t], to_y)
        b = rcopy(w.at[y, 1 - x, rb], w.at[3, 0, rb], red_sem.at[ph, B2S, t], red_sem.at[ph, B2R, t], to_x)
        return a, b

    def pair_in(t):
        rr, _, _ = spans(M_IN, t)
        return rcopy(g_in.at[:, :, 1 - c, rr], win.at[pl.ds(0, 2), :, rr], red_sem.at[0, DSS, t], red_sem.at[0, DSR, t], to_core)

    def own_load(t):
        rr, _, _ = spans(M_IN, t)
        return pltpu.make_async_copy(g_in.at[:, :, c, rr], own_in.at[lax.rem(t, 3)], red_sem.at[0, OWN, t])

    def raw_load(t):
        return pltpu.make_async_copy(g_out.at[pl.ds(aligned(RAW_STEP * t, SUB), RAW_STEP)], raw.at[lax.rem(t, 2)], red_sem.at[1, OWN, t])

    def pair_out(t):
        rr, _, _ = spans(M_OUT, t)
        return rcopy(packed.at[lax.rem(t, 2), :, :, 1 - c], wpk.at[pl.ds(0, 2), :, rr], red_sem.at[1, DSS, t], red_sem.at[1, DSR, t], to_core)

    def start_in(t):
        pair_in(t).start()
        own_load(t).start()

    def pack_out(t):
        raw_load(t).wait()
        slot = lax.rem(t, 2)

        @pl.when(t >= 2)
        def _():
            pair_out(t - 2).wait_send()

        def unit(u, _):
            base = aligned(PART * u, SUB)
            tiles = [[raw[slot, pl.ds(base + SUB * k, SUB), LANE * i:LANE * i + LANE] for i in range(10)] for k in range(QUAD)]
            ln = lanes((SUB, LANE))
            for s in range(SUB):
                jj, first = s % QUAD, 5 * (s // QUAD) + s % QUAD
                tail = NO
                for k in range(QUAD):
                    lo, hi = tiles[k][first], tiles[k][first + 1]
                    head = lo if jj == 0 else pltpu.roll(jnp.where(ln >= PART * jj, lo, hi), LANE - PART * jj, 1)
                    packed[slot, s // QUAD, (s // 2) % 2, s % 2, pl.ds(aligned(SUB * u, SUB), SUB), LANE * k:LANE * k + LANE] = head
                    turn = (PART * (k - jj)) % LANE
                    part = hi if turn == 0 else pltpu.roll(hi, turn, 1)
                    tail = part if tail is NO else jnp.where(ln >= PART * k, part, tail)
                packed[slot, s // QUAD, (s // 2) % 2, s % 2, pl.ds(aligned(SUB * u, SUB), SUB), 512:640] = tail
            return 0

        lax.fori_loop(0, RAW_STEP // PART, unit, 0)
        pair_out(t).start()

        @pl.when(t + 2 < STEPS)
        def _():
            raw_load(t + 2).start()

    def reduce_first(ph, w, m, t):
        rr, _, _ = spans(m, t)
        if ph == 0:
            own_load(t).wait()
            pair_in(t).wait_recv()
            slot = lax.rem(t, 3)
            for yy in range(2):
                for xx in range(2):
                    for r in range(0, 2 * m, SUB):
                        rows = pl.ds(aligned(2 * m * t + r, SUB), SUB)
                        w[yy, xx, rows] = w[yy, xx, rows] + own_in[slot, yy, xx, r:r + SUB]
        else:
            pair_out(t).wait_recv()
            slot = lax.rem(t, 2)

            def add(i, _):
                rows = pl.ds(aligned(2 * m * t + SUB2 * i, SUB), SUB2)
                for yy in range(2):
                    for xx in range(2):
                        w[yy, xx, rows] = w[yy, xx, rows] + packed[slot, yy, xx, c, pl.ds(aligned(SUB2 * i, SUB), SUB2)]
                return 0

            lax.fori_loop(0, 2 * m // SUB2, add, 0)
        for copy in first_copies(ph, w, m, t):
            copy.start()

    def reduce_second(ph, w, m, t):
        _, ra, rb = spans(m, t)
        a, b = first_copies(ph, w, m, t)
        a2, b2_ = second_copies(ph, w, m, t)
        a.wait_recv()
        w[1 - y, x, ra] = w[1 - y, x, ra] + w[2, 1 - y, ra]
        a2.start()
        b.wait_recv()
        w[y, 1 - x, rb] = w[y, 1 - x, rb] + w[2, 1 - x, rb]
        b2_.start()

    def reduce_third(ph, w, m, t, gs):
        _, ra, rb = spans(m, t)
        first, second = first_copies(ph, w, m, t), second_copies(ph, w, m, t)
        second[0].wait_recv()
        ga = w[y, x, ra] + w[2, y, ra] + w[3, 0, ra]
        gs[ra] = ga
        second[1].wait_recv()
        gb = w[y, x, rb] + w[2, x, rb] + w[3, 0, rb]
        gs[rb] = gb
        for copy in (*first, *second):
            copy.wait_send()
        if ph == 0:
            pair_in(t).wait_send()
            sa, sb = ga * ga + 1e-30, gb * gb + 1e-30
            col_acc[...] = col_acc[...] + (sa + sb)
            for rows, sq in ((ra, sa), (rb, sb)):
                part = sq[:, 0:LANE]
                for i in range(1, COLS_IN // LANE):
                    part = part + sq[:, LANE * i:LANE * i + LANE]
                row_acc[rows] = part

    def gather_own(ph, w, m, t):
        rr, _, _ = spans(m, t)
        src = w.at[p, c, rr]
        return (rcopy(src, src, gat_sem.at[ph, OXS, t], gat_sem.at[ph, OXR, t], to_x),
                rcopy(src, src, gat_sem.at[ph, OYS, t], gat_sem.at[ph, OYR, t], to_y),
                rcopy(src, src, gat_sem.at[ph, OPS, t], gat_sem.at[ph, OPR, t], to_core))

    def gather_came(ph, w, m, t):
        rr, _, _ = spans(m, t)
        return (rcopy(w.at[p_x, c, rr], w.at[p_x, c, rr], gat_sem.at[ph, OXS, t], gat_sem.at[ph, OXR, t], to_x),
                rcopy(w.at[p_y, c, rr], w.at[p_y, c, rr], gat_sem.at[ph, OYS, t], gat_sem.at[ph, OYR, t], to_y))

    def gather_on(ph, w, m, t):
        _, ra, rb = spans(m, t)
        return (rcopy(w.at[p_y, c, ra], w.at[p_y, c, ra], gat_sem.at[ph, FXS, t], gat_sem.at[ph, FXR, t], to_x),
                rcopy(w.at[p_x, c, rb], w.at[p_x, c, rb], gat_sem.at[ph, FYS, t], gat_sem.at[ph, FYR, t], to_y))

    def gather_diag(ph, w, m, t):
        _, ra, rb = spans(m, t)
        return (rcopy(w.at[p_d, c, ra], w.at[p_d, c, ra], gat_sem.at[ph, FXS, t], gat_sem.at[ph, FXR, t], to_x),
                rcopy(w.at[p_d, c, rb], w.at[p_d, c, rb], gat_sem.at[ph, FYS, t], gat_sem.at[ph, FYR, t], to_y))

    def gather_pair(ph, w, m, t, cc):
        rr, _, _ = spans(m, t)
        return [rcopy(w.at[pp, cc, rr], w.at[pp, cc, rr], gat_sem.at[ph, s, t], gat_sem.at[ph, s + 1, t], to_core)
                for pp, s in ((p_x, PXS), (p_y, PYS), (p_d, PDS))]

    def gather_first(ph, w, m, t):
        for copy in gather_own(ph, w, m, t):
            copy.start()

    def gather_second(ph, w, m, t):
        came = gather_came(ph, w, m, t)
        on = gather_on(ph, w, m, t)
        pair = gather_pair(ph, w, m, t, c)
        came[0].wait_recv()
        on[1].start()
        pair[0].start()
        came[1].wait_recv()
        on[0].start()
        pair[1].start()

    def gather_third(ph, w, m, t):
        diag = gather_diag(ph, w, m, t)
        diag[0].wait_recv()
        diag[1].wait_recv()
        gather_pair(ph, w, m, t, c)[2].start()

    def gather_last(ph, w, m, t):
        rr, _, _ = spans(m, t)
        own_pair = rcopy(w.at[p, 1 - c, rr], w.at[p, 1 - c, rr], gat_sem.at[ph, OPS, t], gat_sem.at[ph, OPR, t], to_core)
        own_pair.wait_recv()
        for copy in gather_pair(ph, w, m, t, 1 - c):
            copy.wait_recv()
        for copy in (*gather_own(ph, w, m, t), *gather_on(ph, w, m, t), *gather_pair(ph, w, m, t, c)):
            copy.wait_send()

    def to_all(buf, which):
        def send(d, _):
            other = lax.rem(me + d, n_all)
            dev = {'tp': other // n_dp, 'dp': lax.rem(other, n_dp)}
            rcopy(buf.at[me], buf.at[me], tot_send.at[which, d], tot_recv.at[which, me], dev).start()
            return 0

        lax.fori_loop(1, n_all, send, 0)

    def from_all(buf, which):
        def take(d, _):
            other = lax.rem(me + d, n_all)
            rcopy(buf.at[other], buf.at[other], tot_send.at[which, d], tot_recv.at[which, other], to_z).wait()
            return 0

        lax.fori_loop(1, n_all, take, 0)

    def to_group(buf, which):
        def send(d, _):
            other = lax.rem(q + d, n_dp)
            rcopy(buf.at[q], buf.at[q], sv_send.at[which, d], sv_recv.at[which, q], {'dp': other}).start()
            return 0

        lax.fori_loop(1, n_dp, send, 0)

    def from_group(buf, which):
        def take(d, _):
            other = lax.rem(q + d, n_dp)
            rcopy(buf.at[other], buf.at[other], sv_send.at[which, d], sv_recv.at[which, other], to_z).wait()
            return 0

        lax.fori_loop(1, n_dp, take, 0)

    def add_all(buf, n):
        total = buf[0]
        for i in range(1, n):
            total = total + buf[i]
        return total

    def z_in():
        return rcopy(row_acc, row_peer, zv_sem.at[0], zv_sem.at[1], to_z)

    def z_out():
        return rcopy(col_acc_out, col_peer_out, zv_sem.at[2], zv_sem.at[3], to_z)

    def total(value):
        return jnp.sum(jnp.sum(value, axis=0, keepdims=True), axis=1, keepdims=True)

    def old_total(ref, width):
        acc = jnp.zeros((1, LANE), F32)
        for i in range(0, width, LANE):
            part = ref[:, i:min(i + LANE, width)]
            acc = acc + (part if part.shape[1] == LANE else pad_lanes(part))
        return jnp.broadcast_to(total(acc), (SUB, LANE))

    def stats_in_send():
        part = col_acc[:, 0:LANE]
        for i in range(1, COLS_IN // LANE):
            part = part + col_acc[:, LANE * i:LANE * i + LANE]
        sv_in[q] = jnp.sum(col_acc[...], axis=0, keepdims=True)
        tot1_in[me, 0:SUB] = part
        tot1_in[me, SUB:SUB2] = old_total(r_in, ROWS_IN)
        z_in().start()
        to_group(sv_in, 0)
        to_all(tot1_in, 0)
        w_load_in().start()

    def w_load_in():
        return pltpu.make_async_copy(w_in.at[p, c], win.at[p, c], load_sem.at[0])

    def stats_in_norm():
        z_in().wait()
        from_group(sv_in, 0)
        from_all(tot1_in, 0)
        col_mean = add_all(sv_in, n_dp) / rows_all_in
        c_new = b2 * c_in[...] + (1.0 - b2) * col_mean
        c_in_new[...] = c_new
        bj_in[...] = 1.0 / jnp.sqrt(c_new)
        all_tot = add_all(tot1_in, n_all)
        r_total = all_tot[SUB:9, 0:1] / n_tp
        r_avg = (b2 * r_total + (1.0 - b2) * (total(all_tot[0:SUB]) / cols_all_in)) / rows_all_in
        root_avg = jnp.sqrt(r_avg)
        row_mean = jnp.sum(row_acc[...] + row_peer[...], axis=1, keepdims=True) / cols_all_in
        row_mean = jnp.broadcast_to(row_mean, (ROWS_IN, LANE))
        r_old = jnp.concatenate([row_to_col(r_in[:, 0:LANE]), row_to_col(pad_lanes(r_in[:, LANE:WIDTH]))[0:PART]], axis=0)
        r_new = b2 * r_old + (1.0 - b2) * row_mean
        r_in_new[:, 0:LANE] = r_new[0:LANE].T[0:1]
        r_in_new[:, LANE:WIDTH] = jnp.concatenate([r_new[LANE:WIDTH], jnp.zeros((96, LANE), F32)], axis=0).T[0:1, 0:PART]
        ai_in[...] = root_avg / jnp.sqrt(r_new)

        def body(i, acc):
            rows = pl.ds(aligned(SUB * i, SUB), SUB)
            a = ai_in[rows]
            for k in range(COLS_IN // LANE):
                col = slice(LANE * k, LANE * k + LANE)
                u = gs_in[rows, col] * a * bj_in[:, col]
                acc = acc + u * u
            return acc

        tot2_in[me] = lax.fori_loop(0, ROWS_IN // SUB, body, jnp.zeros((SUB, LANE), F32))
        to_all(tot2_in, 1)

    def scale_of(buf, count):
        mean = total(add_all(buf, n_all)) / count
        return 0.1 / jnp.maximum(1.0, jnp.sqrt(mean))

    def update_in():
        from_all(tot2_in, 1)
        scale = scale_of(tot2_in, float(rows_all_in * cols_all_in))
        w_load_in().wait()
        m_load_in().wait()

        def body(i, _):
            rows = pl.ds(aligned(SUB2 * i, SUB2), SUB2)
            a = ai_in[rows] * scale
            for k in range(COLS_IN // LANE):
                col = slice(LANE * k, LANE * k + LANE)
                u = gs_in[rows, col] * a * bj_in[:, col]
                mom = (0.9 * m_in_new[rows, col].astype(F32) + u).astype(BF16)
                m_in_new[rows, col] = mom
                old = win[p, c, rows, col]
                win[p, c, rows, col] = old - lr * mom.astype(F32) - lr * wd * old
            return 0

        lax.fori_loop(0, ROWS_IN // SUB2, body, 0)

    def m_load_in():
        return pltpu.make_async_copy(m_in, m_in_new, load_sem.at[1])

    def block_out(t):
        heads, tails = [], []
        for u in range(QUAD):
            rows = pl.ds(aligned(PART * t + SUB * u, SUB), SUB)
            tail = gs_out[rows, 512:640]
            for k in range(QUAD):
                heads.append(gs_out[rows, LANE * k:LANE * k + LANE])
                tails.append(tail if k == 0 else pltpu.roll(tail, LANE - PART * k, 1))
        tails = jnp.concatenate(tails, axis=0)
        return jnp.concatenate(heads, axis=0), jnp.where(lanes((LANE, LANE)) < PART, tails, 0.0)

    def stats_out_send():
        def body(t, acc):
            head, tail = block_out(t)
            sh = head * head + 1e-30
            st = jnp.where(lanes((LANE, LANE)) < PART, tail * tail + 1e-30, 0.0)
            sv_out[q, :, pl.ds(aligned(LANE * t, LANE), LANE)] = jnp.sum((sh + st).T, axis=0, keepdims=True)
            ah, at = acc
            for i in range(SUB2):
                ah = ah + sh[SUB * i:SUB * i + SUB]
                at = at + st[SUB * i:SUB * i + SUB]
            return ah, at

        zero = jnp.zeros((SUB, LANE), F32)
        ah, at = lax.fori_loop(0, TILES_OUT, body, (zero, zero))
        col_acc_out[0:SUB] = ah
        col_acc_out[SUB:SUB2] = at
        tot1_out[me, 0:SUB] = ah + at
        tot1_out[me, SUB:SUB2] = old_total(r_out, RAW_OUT)
        z_out().start()
        to_group(sv_out, 1)
        to_all(tot1_out, 2)

    def stats_out_norm():
        z_out().wait()
        from_group(sv_out, 1)
        from_all(tot1_out, 2)
        row_mean = add_all(sv_out, n_dp) / cols_all_out
        r_new = b2 * r_out[...] + (1.0 - b2) * row_mean
        r_out_new[...] = r_new
        all_tot = add_all(tot1_out, n_all)
        r_total = all_tot[SUB:9, 0:1] / n_dp
        r_avg = (b2 * r_total + (1.0 - b2) * (total(all_tot[0:SUB]) / cols_all_out)) / rows_all_out
        root_avg = jnp.sqrt(r_avg)
        cols = col_acc_out[...] + col_peer_out[...]
        c_new_h = b2 * c_out[:, 0:LANE] + (1.0 - b2) * (jnp.sum(cols[0:SUB], axis=0, keepdims=True) / rows_all_out)
        c_new_t = b2 * pad_lanes(c_out[:, LANE:WIDTH]) + (1.0 - b2) * (jnp.sum(cols[SUB:SUB2], axis=0, keepdims=True) / rows_all_out)
        c_out_new[:, 0:LANE] = c_new_h
        c_out_new[:, LANE:WIDTH] = c_new_t[:, 0:PART]
        vec_x[...] = jnp.broadcast_to(1.0 / jnp.sqrt(c_new_h), (SUB, LANE))
        vec_y[...] = jnp.broadcast_to(1.0 / jnp.sqrt(jnp.where(lanes((1, LANE)) < PART, c_new_t, 1.0)), (SUB, LANE))
        bh, bt = vec_x[0:1], vec_y[0:1]

        def body(t, acc):
            rows = pl.ds(aligned(LANE * t, LANE), LANE)
            a = row_to_col(root_avg / jnp.sqrt(r_out_new[:, rows]))
            ai_out[rows] = a
            head, tail = block_out(t)
            uh, ut = head * a * bh, tail * a * bt
            sq = uh * uh + ut * ut
            for i in range(SUB2):
                acc = acc + sq[SUB * i:SUB * i + SUB]
            return acc

        tot2_out[me] = lax.fori_loop(0, TILES_OUT, body, jnp.zeros((SUB, LANE), F32))
        to_all(tot2_out, 3)

    def w_load_out():
        first = 5 * (q // QUAD) + j
        return pltpu.make_async_copy(w_out.at[:, pl.ds(aligned(LANE * first, LANE), 256)], w_cols, load_sem.at[2])

    def m_load_out():
        return pltpu.make_async_copy(m_out, m_out_new, load_sem.at[3])

    def update_out():
        from_all(tot2_out, 3)
        scale = scale_of(tot2_out, float(rows_all_out * cols_all_out))
        w_load_out().wait()
        m_load_out().wait()
        bh, bt = vec_x[0:1], vec_y[0:1]
        back = PART * ((QUAD - j) % QUAD)

        def body(t, _):
            rows = pl.ds(aligned(LANE * t, LANE), LANE)
            a = ai_out[rows] * scale
            head, tail = block_out(t)
            uh, ut = head * a * bh, tail * a * bt
            mom = m_out_new[:, rows].astype(F32)
            mh = (0.9 * mom[0:LANE].T + uh).astype(BF16).astype(F32)
            mt = (0.9 * jnp.concatenate([mom[LANE:WIDTH], jnp.zeros((96, LANE), F32)], axis=0).T + ut).astype(BF16).astype(F32)
            m_out_new[0:LANE, rows] = mh.T.astype(BF16)
            m_out_new[LANE:WIDTH, rows] = mt.T[0:PART].astype(BF16)
            lo, hi = w_cols[rows, 0:LANE], w_cols[rows, LANE:256]
            wh = pltpu.roll(jnp.where(lanes((LANE, LANE)) >= PART * j, lo, hi), back, 1)
            wt = pltpu.roll(hi, back, 1)
            wh = wh - lr * mh - lr * wd * wh
            wt = wt - lr * mt - lr * wd * wt
            ln = lanes((SUB, LANE))
            for u in range(QUAD):
                to = pl.ds(aligned(PART * t + SUB * u, SUB), SUB)
                joined = NO
                for k in range(QUAD):
                    at = PART * u + SUB * k
                    wpk[p, c, to, LANE * k:LANE * k + LANE] = wh[at:at + SUB]
                    part = wt[at:at + SUB] if k == 0 else pltpu.roll(wt[at:at + SUB], PART * k, 1)
                    joined = part if joined is NO else jnp.where(ln >= PART * k, part, joined)
                wpk[p, c, to, 512:640] = joined
            return 0

        lax.fori_loop(0, TILES_OUT, body, 0)

    col_acc[...] = jnp.zeros_like(col_acc)
    start_in(0)
    start_in(1)

    def at_step(cond, fn, *args):
        @pl.when(cond)
        def _():
            fn(*args)

    n = STEPS

    def step(s, _):
        def within(lo, hi):
            return jnp.logical_and(s >= lo, s < hi)

        at_step(s + 2 < n, start_in, s + 2)
        at_step(s < n, reduce_first, 0, win, M_IN, s)
        at_step(within(2, n + 2), reduce_second, 0, win, M_IN, s - 2)
        at_step(within(QUAD, n + QUAD), reduce_third, 0, win, M_IN, s - QUAD, gs_in)

        @pl.when(s == 2)
        def _():
            m_load_in().start()
            m_load_out().start()
            w_load_out().start()

        @pl.when(s == n - 3)
        def _():
            raw_load(0).start()
            raw_load(1).start()

        at_step(within(n, 2 * n), reduce_first, 1, wpk, M_OUT, s - n)
        at_step(within(n - 1, 2 * n - 1), pack_out, s - n + 1)
        at_step(within(n + 2, 2 * n + 2), reduce_second, 1, wpk, M_OUT, s - n - 2)
        at_step(within(n + QUAD, 2 * n + QUAD), reduce_third, 1, wpk, M_OUT, s - n - QUAD, gs_out)
        at_step(s == n + 3, stats_in_send)
        at_step(s == n + 6, stats_in_norm)
        at_step(s == n + 9, update_in)
        at_step(within(2 * n, 3 * n), gather_first, 0, win, M_IN, s - 2 * n)
        at_step(within(2 * n + 2, 3 * n + 2), gather_second, 0, win, M_IN, s - 2 * n - 2)
        at_step(within(2 * n + QUAD, 3 * n + QUAD), gather_third, 0, win, M_IN, s - 2 * n - QUAD)
        at_step(s == 2 * n + 3, stats_out_send)
        at_step(s == 2 * n + 6, stats_out_norm)
        at_step(s == 2 * n + 9, update_out)
        at_step(within(3 * n, QUAD * n), gather_first, 1, wpk, M_OUT, s - 3 * n)
        at_step(within(3 * n + 2, QUAD * n + 2), gather_second, 1, wpk, M_OUT, s - 3 * n - 2)
        at_step(within(3 * n + QUAD, QUAD * n + QUAD), gather_third, 1, wpk, M_OUT, s - 3 * n - QUAD)
        return 0

    lax.fori_loop(0, QUAD * n + QUAD, step, 0)

    def finish(t, _):
        gather_last(0, win, M_IN, t)
        gather_last(1, wpk, M_OUT, t)
        return 0

    lax.fori_loop(0, n, finish, 0)
    pair_out(n - 2).wait_send()
    pair_out(n - 1).wait_send()


def final_kernel(win, wpk, mi, mo, ri, ci, ro, co, win_o, wout_o, mi_o, mo_o, ri_o, ci_o, ro_o, co_o, stage, sem, stage_sem):
    plain = [pltpu.make_async_copy(win, win_o, sem.at[0])]
    for i, (src, dst) in enumerate(((mi, mi_o), (mo, mo_o), (ri, ri_o), (ci, ci_o), (ro, ro_o), (co, co_o))):
        plain.append(pltpu.make_async_copy(src, dst, sem.at[i + 1]))
    for copy in plain:
        copy.start()

    def rows_of(t):
        return pl.ds(aligned(RAW_STEP * t, SUB), RAW_STEP)

    def put(t):
        return pltpu.make_async_copy(stage.at[rows_of(t)], wout_o.at[rows_of(t)], stage_sem.at[t])

    def chunk(t, _):
        def unit(u, _):
            ln = lanes((SUB, LANE))
            rows = pl.ds(aligned(2 * M_OUT * t + SUB * u, SUB), SUB)
            for half in range(2):
                tails = [wpk[2 * half + jj // 2, jj % 2, rows, 512:640] for jj in range(QUAD)]
                for k in range(QUAD):
                    to = pl.ds(aligned(RAW_STEP * t + PART * u + SUB * k, SUB), SUB)
                    heads = []
                    for jj in range(QUAD):
                        head = wpk[2 * half + jj // 2, jj % 2, rows, LANE * k:LANE * k + LANE]
                        heads.append(head if jj == 0 else pltpu.roll(head, PART * jj, 1))
                    ends = [tails[jj] if jj == k else pltpu.roll(tails[jj], (PART * (jj - k)) % LANE, 1) for jj in range(QUAD)]
                    for tile in range(5):
                        if tile == 0:
                            out = heads[0]
                        else:
                            out = ends[tile - 1]
                            if tile > 1:
                                out = jnp.where(ln < PART * (tile - 1), heads[tile - 1], out)
                            if tile < QUAD:
                                out = jnp.where(ln >= PART * tile, heads[tile], out)
                        at = LANE * (5 * half + tile)
                        stage[to, at:at + LANE] = out
            return 0

        lax.fori_loop(0, RAW_STEP // PART, unit, 0)
        put(t).start()
        return 0

    lax.fori_loop(0, STEPS, chunk, 0)
    for t in range(STEPS):
        put(t).wait()
    for copy in plain:
        copy.wait()


def solution(mesh):
    n_tp = mesh.shape['tp']
    n_dp = mesh.shape['dp']
    vmem = pl.BlockSpec(memory_space=pltpu.VMEM)
    hbm = pl.BlockSpec(memory_space=pltpu.HBM)
    smem = pl.BlockSpec(memory_space=pltpu.SMEM)
    dma = pltpu.SemaphoreType.DMA
    kept = (
        ((QUAD, 2, ROWS_IN, COLS_IN), F32),
        ((QUAD, 2, ROWS_OUT, COLS_OUT), F32),
        ((ROWS_IN, COLS_IN), BF16),
        ((WIDTH, RAW_OUT), BF16),
        ((1, ROWS_IN), F32),
        ((1, COLS_IN), F32),
        ((1, RAW_OUT), F32),
        ((1, WIDTH), F32),
    )
    main = pl.pallas_call(
        functools.partial(main_kernel, n_tp, n_dp, D, COLS_IN * n_tp, RAW_OUT * n_tp, D),
        out_shape=[pltpu.VMEM(shape, dtype) for shape, dtype in kept],
        in_specs=[hbm] * 6 + [vmem] * QUAD + [smem] * 3,
        out_specs=[vmem] * SUB,
        scratch_shapes=[
            pltpu.VMEM((3, 2, 2, 2 * M_IN, COLS_IN), F32),
            pltpu.VMEM((2, RAW_STEP, D), F32),
            pltpu.VMEM((2, 2, 2, 2, 2 * M_OUT, COLS_OUT), F32),
            pltpu.VMEM((ROWS_IN, COLS_IN), F32),
            pltpu.VMEM((ROWS_OUT, COLS_OUT), F32),
            pltpu.VMEM((RAW_OUT, 256), F32),
            pltpu.VMEM((RAW_OUT, LANE), F32),
            pltpu.VMEM((ROWS_IN, LANE), F32),
            pltpu.VMEM((1, COLS_IN), F32),
            pltpu.VMEM((SUB, LANE), F32),
            pltpu.VMEM((SUB, LANE), F32),
            pltpu.VMEM((SUB, COLS_IN), F32),
            pltpu.VMEM((ROWS_IN, LANE), F32),
            pltpu.VMEM((ROWS_IN, LANE), F32),
            pltpu.VMEM((SUB2, LANE), F32),
            pltpu.VMEM((SUB2, LANE), F32),
            pltpu.VMEM((n_dp, 1, COLS_IN), F32),
            pltpu.VMEM((n_dp, 1, RAW_OUT), F32),
            pltpu.VMEM((n_tp * n_dp, SUB2, LANE), F32),
            pltpu.VMEM((n_tp * n_dp, SUB, LANE), F32),
            pltpu.VMEM((n_tp * n_dp, SUB2, LANE), F32),
            pltpu.VMEM((n_tp * n_dp, SUB, LANE), F32),
            dma((2, N_RED, STEPS)),
            dma((2, N_GAT, STEPS)),
            dma((QUAD,)),
            dma((2, n_dp)),
            dma((2, n_dp)),
            dma((QUAD,)),
            dma((QUAD, n_tp * n_dp)),
            dma((QUAD, n_tp * n_dp)),
        ],
        compiler_params=pltpu.CompilerParams(collective_id=0, has_side_effects=True, vmem_limit_bytes=GRANT),
    )
    final = pl.pallas_call(
        final_kernel,
        out_shape=[
            jax.ShapeDtypeStruct((QUAD, 2, ROWS_IN, COLS_IN), F32),
            jax.ShapeDtypeStruct((RAW_OUT, D), F32),
        ] + [jax.ShapeDtypeStruct(shape, dtype) for shape, dtype in kept[2:]],
        in_specs=[vmem] * SUB,
        out_specs=[hbm] * SUB,
        scratch_shapes=[pltpu.VMEM((RAW_OUT, D), F32), dma((7,)), dma((STEPS,))],
        compiler_params=pltpu.CompilerParams(vmem_limit_bytes=GRANT),
    )

    def body(w_in, w_out, g_in, g_out, m_in, m_out, r_in, c_in, r_out, c_out, learn_rate, weight_decay, beta_two):
        shards = (QUAD, 2, ROWS_IN, COLS_IN)
        got = main(
            w_in.reshape(shards), w_out[0], g_in.reshape((2, 2, 2, ROWS_IN, COLS_IN)), g_out[0, 0], m_in[0], m_out[0].T,
            r_in, c_in, r_out, c_out, learn_rate.reshape(1), weight_decay.reshape(1), beta_two.reshape(1))
        w_i, w_o, m_i, m_o, r_i, c_i, r_o, c_o = final(*[pltpu.with_memory_space_constraint(g, pltpu.VMEM) for g in got])
        return w_i.reshape((1, D, COLS_IN)), w_o[NO], m_i[NO], m_o.T[NO], r_i, c_i, r_o, c_o

    in_specs = (P(NO, NO, 'tp'), P(NO, 'tp', NO), P('dp', NO, NO, 'tp'), P('dp', NO, 'tp', NO), P(NO, 'dp', 'tp'), P(NO, 'tp', 'dp'), P(NO, 'dp'), P(NO, 'tp'), P(NO, 'tp'), P(NO, 'dp'), P(), P(), P())
    out_specs = (P(NO, NO, 'tp'), P(NO, 'tp', NO), P(NO, 'dp', 'tp'), P(NO, 'tp', 'dp'), P(NO, 'dp'), P(NO, 'tp'), P(NO, 'tp'), P(NO, 'dp'))
    return jax.shard_map(body, mesh=mesh, in_specs=in_specs, out_specs=out_specs, check_vma=False)
```

```python
import functools

import jax
import jax.numpy as jnp
from jax import lax
from jax.experimental import pallas as pl
from jax.experimental.pallas import tpu as pltpu
from jax.sharding import PartitionSpec as P

F32 = jnp.float32
BF16 = jnp.bfloat16
MESH = pl.DeviceIdType.MESH
LANE, SUB, SUB2, PART, QUAD, WIDTH = 128, 8, 16, 32, 4, 160
NO = None

D = 1280
ROWS_IN, COLS_IN = WIDTH, 4480
ROWS_OUT, COLS_OUT = 800, 640
RAW_OUT = 3200
STEPS = 10
M_IN = ROWS_IN // STEPS // 2
M_OUT = ROWS_OUT // STEPS // 2
RAW_STEP = RAW_OUT // STEPS
TILES_OUT = RAW_OUT // LANE

GRANT = 24 << 20

N_RED = 11
N_GAT = 16
SLOTS = 6
(OWN, DSS, DSR, A1S, A1R, B1S, B1R, A2S, A2R, B2S, B2R) = range(N_RED)
(OXS, OXR, OYS, OYR, OPS, OPR, FXS, FXR, FYS, FYR, PXS, PXR, PYS, PYR, PDS, PDR) = range(N_GAT)


def lanes(shape):
    return lax.broadcasted_iota(jnp.int32, shape, 1)


def aligned(value, by):
    return pl.multiple_of(value, by)


def pad_lanes(row):
    return jnp.concatenate([row, jnp.zeros((1, LANE - row.shape[1]), F32)], axis=1)


def row_to_col(row):
    return jnp.broadcast_to(row, (LANE, LANE)).T


def main_kernel(n_tp, n_dp, rows_all_in, cols_all_in, rows_all_out, cols_all_out,
                w_in, w_out, g_in, g_out, m_in, m_out, r_in, c_in, r_out, c_out, lr_ref, wd_ref, b2_ref,
                win, wpk, m_in_new, m_out_new, r_in_new, c_in_new, r_out_new, c_out_new,
                own_in, raw, packed, gs_in, gs_out, w_cols, ai_out, ai_in, bj_in, vec_x, vec_y,
                col_acc, row_acc, row_peer, col_acc_out, col_peer_out, v_in, vc_in, v_out, vc_out,
                zt_in, pt_in, ct_in, zt_out, pt_out, ct_out,
                red_sem, gat_sem, load_sem, ex_sem):
    tp = lax.axis_index('tp')
    q = lax.axis_index('dp')
    p, c = q // 2, q % 2
    y, x = p // 2, p % 2
    p_x, p_y, p_d = 2 * y + (1 - x), 2 * (1 - y) + x, 2 * (1 - y) + (1 - x)
    to_x = {'dp': 2 * p_x + c}
    to_y = {'dp': 2 * p_y + c}
    to_d = {'dp': 2 * p_d + c}
    to_core = {'dp': 2 * p + (1 - c)}
    to_z = {'tp': 1 - tp}
    j = q % QUAD
    lr, wd, b2 = lr_ref[0], wd_ref[0], b2_ref[0]

    barrier = pltpu.get_barrier_semaphore()
    for dev in (to_x, to_y, to_core, to_z):
        pl.semaphore_signal(barrier, inc=1, device_id=dev, device_id_type=MESH)

    def rcopy(src, dst, send, recv, dev):
        return pltpu.make_async_remote_copy(src_ref=src, dst_ref=dst, send_sem=send, recv_sem=recv, device_id=dev, device_id_type=MESH)

    def slot_of(ph, t):
        return lax.rem(ph * STEPS + t, SLOTS)

    def spans(m, t):
        base = aligned(2 * m * t, SUB)
        return pl.ds(base, 2 * m), pl.ds(base, m), pl.ds(aligned(base + m, SUB), m)

    def first_copies(ph, w, m, t):
        _, ra, rb = spans(m, t)
        a = rcopy(w.at[pl.ds(0, 2), 1 - x, ra], w.at[2, pl.ds(0, 2), ra], red_sem.at[A1S, slot_of(ph, t)], red_sem.at[A1R, slot_of(ph, t)], to_x)
        b = rcopy(w.at[1 - y, pl.ds(0, 2), rb], w.at[2, pl.ds(0, 2), rb], red_sem.at[B1S, slot_of(ph, t)], red_sem.at[B1R, slot_of(ph, t)], to_y)
        return a, b

    def second_copies(ph, w, m, t):
        _, ra, rb = spans(m, t)
        a = rcopy(w.at[1 - y, x, ra], w.at[3, 0, ra], red_sem.at[A2S, slot_of(ph, t)], red_sem.at[A2R, slot_of(ph, t)], to_y)
        b = rcopy(w.at[y, 1 - x, rb], w.at[3, 0, rb], red_sem.at[B2S, slot_of(ph, t)], red_sem.at[B2R, slot_of(ph, t)], to_x)
        return a, b

    def pair_in(t):
        rr, _, _ = spans(M_IN, t)
        return rcopy(g_in.at[:, :, 1 - c, rr], win.at[pl.ds(0, 2), :, rr], red_sem.at[DSS, slot_of(0, t)], red_sem.at[DSR, slot_of(0, t)], to_core)

    def own_load(t):
        rr, _, _ = spans(M_IN, t)
        return pltpu.make_async_copy(g_in.at[:, :, c, rr], own_in.at[lax.rem(t, 3)], red_sem.at[OWN, slot_of(0, t)])

    def raw_load(t):
        return pltpu.make_async_copy(g_out.at[pl.ds(aligned(RAW_STEP * t, SUB), RAW_STEP)], raw.at[lax.rem(t, 2)], red_sem.at[OWN, slot_of(1, t)])

    def pair_out(t):
        rr, _, _ = spans(M_OUT, t)
        return rcopy(packed.at[lax.rem(t, 2), :, :, 1 - c], wpk.at[pl.ds(0, 2), :, rr], red_sem.at[DSS, slot_of(1, t)], red_sem.at[DSR, slot_of(1, t)], to_core)

    def start_in(t):
        own_load(t).start()
        pair_in(t).start()

    def pack_out(t):
        raw_load(t).wait()
        slot = lax.rem(t, 2)

        @pl.when(t >= 2)
        def _():
            pair_out(t - 2).wait_send()

        def unit(u, _):
            base = aligned(PART * u, SUB)
            tiles = [[raw[slot, pl.ds(base + SUB * k, SUB), LANE * i:LANE * i + LANE] for i in range(10)] for k in range(QUAD)]
            ln = lanes((SUB, LANE))
            for s in range(SUB):
                jj, first = s % QUAD, 5 * (s // QUAD) + s % QUAD
                tail = NO
                for k in range(QUAD):
                    lo, hi = tiles[k][first], tiles[k][first + 1]
                    head = lo if jj == 0 else pltpu.roll(jnp.where(ln >= PART * jj, lo, hi), LANE - PART * jj, 1)
                    packed[slot, s // QUAD, (s // 2) % 2, s % 2, pl.ds(aligned(SUB * u, SUB), SUB), LANE * k:LANE * k + LANE] = head
                    turn = (PART * (k - jj)) % LANE
                    part = hi if turn == 0 else pltpu.roll(hi, turn, 1)
                    tail = part if tail is NO else jnp.where(ln >= PART * k, part, tail)
                packed[slot, s // QUAD, (s // 2) % 2, s % 2, pl.ds(aligned(SUB * u, SUB), SUB), 512:640] = tail
            return 0

        lax.fori_loop(0, RAW_STEP // PART, unit, 0)
        pair_out(t).start()

        @pl.when(t + 2 < STEPS)
        def _():
            raw_load(t + 2).start()

    def reduce_first(ph, w, m, t):
        rr, _, _ = spans(m, t)
        if ph == 0:
            own_load(t).wait()
            pair_in(t).wait_recv()
            slot = lax.rem(t, 3)
            for yy in range(2):
                for xx in range(2):
                    for r in range(0, 2 * m, SUB):
                        rows = pl.ds(aligned(2 * m * t + r, SUB), SUB)
                        w[yy, xx, rows] = w[yy, xx, rows] + own_in[slot, yy, xx, r:r + SUB]
        else:
            pair_out(t).wait_recv()
            slot = lax.rem(t, 2)

            def add(i, _):
                rows = pl.ds(aligned(2 * m * t + SUB2 * i, SUB), SUB2)
                for yy in range(2):
                    for xx in range(2):
                        w[yy, xx, rows] = w[yy, xx, rows] + packed[slot, yy, xx, c, pl.ds(aligned(SUB2 * i, SUB), SUB2)]
                return 0

            lax.fori_loop(0, 2 * m // SUB2, add, 0)
        for copy in first_copies(ph, w, m, t):
            copy.start()

    def reduce_second(ph, w, m, t):
        _, ra, rb = spans(m, t)
        a, b = first_copies(ph, w, m, t)
        a2, b2_ = second_copies(ph, w, m, t)
        if ph == 0:
            pair_in(t).wait_send()
        a.wait_recv()
        w[1 - y, x, ra] = w[1 - y, x, ra] + w[2, 1 - y, ra]
        a2.start()
        b.wait_recv()
        w[y, 1 - x, rb] = w[y, 1 - x, rb] + w[2, 1 - x, rb]
        b2_.start()

    def reduce_third(ph, w, m, t, gs):
        _, ra, rb = spans(m, t)
        first, second = first_copies(ph, w, m, t), second_copies(ph, w, m, t)
        second[0].wait_recv()
        ga = w[y, x, ra] + w[2, y, ra] + w[3, 0, ra]
        gs[ra] = ga
        second[1].wait_recv()
        gb = w[y, x, rb] + w[2, x, rb] + w[3, 0, rb]
        gs[rb] = gb
        for copy in (*first, *second):
            copy.wait_send()
        if ph == 0:
            sa, sb = ga * ga + 1e-30, gb * gb + 1e-30
            col_acc[...] = col_acc[...] + (sa + sb)
            for rows, sq in ((ra, sa), (rb, sb)):
                part = sq[:, 0:LANE]
                for i in range(1, COLS_IN // LANE):
                    part = part + sq[:, LANE * i:LANE * i + LANE]
                row_acc[rows] = part

    def gather_own(ph, w, m, t):
        rr, _, _ = spans(m, t)
        src = w.at[p, c, rr]
        return (rcopy(src, src, gat_sem.at[OXS, slot_of(ph, t)], gat_sem.at[OXR, slot_of(ph, t)], to_x),
                rcopy(src, src, gat_sem.at[OYS, slot_of(ph, t)], gat_sem.at[OYR, slot_of(ph, t)], to_y),
                rcopy(src, src, gat_sem.at[OPS, slot_of(ph, t)], gat_sem.at[OPR, slot_of(ph, t)], to_core))

    def gather_came(ph, w, m, t):
        rr, _, _ = spans(m, t)
        return (rcopy(w.at[p_x, c, rr], w.at[p_x, c, rr], gat_sem.at[OXS, slot_of(ph, t)], gat_sem.at[OXR, slot_of(ph, t)], to_x),
                rcopy(w.at[p_y, c, rr], w.at[p_y, c, rr], gat_sem.at[OYS, slot_of(ph, t)], gat_sem.at[OYR, slot_of(ph, t)], to_y))

    def gather_on(ph, w, m, t):
        _, ra, rb = spans(m, t)
        return (rcopy(w.at[p_y, c, ra], w.at[p_y, c, ra], gat_sem.at[FXS, slot_of(ph, t)], gat_sem.at[FXR, slot_of(ph, t)], to_x),
                rcopy(w.at[p_x, c, rb], w.at[p_x, c, rb], gat_sem.at[FYS, slot_of(ph, t)], gat_sem.at[FYR, slot_of(ph, t)], to_y))

    def gather_diag(ph, w, m, t):
        _, ra, rb = spans(m, t)
        return (rcopy(w.at[p_d, c, ra], w.at[p_d, c, ra], gat_sem.at[FXS, slot_of(ph, t)], gat_sem.at[FXR, slot_of(ph, t)], to_x),
                rcopy(w.at[p_d, c, rb], w.at[p_d, c, rb], gat_sem.at[FYS, slot_of(ph, t)], gat_sem.at[FYR, slot_of(ph, t)], to_y))

    def gather_pair(ph, w, m, t, cc):
        rr, _, _ = spans(m, t)
        return [rcopy(w.at[pp, cc, rr], w.at[pp, cc, rr], gat_sem.at[s, slot_of(ph, t)], gat_sem.at[s + 1, slot_of(ph, t)], to_core)
                for pp, s in ((p_x, PXS), (p_y, PYS), (p_d, PDS))]

    def gather_first(ph, w, m, t):
        for copy in gather_own(ph, w, m, t):
            copy.start()

    def gather_second(ph, w, m, t):
        rr, _, _ = spans(m, t)
        came = gather_came(ph, w, m, t)
        on = gather_on(ph, w, m, t)
        pair = gather_pair(ph, w, m, t, c)
        came[0].wait_recv()
        on[1].start()
        pair[0].start()
        came[1].wait_recv()
        on[0].start()
        pair[1].start()
        rcopy(w.at[p, 1 - c, rr], w.at[p, 1 - c, rr], gat_sem.at[OPS, slot_of(ph, t)], gat_sem.at[OPR, slot_of(ph, t)], to_core).wait_recv()

    def gather_third(ph, w, m, t):
        diag = gather_diag(ph, w, m, t)
        diag[0].wait_recv()
        diag[1].wait_recv()
        gather_pair(ph, w, m, t, c)[2].start()
        for copy in gather_pair(ph, w, m, t, 1 - c)[:2]:
            copy.wait_recv()
        for copy in gather_own(ph, w, m, t):
            copy.wait_send()

    def gather_last(ph, w, m, t):
        gather_pair(ph, w, m, t, 1 - c)[2].wait_recv()
        for copy in (*gather_on(ph, w, m, t), *gather_pair(ph, w, m, t, c)):
            copy.wait_send()

    def z_share(src, dst, k):
        return rcopy(src, dst, ex_sem.at[k, 0], ex_sem.at[k, 1], to_z)

    def share(buf, k):
        copy = rcopy(buf.at[0], buf.at[1], ex_sem.at[k, 2], ex_sem.at[k, 3], to_core)
        copy.start()
        copy.wait()
        return buf[0] + buf[1]

    def to_chips(buf, k):
        for i, dev in enumerate((to_x, to_y, to_d)):
            rcopy(buf.at[p], buf.at[p], ex_sem.at[k, QUAD + i], ex_sem.at[k, QUAD + 3 + i], dev).start()

    def from_chips(buf, k):
        for i, (dev, other) in enumerate(((to_x, p_x), (to_y, p_y), (to_d, p_d))):
            rcopy(buf.at[other], buf.at[other], ex_sem.at[k, QUAD + i], ex_sem.at[k, QUAD + 3 + i], dev).wait()
        return buf[0] + buf[1] + buf[2] + buf[3]

    def old_lanes(ref, width):
        acc = jnp.zeros((1, LANE), F32)
        for i in range(0, width, LANE):
            part = ref[:, i:min(i + LANE, width)]
            acc = acc + (part if part.shape[1] == LANE else pad_lanes(part))
        return acc

    def share_squares(acc, zt, pt, ct):
        zt[0] = jnp.sum(acc, axis=0, keepdims=True)
        copy = z_share(zt.at[0], zt.at[1], 1)
        copy.start()
        copy.wait()
        pt[0] = zt[0] + zt[1]
        ct[p] = share(pt, 1)
        to_chips(ct, 1)

    def scale_from(ct, count):
        mean = jnp.sum(from_chips(ct, 1), axis=1, keepdims=True) / count
        return 0.1 / jnp.maximum(1.0, jnp.sqrt(mean))

    def stats_in_send():
        copy = z_share(row_acc, row_peer, 0)
        copy.start()
        v_in[0, :, 0:COLS_IN] = jnp.sum(col_acc[...], axis=0, keepdims=True)
        v_in[0, :, COLS_IN + LANE:COLS_IN + 2 * LANE] = old_lanes(r_in, ROWS_IN)
        copy.wait()
        v_in[0, :, COLS_IN:COLS_IN + LANE] = jnp.sum(row_acc[...] + row_peer[...], axis=0, keepdims=True)
        vc_in[p] = share(v_in, 0)
        to_chips(vc_in, 0)
        w_load_in().start()

    def w_load_in():
        return pltpu.make_async_copy(w_in.at[p, c], win.at[p, c], load_sem.at[0])

    def stats_in_norm():
        vec = from_chips(vc_in, 0)
        c_new = b2 * c_in[...] + (1.0 - b2) * (vec[:, 0:COLS_IN] / rows_all_in)
        c_in_new[...] = c_new
        bj_in[...] = 1.0 / jnp.sqrt(c_new)
        s_total = jnp.sum(vec[:, COLS_IN:COLS_IN + LANE], axis=1, keepdims=True)
        r_total = jnp.sum(vec[:, COLS_IN + LANE:COLS_IN + 2 * LANE], axis=1, keepdims=True)
        r_avg = (b2 * r_total + (1.0 - b2) * (s_total / cols_all_in)) / rows_all_in
        root_avg = jnp.sqrt(r_avg)
        row_mean = jnp.sum(row_acc[...] + row_peer[...], axis=1, keepdims=True) / cols_all_in
        row_mean = jnp.broadcast_to(row_mean, (ROWS_IN, LANE))
        r_old = jnp.concatenate([row_to_col(r_in[:, 0:LANE]), row_to_col(pad_lanes(r_in[:, LANE:WIDTH]))[0:PART]], axis=0)
        r_new = b2 * r_old + (1.0 - b2) * row_mean
        r_in_new[:, 0:LANE] = r_new[0:LANE].T[0:1]
        r_in_new[:, LANE:WIDTH] = jnp.concatenate([r_new[LANE:WIDTH], jnp.zeros((96, LANE), F32)], axis=0).T[0:1, 0:PART]
        ai_in[...] = root_avg / jnp.sqrt(r_new)

        def body(i, acc):
            rows = pl.ds(aligned(SUB * i, SUB), SUB)
            a = ai_in[rows]
            for k in range(COLS_IN // LANE):
                col = slice(LANE * k, LANE * k + LANE)
                u = gs_in[rows, col] * a * bj_in[:, col]
                acc = acc + u * u
            return acc

        share_squares(lax.fori_loop(0, ROWS_IN // SUB, body, jnp.zeros((SUB, LANE), F32)), zt_in, pt_in, ct_in)

    def update_in():
        scale = scale_from(ct_in, float(rows_all_in * cols_all_in))
        w_load_in().wait()
        m_load_in().wait()

        def body(i, _):
            rows = pl.ds(aligned(SUB2 * i, SUB2), SUB2)
            a = ai_in[rows] * scale
            for k in range(COLS_IN // LANE):
                col = slice(LANE * k, LANE * k + LANE)
                u = gs_in[rows, col] * a * bj_in[:, col]
                mom = (0.9 * m_in_new[rows, col].astype(F32) + u).astype(BF16)
                m_in_new[rows, col] = mom
                old = win[p, c, rows, col]
                win[p, c, rows, col] = old - lr * mom.astype(F32) - lr * wd * old
            return 0

        lax.fori_loop(0, ROWS_IN // SUB2, body, 0)

    def m_load_in():
        return pltpu.make_async_copy(m_in, m_in_new, load_sem.at[1])

    def block_out(t):
        heads, tails = [], []
        for u in range(QUAD):
            rows = pl.ds(aligned(PART * t + SUB * u, SUB), SUB)
            tail = gs_out[rows, 512:640]
            for k in range(QUAD):
                heads.append(gs_out[rows, LANE * k:LANE * k + LANE])
                tails.append(tail if k == 0 else pltpu.roll(tail, LANE - PART * k, 1))
        tails = jnp.concatenate(tails, axis=0)
        return jnp.concatenate(heads, axis=0), jnp.where(lanes((LANE, LANE)) < PART, tails, 0.0)

    def stats_out_send():
        def body(t, acc):
            head, tail = block_out(t)
            sh = head * head + 1e-30
            st = jnp.where(lanes((LANE, LANE)) < PART, tail * tail + 1e-30, 0.0)
            v_out[0, :, pl.ds(aligned(LANE * t, LANE), LANE)] = jnp.sum((sh + st).T, axis=0, keepdims=True)
            ah, at = acc
            for i in range(SUB2):
                ah = ah + sh[SUB * i:SUB * i + SUB]
                at = at + st[SUB * i:SUB * i + SUB]
            return ah, at

        zero = jnp.zeros((SUB, LANE), F32)
        ah, at = lax.fori_loop(0, TILES_OUT, body, (zero, zero))
        col_acc_out[0:SUB] = ah
        col_acc_out[SUB:SUB2] = at
        col_acc_out[SUB2:SUB2 + SUB] = jnp.broadcast_to(old_lanes(r_out, RAW_OUT), (SUB, LANE))
        copy = z_share(col_acc_out, col_peer_out, 0)
        copy.start()
        copy.wait()
        v_out[0, :, RAW_OUT:RAW_OUT + LANE] = jnp.sum(col_acc_out[0:SUB2] + col_peer_out[0:SUB2], axis=0, keepdims=True)
        vc_out[p] = share(v_out, 0)
        to_chips(vc_out, 0)

    def stats_out_norm():
        vec = from_chips(vc_out, 0)
        r_out_new[...] = b2 * r_out[...] + (1.0 - b2) * (vec[:, 0:RAW_OUT] / cols_all_out)
        s_total = jnp.sum(vec[:, RAW_OUT:RAW_OUT + LANE], axis=1, keepdims=True)
        r_total = jnp.sum((col_acc_out[SUB2:SUB2 + SUB] + col_peer_out[SUB2:SUB2 + SUB])[0:1], axis=1, keepdims=True)
        r_avg = (b2 * r_total + (1.0 - b2) * (s_total / cols_all_out)) / rows_all_out
        root_avg = jnp.sqrt(r_avg)
        cols = col_acc_out[...] + col_peer_out[...]
        c_new_h = b2 * c_out[:, 0:LANE] + (1.0 - b2) * (jnp.sum(cols[0:SUB], axis=0, keepdims=True) / rows_all_out)
        c_new_t = b2 * pad_lanes(c_out[:, LANE:WIDTH]) + (1.0 - b2) * (jnp.sum(cols[SUB:SUB2], axis=0, keepdims=True) / rows_all_out)
        c_out_new[:, 0:LANE] = c_new_h
        c_out_new[:, LANE:WIDTH] = c_new_t[:, 0:PART]
        vec_x[...] = jnp.broadcast_to(1.0 / jnp.sqrt(c_new_h), (SUB, LANE))
        vec_y[...] = jnp.broadcast_to(1.0 / jnp.sqrt(jnp.where(lanes((1, LANE)) < PART, c_new_t, 1.0)), (SUB, LANE))
        bh, bt = vec_x[0:1], vec_y[0:1]

        def body(t, acc):
            rows = pl.ds(aligned(LANE * t, LANE), LANE)
            a = row_to_col(root_avg / jnp.sqrt(r_out_new[:, rows]))
            ai_out[rows] = a
            head, tail = block_out(t)
            uh, ut = head * a * bh, tail * a * bt
            sq = uh * uh + ut * ut
            for i in range(SUB2):
                acc = acc + sq[SUB * i:SUB * i + SUB]
            return acc

        share_squares(lax.fori_loop(0, TILES_OUT, body, jnp.zeros((SUB, LANE), F32)), zt_out, pt_out, ct_out)

    def w_load_out():
        first = 5 * (q // QUAD) + j
        return pltpu.make_async_copy(w_out.at[:, pl.ds(aligned(LANE * first, LANE), 256)], w_cols, load_sem.at[2])

    def m_load_out():
        return pltpu.make_async_copy(m_out, m_out_new, load_sem.at[3])

    def update_out():
        scale = scale_from(ct_out, float(rows_all_out * cols_all_out))
        w_load_out().wait()
        m_load_out().wait()
        bh, bt = vec_x[0:1], vec_y[0:1]
        back = PART * ((QUAD - j) % QUAD)

        def body(t, _):
            rows = pl.ds(aligned(LANE * t, LANE), LANE)
            a = ai_out[rows] * scale
            head, tail = block_out(t)
            uh, ut = head * a * bh, tail * a * bt
            mom = m_out_new[:, rows].astype(F32)
            mh = (0.9 * mom[0:LANE].T + uh).astype(BF16).astype(F32)
            mt = (0.9 * jnp.concatenate([mom[LANE:WIDTH], jnp.zeros((96, LANE), F32)], axis=0).T + ut).astype(BF16).astype(F32)
            m_out_new[0:LANE, rows] = mh.T.astype(BF16)
            m_out_new[LANE:WIDTH, rows] = mt.T[0:PART].astype(BF16)
            lo, hi = w_cols[rows, 0:LANE], w_cols[rows, LANE:256]
            wh = pltpu.roll(jnp.where(lanes((LANE, LANE)) >= PART * j, lo, hi), back, 1)
            wt = pltpu.roll(hi, back, 1)
            wh = wh - lr * mh - lr * wd * wh
            wt = wt - lr * mt - lr * wd * wt
            ln = lanes((SUB, LANE))
            for u in range(QUAD):
                to = pl.ds(aligned(PART * t + SUB * u, SUB), SUB)
                joined = NO
                for k in range(QUAD):
                    at = PART * u + SUB * k
                    wpk[p, c, to, LANE * k:LANE * k + LANE] = wh[at:at + SUB]
                    part = wt[at:at + SUB] if k == 0 else pltpu.roll(wt[at:at + SUB], PART * k, 1)
                    joined = part if joined is NO else jnp.where(ln >= PART * k, part, joined)
                wpk[p, c, to, 512:640] = joined
            return 0

        lax.fori_loop(0, TILES_OUT, body, 0)

    col_acc[...] = jnp.zeros_like(col_acc)
    own_load(0).start()
    own_load(1).start()
    pl.semaphore_wait(barrier, QUAD)
    pair_in(0).start()
    pair_in(1).start()

    def at_step(cond, fn, *args):
        @pl.when(cond)
        def _():
            fn(*args)

    n = STEPS

    def step(s, _):
        def within(lo, hi):
            return jnp.logical_and(s >= lo, s < hi)

        at_step(s + 2 < n, start_in, s + 2)
        at_step(s < n, reduce_first, 0, win, M_IN, s)
        at_step(within(2, n + 2), reduce_second, 0, win, M_IN, s - 2)
        at_step(within(QUAD, n + QUAD), reduce_third, 0, win, M_IN, s - QUAD, gs_in)

        @pl.when(s == 2)
        def _():
            m_load_in().start()
            m_load_out().start()
            w_load_out().start()

        @pl.when(s == n - 3)
        def _():
            raw_load(0).start()
            raw_load(1).start()

        at_step(within(n, 2 * n), reduce_first, 1, wpk, M_OUT, s - n)
        at_step(within(n - 1, 2 * n - 1), pack_out, s - n + 1)
        at_step(within(n + 2, 2 * n + 2), reduce_second, 1, wpk, M_OUT, s - n - 2)
        at_step(within(n + QUAD, 2 * n + QUAD), reduce_third, 1, wpk, M_OUT, s - n - QUAD, gs_out)
        at_step(s == n + 3, stats_in_send)
        at_step(s == n + 6, stats_in_norm)
        at_step(s == n + 9, update_in)
        at_step(within(2 * n, 3 * n), gather_first, 0, win, M_IN, s - 2 * n)
        at_step(within(2 * n + 2, 3 * n + 2), gather_second, 0, win, M_IN, s - 2 * n - 2)
        at_step(within(2 * n + QUAD, 3 * n + QUAD), gather_third, 0, win, M_IN, s - 2 * n - QUAD)
        at_step(s == 2 * n + 3, stats_out_send)
        at_step(s == 2 * n + 6, stats_out_norm)
        at_step(s == 2 * n + 9, update_out)
        at_step(within(3 * n, QUAD * n), gather_first, 1, wpk, M_OUT, s - 3 * n)
        at_step(within(3 * n + 2, QUAD * n + 2), gather_second, 1, wpk, M_OUT, s - 3 * n - 2)
        at_step(within(3 * n + QUAD, QUAD * n + QUAD), gather_third, 1, wpk, M_OUT, s - 3 * n - QUAD)
        at_step(within(2 * n + 6, 3 * n + 6), gather_last, 0, win, M_IN, s - 2 * n - 6)
        at_step(within(3 * n + 6, QUAD * n + 6), gather_last, 1, wpk, M_OUT, s - 3 * n - 6)
        return 0

    lax.fori_loop(0, QUAD * n + 6, step, 0)
    pair_out(n - 2).wait_send()
    pair_out(n - 1).wait_send()


def final_kernel(win, wpk, mi, mo, ri, ci, ro, co, win_o, wout_o, mi_o, mo_o, ri_o, ci_o, ro_o, co_o, stage, sem, stage_sem):
    plain = [pltpu.make_async_copy(win, win_o, sem.at[0])]
    for i, (src, dst) in enumerate(((mi, mi_o), (mo, mo_o), (ri, ri_o), (ci, ci_o), (ro, ro_o), (co, co_o))):
        plain.append(pltpu.make_async_copy(src, dst, sem.at[i + 1]))
    for copy in plain:
        copy.start()

    def rows_of(t):
        return pl.ds(aligned(RAW_STEP * t, SUB), RAW_STEP)

    def put(t):
        return pltpu.make_async_copy(stage.at[rows_of(t)], wout_o.at[rows_of(t)], stage_sem.at[t])

    def chunk(t, _):
        def unit(u, _):
            ln = lanes((SUB, LANE))
            rows = pl.ds(aligned(2 * M_OUT * t + SUB * u, SUB), SUB)
            for half in range(2):
                tails = [wpk[2 * half + jj // 2, jj % 2, rows, 512:640] for jj in range(QUAD)]
                for k in range(QUAD):
                    to = pl.ds(aligned(RAW_STEP * t + PART * u + SUB * k, SUB), SUB)
                    heads = []
                    for jj in range(QUAD):
                        head = wpk[2 * half + jj // 2, jj % 2, rows, LANE * k:LANE * k + LANE]
                        heads.append(head if jj == 0 else pltpu.roll(head, PART * jj, 1))
                    ends = [tails[jj] if jj == k else pltpu.roll(tails[jj], (PART * (jj - k)) % LANE, 1) for jj in range(QUAD)]
                    for tile in range(5):
                        if tile == 0:
                            out = heads[0]
                        else:
                            out = ends[tile - 1]
                            if tile > 1:
                                out = jnp.where(ln < PART * (tile - 1), heads[tile - 1], out)
                            if tile < QUAD:
                                out = jnp.where(ln >= PART * tile, heads[tile], out)
                        at = LANE * (5 * half + tile)
                        stage[to, at:at + LANE] = out
            return 0

        lax.fori_loop(0, RAW_STEP // PART, unit, 0)
        put(t).start()
        return 0

    lax.fori_loop(0, STEPS, chunk, 0)
    for t in range(STEPS):
        put(t).wait()
    for copy in plain:
        copy.wait()


def solution(mesh):
    n_tp = mesh.shape['tp']
    n_dp = mesh.shape['dp']
    vmem = pl.BlockSpec(memory_space=pltpu.VMEM)
    hbm = pl.BlockSpec(memory_space=pltpu.HBM)
    smem = pl.BlockSpec(memory_space=pltpu.SMEM)
    dma = pltpu.SemaphoreType.DMA
    kept = (
        ((QUAD, 2, ROWS_IN, COLS_IN), F32),
        ((QUAD, 2, ROWS_OUT, COLS_OUT), F32),
        ((ROWS_IN, COLS_IN), BF16),
        ((WIDTH, RAW_OUT), BF16),
        ((1, ROWS_IN), F32),
        ((1, COLS_IN), F32),
        ((1, RAW_OUT), F32),
        ((1, WIDTH), F32),
    )
    main = pl.pallas_call(
        functools.partial(main_kernel, n_tp, n_dp, D, COLS_IN * n_tp, RAW_OUT * n_tp, D),
        out_shape=[pltpu.VMEM(shape, dtype) for shape, dtype in kept],
        in_specs=[hbm] * 6 + [vmem] * QUAD + [smem] * 3,
        out_specs=[vmem] * SUB,
        scratch_shapes=[
            pltpu.VMEM((3, 2, 2, 2 * M_IN, COLS_IN), F32),
            pltpu.VMEM((2, RAW_STEP, D), F32),
            pltpu.VMEM((2, 2, 2, 2, 2 * M_OUT, COLS_OUT), F32),
            pltpu.VMEM((ROWS_IN, COLS_IN), F32),
            pltpu.VMEM((ROWS_OUT, COLS_OUT), F32),
            pltpu.VMEM((RAW_OUT, 256), F32),
            pltpu.VMEM((RAW_OUT, LANE), F32),
            pltpu.VMEM((ROWS_IN, LANE), F32),
            pltpu.VMEM((1, COLS_IN), F32),
            pltpu.VMEM((SUB, LANE), F32),
            pltpu.VMEM((SUB, LANE), F32),
            pltpu.VMEM((SUB, COLS_IN), F32),
            pltpu.VMEM((ROWS_IN, LANE), F32),
            pltpu.VMEM((ROWS_IN, LANE), F32),
            pltpu.VMEM((SUB2 + SUB, LANE), F32),
            pltpu.VMEM((SUB2 + SUB, LANE), F32),
            pltpu.VMEM((2, 1, COLS_IN + 2 * LANE), F32),
            pltpu.VMEM((QUAD, 1, COLS_IN + 2 * LANE), F32),
            pltpu.VMEM((2, 1, RAW_OUT + LANE), F32),
            pltpu.VMEM((QUAD, 1, RAW_OUT + LANE), F32),
        ] + [pltpu.VMEM((i, 1, LANE), F32) for i in (2, 2, QUAD)] * 2 + [
            dma((N_RED, SLOTS)),
            dma((N_GAT, SLOTS)),
            dma((QUAD,)),
            dma((2, 10)),
        ],
        compiler_params=pltpu.CompilerParams(collective_id=0, has_side_effects=True, vmem_limit_bytes=GRANT),
    )
    final = pl.pallas_call(
        final_kernel,
        out_shape=[
            jax.ShapeDtypeStruct((QUAD, 2, ROWS_IN, COLS_IN), F32),
            jax.ShapeDtypeStruct((RAW_OUT, D), F32),
        ] + [jax.ShapeDtypeStruct(shape, dtype) for shape, dtype in kept[2:]],
        in_specs=[vmem] * SUB,
        out_specs=[hbm] * SUB,
        scratch_shapes=[pltpu.VMEM((RAW_OUT, D), F32), dma((7,)), dma((STEPS,))],
        compiler_params=pltpu.CompilerParams(vmem_limit_bytes=GRANT),
    )

    def body(w_in, w_out, g_in, g_out, m_in, m_out, r_in, c_in, r_out, c_out, learn_rate, weight_decay, beta_two):
        shards = (QUAD, 2, ROWS_IN, COLS_IN)
        got = main(
            w_in.reshape(shards), w_out[0], g_in.reshape((2, 2, 2, ROWS_IN, COLS_IN)), g_out[0, 0], m_in[0], m_out[0].T,
            r_in, c_in, r_out, c_out, learn_rate.reshape(1), weight_decay.reshape(1), beta_two.reshape(1))
        w_i, w_o, m_i, m_o, r_i, c_i, r_o, c_o = final(*[pltpu.with_memory_space_constraint(g, pltpu.VMEM) for g in got])
        return w_i.reshape((1, D, COLS_IN)), w_o[NO], m_i[NO], m_o.T[NO], r_i, c_i, r_o, c_o

    in_specs = (P(NO, NO, 'tp'), P(NO, 'tp', NO), P('dp', NO, NO, 'tp'), P('dp', NO, 'tp', NO), P(NO, 'dp', 'tp'), P(NO, 'tp', 'dp'), P(NO, 'dp'), P(NO, 'tp'), P(NO, 'tp'), P(NO, 'dp'), P(), P(), P())
    out_specs = (P(NO, NO, 'tp'), P(NO, 'tp', NO), P(NO, 'dp', 'tp'), P(NO, 'tp', 'dp'), P(NO, 'dp'), P(NO, 'tp'), P(NO, 'tp'), P(NO, 'dp'))
    return jax.shard_map(body, mesh=mesh, in_specs=in_specs, out_specs=out_specs, check_vma=False)
```

```python
import functools

import jax
import jax.numpy as jnp
from jax import lax
from jax.experimental import pallas as pl
from jax.experimental.pallas import tpu as pltpu
from jax.sharding import PartitionSpec as P

F32 = jnp.float32
BF16 = jnp.bfloat16
MESH = pl.DeviceIdType.MESH
LANE, SUB, SUB2, PART, QUAD, WIDTH = 128, 8, 16, 32, 4, 160
NO = None
BOTH, THREE = pl.ds(0, 2), pl.ds(0, 3)

D = 1280
ROWS_IN, COLS_IN = WIDTH, 4480
ROWS_OUT, COLS_OUT = 800, 640
RAW_OUT = 3200
STEPS = 10
M_IN = ROWS_IN // STEPS // 2
M_OUT = ROWS_OUT // STEPS // 2
RAW_STEP = RAW_OUT // STEPS
TILES_OUT = RAW_OUT // LANE

GRANT = 24 << 20

SLOTS, PAIR_SLOTS = 6, 10
N_RED, N_GAT, N_EX = 6, 4, 8
(OWN, DSS, DSR, SENT, R1, R2) = range(N_RED)
(S1, S2, R_OWN, R_ON) = range(N_GAT)
(ZS, ZR, CS, CR, TS, TR, BS, BR) = range(N_EX)
PIECES, PIECE = 5, COLS_IN // 5
LEN_IN, LEN_OUT = COLS_IN + 3 * LANE, RAW_OUT + LANE

def lanes(shape):
    return lax.broadcasted_iota(jnp.int32, shape, 1)


def aligned(value, by):
    return pl.multiple_of(value, by)


def pad_lanes(row):
    return jnp.concatenate([row, jnp.zeros((1, LANE - row.shape[1]), F32)], axis=1)


def row_to_col(row):
    return jnp.broadcast_to(row, (LANE, LANE)).T


def main_kernel(n_tp, n_dp, rows_all_in, cols_all_in, rows_all_out, cols_all_out,
                w_in, w_out, g_in, g_out, m_in, m_out, r_in_hbm, c_in_hbm, r_out_hbm, c_out_hbm, lr_ref, wd_ref, b2_ref,
                win, wpk, m_in_new, m_out_new, r_in_new, c_in_new, r_out_new, c_out_new,
                own_in, raw, packed, gs_in, gs_out, w_cols, ai_out, ai_in, bj_in, vec_x, vec_y,
                col_acc, row_acc, row_peer, col_acc_out, col_peer_out, v_in, vc_in, vf_in, v_out, vc_out, vf_out,
                r_in, c_in, r_out, c_out, zt_in, pt_in, ct_in, zt_out, pt_out, ct_out,
                red_sem, gat_sem, pair_sem, load_sem, ex_sem):
    tp = lax.axis_index('tp')
    q = lax.axis_index('dp')
    p, c = q // 2, q % 2
    y, x = p // 2, p % 2
    nx, ny, nc = 1 - x, 1 - y, 1 - c
    p_x, p_y, p_d = 2 * y + nx, 2 * ny + x, 2 * ny + nx
    to_x = {'dp': 2 * p_x + c}
    to_y = {'dp': 2 * p_y + c}
    to_d = {'dp': 2 * p_d + c}
    to_core = {'dp': 2 * p + nc}
    to_z = {'tp': 1 - tp}
    j = q % QUAD
    lr, wd, b2 = lr_ref[0], wd_ref[0], b2_ref[0]

    barrier = pltpu.get_barrier_semaphore()
    for dev in (to_x, to_y, to_core, to_z):
        pl.semaphore_signal(barrier, inc=1, device_id=dev, device_id_type=MESH)

    def rcopy(src, dst, send, recv, dev):
        return pltpu.make_async_remote_copy(src_ref=src, dst_ref=dst, send_sem=send, recv_sem=recv, device_id=dev, device_id_type=MESH)

    def slot_of(ph, t):
        return lax.rem(ph * STEPS + t, SLOTS)

    def spans(m, t):
        base = aligned(2 * m * t, SUB)
        return pl.ds(base, 2 * m), pl.ds(base, m), pl.ds(aligned(base + m, SUB), m)

    def first_copies(ph, w, m, t):
        _, ra, rb = spans(m, t)
        a = rcopy(w.at[BOTH, nx, ra], w.at[2, BOTH, ra], red_sem.at[SENT, slot_of(ph, t)], red_sem.at[R1, slot_of(ph, t)], to_x)
        b = rcopy(w.at[ny, BOTH, rb], w.at[2, BOTH, rb], red_sem.at[SENT, slot_of(ph, t)], red_sem.at[R1, slot_of(ph, t)], to_y)
        return a, b

    def second_copies(ph, w, m, t):
        _, ra, rb = spans(m, t)
        a = rcopy(w.at[ny, x, ra], w.at[3, 0, ra], red_sem.at[SENT, slot_of(ph, t)], red_sem.at[R2, slot_of(ph, t)], to_y)
        b = rcopy(w.at[y, nx, rb], w.at[3, 0, rb], red_sem.at[SENT, slot_of(ph, t)], red_sem.at[R2, slot_of(ph, t)], to_x)
        return a, b

    def wait_first(ph, w, m, t):
        rr, _, _ = spans(m, t)
        part = w.at[2, BOTH, rr]
        rcopy(part, part, red_sem.at[SENT, slot_of(ph, t)], red_sem.at[R1, slot_of(ph, t)], to_x).wait_recv()

    def wait_second(ph, w, m, t):
        rr, _, _ = spans(m, t)
        part = w.at[3, 0, rr]
        rcopy(part, part, red_sem.at[SENT, slot_of(ph, t)], red_sem.at[R2, slot_of(ph, t)], to_y).wait_recv()

    def wait_sent(ph, w, m, t):
        rr, _, _ = spans(m, t)
        part = w.at[THREE, 0, rr]
        rcopy(part, part, red_sem.at[SENT, slot_of(ph, t)], red_sem.at[R1, slot_of(ph, t)], to_x).wait_send()

    def pair_in(t):
        rr, _, _ = spans(M_IN, t)
        return rcopy(g_in.at[:, :, nc, rr], win.at[BOTH, :, rr], red_sem.at[DSS, slot_of(0, t)], red_sem.at[DSR, slot_of(0, t)], to_core)

    def piece_in(k):
        rows, cols = pl.ds(0, 2 * M_IN), pl.ds(PIECE * k, PIECE)
        return rcopy(g_in.at[:, :, nc, rows, cols], win.at[BOTH, :, rows, cols], red_sem.at[DSS, 0], load_sem.at[2 * QUAD + k], to_core)

    def reduce_start():
        own_load(0).wait()
        for k in range(PIECES):
            cols = pl.ds(PIECE * k, PIECE)
            piece_in(k).wait_recv()
            for yy in range(2):
                for xx in range(2):
                    win[yy, xx, 0:2 * M_IN, cols] = win[yy, xx, 0:2 * M_IN, cols] + own_in[0, yy, xx, :, cols]
            ra, rb = pl.ds(0, M_IN), pl.ds(M_IN, M_IN)
            rcopy(win.at[BOTH, nx, ra, cols], win.at[2, BOTH, ra, cols], red_sem.at[SENT, 0], red_sem.at[R1, 0], to_x).start()
            rcopy(win.at[ny, BOTH, rb, cols], win.at[2, BOTH, rb, cols], red_sem.at[SENT, 0], red_sem.at[R1, 0], to_y).start()

    def own_load(t):
        rr, _, _ = spans(M_IN, t)
        return pltpu.make_async_copy(g_in.at[:, :, c, rr], own_in.at[lax.rem(t, 3)], red_sem.at[OWN, slot_of(0, t)])

    def raw_load(t):
        return pltpu.make_async_copy(g_out.at[pl.ds(aligned(RAW_STEP * t, SUB), RAW_STEP)], raw.at[lax.rem(t, 2)], red_sem.at[OWN, slot_of(1, t)])

    def pair_out(t):
        rr, _, _ = spans(M_OUT, t)
        return rcopy(packed.at[lax.rem(t, 2), :, :, nc], wpk.at[BOTH, :, rr], red_sem.at[DSS, slot_of(1, t)], red_sem.at[DSR, slot_of(1, t)], to_core)

    def start_in(t):
        own_load(t).start()
        pair_in(t).start()

    def pack_out(t):
        raw_load(t).wait()
        slot = lax.rem(t, 2)

        @pl.when(t >= 2)
        def _():
            pair_out(t - 2).wait_send()

        def unit(u, _):
            base = aligned(PART * u, SUB)
            tiles = [[raw[slot, pl.ds(base + SUB * k, SUB), LANE * i:LANE * i + LANE] for i in range(10)] for k in range(QUAD)]
            ln = lanes((SUB, LANE))
            for s in range(SUB):
                jj, first = s % QUAD, 5 * (s // QUAD) + s % QUAD
                tail = NO
                for k in range(QUAD):
                    lo, hi = tiles[k][first], tiles[k][first + 1]
                    head = lo if jj == 0 else pltpu.roll(jnp.where(ln >= PART * jj, lo, hi), LANE - PART * jj, 1)
                    packed[slot, s // QUAD, (s // 2) % 2, s % 2, pl.ds(aligned(SUB * u, SUB), SUB), LANE * k:LANE * k + LANE] = head
                    turn = (PART * (k - jj)) % LANE
                    part = hi if turn == 0 else pltpu.roll(hi, turn, 1)
                    tail = part if tail is NO else jnp.where(ln >= PART * k, part, tail)
                packed[slot, s // QUAD, (s // 2) % 2, s % 2, pl.ds(aligned(SUB * u, SUB), SUB), 512:640] = tail
            return 0

        lax.fori_loop(0, RAW_STEP // PART, unit, 0)
        pair_out(t).start()

        @pl.when(t + 2 < STEPS)
        def _():
            raw_load(t + 2).start()

    def reduce_first(ph, w, m, t):
        rr, _, _ = spans(m, t)
        if ph == 0:
            own_load(t).wait()
            pair_in(t).wait_recv()
            slot = lax.rem(t, 3)
            for yy in range(2):
                for xx in range(2):
                    for r in range(0, 2 * m, SUB):
                        rows = pl.ds(aligned(2 * m * t + r, SUB), SUB)
                        w[yy, xx, rows] = w[yy, xx, rows] + own_in[slot, yy, xx, r:r + SUB]
        else:
            pair_out(t).wait_recv()
            slot = lax.rem(t, 2)

            def add(i, _):
                rows = pl.ds(aligned(2 * m * t + SUB2 * i, SUB), SUB2)
                for yy in range(2):
                    for xx in range(2):
                        w[yy, xx, rows] = w[yy, xx, rows] + packed[slot, yy, xx, c, pl.ds(aligned(SUB2 * i, SUB), SUB2)]
                return 0

            lax.fori_loop(0, 2 * m // SUB2, add, 0)
        for copy in first_copies(ph, w, m, t):
            copy.start()

    def reduce_second(ph, w, m, t):
        _, ra, rb = spans(m, t)
        on_y, on_x = second_copies(ph, w, m, t)
        if ph == 0:
            pair_in(t).wait_send()
        wait_first(ph, w, m, t)
        w[ny, x, ra] = w[ny, x, ra] + w[2, ny, ra]
        on_y.start()
        w[y, nx, rb] = w[y, nx, rb] + w[2, nx, rb]
        on_x.start()

    def reduce_third(ph, w, m, t, gs):
        _, ra, rb = spans(m, t)
        wait_second(ph, w, m, t)
        ga = w[y, x, ra] + w[2, y, ra] + w[3, 0, ra]
        gs[ra] = ga
        gb = w[y, x, rb] + w[2, x, rb] + w[3, 0, rb]
        gs[rb] = gb
        wait_sent(ph, w, m, t)
        if ph == 0:
            sa, sb = ga * ga + 1e-30, gb * gb + 1e-30
            col_acc[...] = col_acc[...] + (sa + sb)
            for rows, sq in ((ra, sa), (rb, sb)):
                part = sq[:, 0:LANE]
                for i in range(1, COLS_IN // LANE):
                    part = part + sq[:, LANE * i:LANE * i + LANE]
                row_acc[rows] = part

    def sems(ph, t, send, recv):
        return gat_sem.at[send, slot_of(ph, t)], gat_sem.at[recv, slot_of(ph, t)]

    def pair_sems(ph, t, send):
        return gat_sem.at[send, slot_of(ph, t)], pair_sem.at[lax.rem(ph * STEPS + t, PAIR_SLOTS)]

    def gather_first(ph, w, m, t):
        rr, _, _ = spans(m, t)
        src = w.at[p, c, rr]
        rcopy(src, src, *sems(ph, t, S1, R_OWN), to_x).start()
        rcopy(src, src, *sems(ph, t, S1, R_OWN), to_y).start()
        rcopy(src, src, *pair_sems(ph, t, S1), to_core).start()

    def gather_second(ph, w, m, t):
        rr, ra, rb = spans(m, t)
        both = w.at[BOTH, c, rr]
        rcopy(both, both, *sems(ph, t, S1, R_OWN), to_x).wait_recv()
        for other, rows, dev in ((p_x, rb, to_y), (p_y, ra, to_x)):
            rcopy(w.at[other, c, rows], w.at[other, c, rows], *sems(ph, t, S2, R_ON), dev).start()
            rcopy(w.at[other, c, rr], w.at[other, c, rr], *pair_sems(ph, t, S2), to_core).start()

    def gather_third(ph, w, m, t):
        rr, _, _ = spans(m, t)
        diag = w.at[p_d, c, rr]
        rcopy(diag, diag, *sems(ph, t, S2, R_ON), to_x).wait_recv()
        rcopy(diag, diag, *pair_sems(ph, t, S2), to_core).start()
        three = w.at[THREE, c, rr]
        rcopy(three, three, *sems(ph, t, S1, R_OWN), to_x).wait_send()

    def gather_last(ph, w, m, t):
        rr, _, _ = spans(m, t)
        four = w.at[:, nc, rr]
        rcopy(four, four, *pair_sems(ph, t, S2), to_core).wait_recv()
        rcopy(four, four, *pair_sems(ph, t, S2), to_core).wait_send()

    def z_share(src, dst, k):
        return rcopy(src, dst, ex_sem.at[k, ZS], ex_sem.at[k, ZR], to_z)

    def share(buf, k):
        copy = rcopy(buf.at[0], buf.at[1], ex_sem.at[k, CS], ex_sem.at[k, CR], to_core)
        copy.start()
        copy.wait()
        return buf[0] + buf[1]

    def to_chips(buf, k):
        for dev in (to_x, to_y, to_d):
            rcopy(buf.at[p], buf.at[p], ex_sem.at[k, TS], ex_sem.at[k, TR], dev).start()

    def from_chips(buf, k):
        three = buf.at[THREE]
        rcopy(three, three, ex_sem.at[k, TS], ex_sem.at[k, TR], to_x).wait()
        return buf[0] + buf[1] + buf[2] + buf[3]

    def halves(length):
        half = length // 2
        return pl.ds(aligned(c * half, LANE), half), pl.ds(aligned(nc * half, LANE), half)

    def vector_send(buf, chips, length):
        mine, other = halves(length)
        copy = rcopy(buf.at[0, :, other], buf.at[1, :, other], ex_sem.at[0, CS], ex_sem.at[0, CR], to_core)
        copy.start()
        copy.wait()
        chips[p] = buf[0, :, mine] + buf[1, :, mine]
        to_chips(chips, 0)

    def vector_take(chips, whole, length):
        mine, _ = halves(length)
        whole[:, mine] = from_chips(chips, 0)
        copy = rcopy(whole.at[:, mine], whole.at[:, mine], ex_sem.at[0, BS], ex_sem.at[0, BR], to_core)
        copy.start()
        copy.wait()

    def old_lanes(ref, width):
        acc = jnp.zeros((1, LANE), F32)
        for i in range(0, width, LANE):
            part = ref[:, i:min(i + LANE, width)]
            acc = acc + (part if part.shape[1] == LANE else pad_lanes(part))
        return acc

    def share_squares(acc, zt, pt, ct):
        zt[0] = jnp.sum(acc, axis=0, keepdims=True)
        copy = z_share(zt.at[0], zt.at[1], 1)
        copy.start()
        copy.wait()
        pt[0] = zt[0] + zt[1]
        ct[p] = share(pt, 1)
        to_chips(ct, 1)

    def scale_from(ct, count):
        mean = jnp.sum(from_chips(ct, 1), axis=1, keepdims=True) / count
        return 0.1 / jnp.maximum(1.0, jnp.sqrt(mean))

    def vec_loads():
        pairs = ((r_in_hbm, r_in), (c_in_hbm, c_in), (r_out_hbm, r_out), (c_out_hbm, c_out))
        return [pltpu.make_async_copy(src, dst, load_sem.at[QUAD + i]) for i, (src, dst) in enumerate(pairs)]

    def stats_in_send():
        for load in vec_loads():
            load.wait()
        copy = z_share(row_acc, row_peer, 0)
        copy.start()
        v_in[0, :, 0:COLS_IN] = jnp.sum(col_acc[...], axis=0, keepdims=True)
        v_in[0, :, COLS_IN + LANE:COLS_IN + 2 * LANE] = old_lanes(r_in, ROWS_IN)
        v_in[0, :, COLS_IN + 2 * LANE:LEN_IN] = jnp.zeros((1, LANE), F32)
        copy.wait()
        v_in[0, :, COLS_IN:COLS_IN + LANE] = jnp.sum(row_acc[...] + row_peer[...], axis=0, keepdims=True)
        vector_send(v_in, vc_in, LEN_IN)
        w_load_in().start()

    def w_load_in():
        return pltpu.make_async_copy(w_in.at[p, c], win.at[p, c], load_sem.at[0])

    def stats_in_norm():
        vector_take(vc_in, vf_in, LEN_IN)
        vec = vf_in[...]
        c_new = b2 * c_in[...] + (1.0 - b2) * (vec[:, 0:COLS_IN] / rows_all_in)
        c_in_new[...] = c_new
        bj_in[...] = 1.0 / jnp.sqrt(c_new)
        s_total = jnp.sum(vec[:, COLS_IN:COLS_IN + LANE], axis=1, keepdims=True)
        r_total = jnp.sum(vec[:, COLS_IN + LANE:COLS_IN + 2 * LANE], axis=1, keepdims=True)
        r_avg = (b2 * r_total + (1.0 - b2) * (s_total / cols_all_in)) / rows_all_in
        root_avg = jnp.sqrt(r_avg)
        row_mean = jnp.sum(row_acc[...] + row_peer[...], axis=1, keepdims=True) / cols_all_in
        row_mean = jnp.broadcast_to(row_mean, (ROWS_IN, LANE))
        r_old = jnp.concatenate([row_to_col(r_in[:, 0:LANE]), row_to_col(pad_lanes(r_in[:, LANE:WIDTH]))[0:PART]], axis=0)
        r_new = b2 * r_old + (1.0 - b2) * row_mean
        r_in_new[:, 0:LANE] = r_new[0:LANE].T[0:1]
        r_in_new[:, LANE:WIDTH] = jnp.concatenate([r_new[LANE:WIDTH], jnp.zeros((96, LANE), F32)], axis=0).T[0:1, 0:PART]
        ai_in[...] = root_avg / jnp.sqrt(r_new)

        def body(i, acc):
            rows = pl.ds(aligned(SUB * i, SUB), SUB)
            a = ai_in[rows]
            for k in range(COLS_IN // LANE):
                col = slice(LANE * k, LANE * k + LANE)
                u = gs_in[rows, col] * a * bj_in[:, col]
                acc = acc + u * u
            return acc

        share_squares(lax.fori_loop(0, ROWS_IN // SUB, body, jnp.zeros((SUB, LANE), F32)), zt_in, pt_in, ct_in)

    def update_in():
        scale = scale_from(ct_in, float(rows_all_in * cols_all_in))
        w_load_in().wait()
        m_load_in().wait()

        def body(i, _):
            rows = pl.ds(aligned(SUB2 * i, SUB2), SUB2)
            a = ai_in[rows] * scale
            for k in range(COLS_IN // LANE):
                col = slice(LANE * k, LANE * k + LANE)
                u = gs_in[rows, col] * a * bj_in[:, col]
                mom = (0.9 * m_in_new[rows, col].astype(F32) + u).astype(BF16)
                m_in_new[rows, col] = mom
                old = win[p, c, rows, col]
                win[p, c, rows, col] = old - lr * mom.astype(F32) - lr * wd * old
            return 0

        lax.fori_loop(0, ROWS_IN // SUB2, body, 0)

    def m_load_in():
        return pltpu.make_async_copy(m_in, m_in_new, load_sem.at[1])

    def block_out(t):
        heads, tails = [], []
        for u in range(QUAD):
            rows = pl.ds(aligned(PART * t + SUB * u, SUB), SUB)
            tail = gs_out[rows, 512:640]
            for k in range(QUAD):
                heads.append(gs_out[rows, LANE * k:LANE * k + LANE])
                tails.append(tail if k == 0 else pltpu.roll(tail, LANE - PART * k, 1))
        tails = jnp.concatenate(tails, axis=0)
        return jnp.concatenate(heads, axis=0), jnp.where(lanes((LANE, LANE)) < PART, tails, 0.0)

    def stats_out_send():
        def body(t, acc):
            head, tail = block_out(t)
            sh = head * head + 1e-30
            st = jnp.where(lanes((LANE, LANE)) < PART, tail * tail + 1e-30, 0.0)
            v_out[0, :, pl.ds(aligned(LANE * t, LANE), LANE)] = jnp.sum((sh + st).T, axis=0, keepdims=True)
            ah, at = acc
            for i in range(SUB2):
                ah = ah + sh[SUB * i:SUB * i + SUB]
                at = at + st[SUB * i:SUB * i + SUB]
            return ah, at

        zero = jnp.zeros((SUB, LANE), F32)
        ah, at = lax.fori_loop(0, TILES_OUT, body, (zero, zero))
        col_acc_out[0:SUB] = ah
        col_acc_out[SUB:SUB2] = at
        col_acc_out[SUB2:SUB2 + SUB] = jnp.broadcast_to(old_lanes(r_out, RAW_OUT), (SUB, LANE))
        copy = z_share(col_acc_out, col_peer_out, 0)
        copy.start()
        copy.wait()
        v_out[0, :, RAW_OUT:RAW_OUT + LANE] = jnp.sum(col_acc_out[0:SUB2] + col_peer_out[0:SUB2], axis=0, keepdims=True)
        vector_send(v_out, vc_out, LEN_OUT)

    def stats_out_norm():
        vector_take(vc_out, vf_out, LEN_OUT)
        vec = vf_out[...]
        r_out_new[...] = b2 * r_out[...] + (1.0 - b2) * (vec[:, 0:RAW_OUT] / cols_all_out)
        s_total = jnp.sum(vec[:, RAW_OUT:RAW_OUT + LANE], axis=1, keepdims=True)
        r_total = jnp.sum((col_acc_out[SUB2:SUB2 + SUB] + col_peer_out[SUB2:SUB2 + SUB])[0:1], axis=1, keepdims=True)
        r_avg = (b2 * r_total + (1.0 - b2) * (s_total / cols_all_out)) / rows_all_out
        root_avg = jnp.sqrt(r_avg)
        cols = col_acc_out[...] + col_peer_out[...]
        c_new_h = b2 * c_out[:, 0:LANE] + (1.0 - b2) * (jnp.sum(cols[0:SUB], axis=0, keepdims=True) / rows_all_out)
        c_new_t = b2 * pad_lanes(c_out[:, LANE:WIDTH]) + (1.0 - b2) * (jnp.sum(cols[SUB:SUB2], axis=0, keepdims=True) / rows_all_out)
        c_out_new[:, 0:LANE] = c_new_h
        c_out_new[:, LANE:WIDTH] = c_new_t[:, 0:PART]
        vec_x[...] = jnp.broadcast_to(1.0 / jnp.sqrt(c_new_h), (SUB, LANE))
        vec_y[...] = jnp.broadcast_to(1.0 / jnp.sqrt(jnp.where(lanes((1, LANE)) < PART, c_new_t, 1.0)), (SUB, LANE))
        bh, bt = vec_x[0:1], vec_y[0:1]

        def body(t, acc):
            rows = pl.ds(aligned(LANE * t, LANE), LANE)
            a = row_to_col(root_avg / jnp.sqrt(r_out_new[:, rows]))
            ai_out[rows] = a
            head, tail = block_out(t)
            uh, ut = head * a * bh, tail * a * bt
            sq = uh * uh + ut * ut
            for i in range(SUB2):
                acc = acc + sq[SUB * i:SUB * i + SUB]
            return acc

        share_squares(lax.fori_loop(0, TILES_OUT, body, jnp.zeros((SUB, LANE), F32)), zt_out, pt_out, ct_out)

    def w_load_out():
        first = 5 * (q // QUAD) + j
        return pltpu.make_async_copy(w_out.at[:, pl.ds(aligned(LANE * first, LANE), 256)], w_cols, load_sem.at[2])

    def m_load_out():
        return pltpu.make_async_copy(m_out, m_out_new, load_sem.at[3])

    def update_out():
        scale = scale_from(ct_out, float(rows_all_out * cols_all_out))
        w_load_out().wait()
        m_load_out().wait()
        bh, bt = vec_x[0:1], vec_y[0:1]
        back = PART * ((QUAD - j) % QUAD)

        def body(t, _):
            rows = pl.ds(aligned(LANE * t, LANE), LANE)
            a = ai_out[rows] * scale
            head, tail = block_out(t)
            uh, ut = head * a * bh, tail * a * bt
            mom = m_out_new[:, rows].astype(F32)
            mh = (0.9 * mom[0:LANE].T + uh).astype(BF16).astype(F32)
            mt = (0.9 * jnp.concatenate([mom[LANE:WIDTH], jnp.zeros((96, LANE), F32)], axis=0).T + ut).astype(BF16).astype(F32)
            m_out_new[0:LANE, rows] = mh.T.astype(BF16)
            m_out_new[LANE:WIDTH, rows] = mt.T[0:PART].astype(BF16)
            lo, hi = w_cols[rows, 0:LANE], w_cols[rows, LANE:256]
            wh = pltpu.roll(jnp.where(lanes((LANE, LANE)) >= PART * j, lo, hi), back, 1)
            wt = pltpu.roll(hi, back, 1)
            wh = wh - lr * mh - lr * wd * wh
            wt = wt - lr * mt - lr * wd * wt
            ln = lanes((SUB, LANE))
            for u in range(QUAD):
                to = pl.ds(aligned(PART * t + SUB * u, SUB), SUB)
                joined = NO
                for k in range(QUAD):
                    at = PART * u + SUB * k
                    wpk[p, c, to, LANE * k:LANE * k + LANE] = wh[at:at + SUB]
                    part = wt[at:at + SUB] if k == 0 else pltpu.roll(wt[at:at + SUB], PART * k, 1)
                    joined = part if joined is NO else jnp.where(ln >= PART * k, part, joined)
                wpk[p, c, to, 512:640] = joined
            return 0

        lax.fori_loop(0, TILES_OUT, body, 0)

    col_acc[...] = jnp.zeros_like(col_acc)
    own_load(0).start()
    own_load(1).start()
    pl.semaphore_wait(barrier, QUAD)
    for k in range(PIECES):
        piece_in(k).start()
    pair_in(1).start()
    reduce_start()

    def at_step(cond, fn, *args):
        @pl.when(cond)
        def _():
            fn(*args)

    n = STEPS

    def step(s, _):
        def within(lo, hi):
            return jnp.logical_and(s >= lo, s < hi)

        at_step(s + 2 < n, start_in, s + 2)
        at_step(within(1, n), reduce_first, 0, win, M_IN, s)
        at_step(within(2, n + 2), reduce_second, 0, win, M_IN, s - 2)
        at_step(within(QUAD, n + QUAD), reduce_third, 0, win, M_IN, s - QUAD, gs_in)

        @pl.when(s == 2)
        def _():
            for copy in vec_loads():
                copy.start()
            m_load_in().start()
            m_load_out().start()
            w_load_out().start()

        @pl.when(s == n - 3)
        def _():
            raw_load(0).start()
            raw_load(1).start()

        at_step(within(n, 2 * n), reduce_first, 1, wpk, M_OUT, s - n)
        at_step(within(n - 1, 2 * n - 1), pack_out, s - n + 1)
        at_step(within(n + 2, 2 * n + 2), reduce_second, 1, wpk, M_OUT, s - n - 2)
        at_step(within(n + QUAD, 2 * n + QUAD), reduce_third, 1, wpk, M_OUT, s - n - QUAD, gs_out)
        at_step(s == n + 3, stats_in_send)
        at_step(s == n + 6, stats_in_norm)
        at_step(s == n + 9, update_in)
        at_step(within(2 * n, 3 * n), gather_first, 0, win, M_IN, s - 2 * n)
        at_step(within(2 * n + 2, 3 * n + 2), gather_second, 0, win, M_IN, s - 2 * n - 2)
        at_step(within(2 * n + QUAD, 3 * n + QUAD), gather_third, 0, win, M_IN, s - 2 * n - QUAD)
        at_step(s == 2 * n + 3, stats_out_send)
        at_step(s == 2 * n + 6, stats_out_norm)
        at_step(s == 2 * n + 9, update_out)
        at_step(within(3 * n, QUAD * n), gather_first, 1, wpk, M_OUT, s - 3 * n)
        at_step(within(3 * n + 2, QUAD * n + 2), gather_second, 1, wpk, M_OUT, s - 3 * n - 2)
        at_step(within(3 * n + QUAD, QUAD * n + QUAD), gather_third, 1, wpk, M_OUT, s - 3 * n - QUAD)
        at_step(within(2 * n + 6, 3 * n + 6), gather_last, 0, win, M_IN, s - 2 * n - 6)
        at_step(within(3 * n + 6, QUAD * n + 6), gather_last, 1, wpk, M_OUT, s - 3 * n - 6)
        return 0

    lax.fori_loop(0, QUAD * n + 6, step, 0)
    pair_out(n - 2).wait_send()
    pair_out(n - 1).wait_send()


def final_kernel(win, wpk, mi, mo, ri, ci, ro, co, win_o, wout_o, mi_o, mo_o, ri_o, ci_o, ro_o, co_o, stage, sem, stage_sem):
    plain = [pltpu.make_async_copy(win, win_o, sem.at[0])]
    for i, (src, dst) in enumerate(((mi, mi_o), (mo, mo_o), (ri, ri_o), (ci, ci_o), (ro, ro_o), (co, co_o))):
        plain.append(pltpu.make_async_copy(src, dst, sem.at[i + 1]))
    for copy in plain:
        copy.start()

    def rows_of(t):
        return pl.ds(aligned(RAW_STEP * t, SUB), RAW_STEP)

    def put(t):
        return pltpu.make_async_copy(stage.at[rows_of(t)], wout_o.at[rows_of(t)], stage_sem.at[t])

    def chunk(t, _):
        def unit(u, _):
            ln = lanes((SUB, LANE))
            rows = pl.ds(aligned(2 * M_OUT * t + SUB * u, SUB), SUB)
            for half in range(2):
                tails = [wpk[2 * half + jj // 2, jj % 2, rows, 512:640] for jj in range(QUAD)]
                for k in range(QUAD):
                    to = pl.ds(aligned(RAW_STEP * t + PART * u + SUB * k, SUB), SUB)
                    heads = []
                    for jj in range(QUAD):
                        head = wpk[2 * half + jj // 2, jj % 2, rows, LANE * k:LANE * k + LANE]
                        heads.append(head if jj == 0 else pltpu.roll(head, PART * jj, 1))
                    ends = [tails[jj] if jj == k else pltpu.roll(tails[jj], (PART * (jj - k)) % LANE, 1) for jj in range(QUAD)]
                    for tile in range(5):
                        if tile == 0:
                            out = heads[0]
                        else:
                            out = ends[tile - 1]
                            if tile > 1:
                                out = jnp.where(ln < PART * (tile - 1), heads[tile - 1], out)
                            if tile < QUAD:
                                out = jnp.where(ln >= PART * tile, heads[tile], out)
                        at = LANE * (5 * half + tile)
                        stage[to, at:at + LANE] = out
            return 0

        lax.fori_loop(0, RAW_STEP // PART, unit, 0)
        put(t).start()
        return 0

    lax.fori_loop(0, STEPS, chunk, 0)
    for t in range(STEPS):
        put(t).wait()
    for copy in plain:
        copy.wait()


def solution(mesh):
    n_tp = mesh.shape['tp']
    n_dp = mesh.shape['dp']
    vmem = pl.BlockSpec(memory_space=pltpu.VMEM)
    hbm = pl.BlockSpec(memory_space=pltpu.HBM)
    smem = pl.BlockSpec(memory_space=pltpu.SMEM)
    dma = pltpu.SemaphoreType.DMA
    kept = (
        ((QUAD, 2, ROWS_IN, COLS_IN), F32),
        ((QUAD, 2, ROWS_OUT, COLS_OUT), F32),
        ((ROWS_IN, COLS_IN), BF16),
        ((WIDTH, RAW_OUT), BF16),
        ((1, ROWS_IN), F32),
        ((1, COLS_IN), F32),
        ((1, RAW_OUT), F32),
        ((1, WIDTH), F32),
    )
    main = pl.pallas_call(
        functools.partial(main_kernel, n_tp, n_dp, D, COLS_IN * n_tp, RAW_OUT * n_tp, D),
        out_shape=[pltpu.VMEM(shape, dtype) for shape, dtype in kept],
        in_specs=[hbm] * 6 + [hbm] * QUAD + [smem] * 3,
        out_specs=[vmem] * SUB,
        scratch_shapes=[
            pltpu.VMEM((3, 2, 2, 2 * M_IN, COLS_IN), F32),
            pltpu.VMEM((2, RAW_STEP, D), F32),
            pltpu.VMEM((2, 2, 2, 2, 2 * M_OUT, COLS_OUT), F32),
            pltpu.VMEM((ROWS_IN, COLS_IN), F32),
            pltpu.VMEM((ROWS_OUT, COLS_OUT), F32),
            pltpu.VMEM((RAW_OUT, 256), F32),
            pltpu.VMEM((RAW_OUT, LANE), F32),
            pltpu.VMEM((ROWS_IN, LANE), F32),
            pltpu.VMEM((1, COLS_IN), F32),
            pltpu.VMEM((SUB, LANE), F32),
            pltpu.VMEM((SUB, LANE), F32),
            pltpu.VMEM((SUB, COLS_IN), F32),
            pltpu.VMEM((ROWS_IN, LANE), F32),
            pltpu.VMEM((ROWS_IN, LANE), F32),
            pltpu.VMEM((SUB2 + SUB, LANE), F32),
            pltpu.VMEM((SUB2 + SUB, LANE), F32),
            pltpu.VMEM((2, 1, LEN_IN), F32),
            pltpu.VMEM((QUAD, 1, LEN_IN // 2), F32),
            pltpu.VMEM((1, LEN_IN), F32),
            pltpu.VMEM((2, 1, LEN_OUT), F32),
            pltpu.VMEM((QUAD, 1, LEN_OUT // 2), F32),
            pltpu.VMEM((1, LEN_OUT), F32),
            pltpu.VMEM((1, ROWS_IN), F32),
            pltpu.VMEM((1, COLS_IN), F32),
            pltpu.VMEM((1, RAW_OUT), F32),
            pltpu.VMEM((1, WIDTH), F32),
        ] + [pltpu.VMEM((i, 1, LANE), F32) for i in (2, 2, QUAD)] * 2 + [
            dma((N_RED, SLOTS)),
            dma((N_GAT, SLOTS)),
            dma((PAIR_SLOTS,)),
            dma((2 * QUAD + PIECES,)),
            dma((2, N_EX)),
        ],
        compiler_params=pltpu.CompilerParams(collective_id=0, has_side_effects=True, vmem_limit_bytes=GRANT),
    )
    final = pl.pallas_call(
        final_kernel,
        out_shape=[
            jax.ShapeDtypeStruct((QUAD, 2, ROWS_IN, COLS_IN), F32),
            jax.ShapeDtypeStruct((RAW_OUT, D), F32),
        ] + [jax.ShapeDtypeStruct(shape, dtype) for shape, dtype in kept[2:]],
        in_specs=[vmem] * SUB,
        out_specs=[hbm] * SUB,
        scratch_shapes=[pltpu.VMEM((RAW_OUT, D), F32), dma((7,)), dma((STEPS,))],
        compiler_params=pltpu.CompilerParams(vmem_limit_bytes=GRANT),
    )

    def body(w_in, w_out, g_in, g_out, m_in, m_out, r_in, c_in, r_out, c_out, learn_rate, weight_decay, beta_two):
        shards = (QUAD, 2, ROWS_IN, COLS_IN)
        got = main(
            w_in.reshape(shards), w_out[0], g_in.reshape((2, 2, 2, ROWS_IN, COLS_IN)), g_out[0, 0], m_in[0], m_out[0].T,
            r_in, c_in, r_out, c_out, learn_rate.reshape(1), weight_decay.reshape(1), beta_two.reshape(1))
        w_i, w_o, m_i, m_o, r_i, c_i, r_o, c_o = final(*[pltpu.with_memory_space_constraint(g, pltpu.VMEM) for g in got])
        return w_i.reshape((1, D, COLS_IN)), w_o[NO], m_i[NO], m_o.T[NO], r_i, c_i, r_o, c_o

    in_specs = (P(NO, NO, 'tp'), P(NO, 'tp', NO), P('dp', NO, NO, 'tp'), P('dp', NO, 'tp', NO), P(NO, 'dp', 'tp'), P(NO, 'tp', 'dp'), P(NO, 'dp'), P(NO, 'tp'), P(NO, 'tp'), P(NO, 'dp'), P(), P(), P())
    out_specs = (P(NO, NO, 'tp'), P(NO, 'tp', NO), P(NO, 'dp', 'tp'), P(NO, 'tp', 'dp'), P(NO, 'dp'), P(NO, 'tp'), P(NO, 'tp'), P(NO, 'dp'))
    return jax.shard_map(body, mesh=mesh, in_specs=in_specs, out_specs=out_specs, check_vma=False)
```

```python
import functools

import jax
import jax.numpy as jnp
from jax import lax
from jax.experimental import pallas as pl
from jax.experimental.pallas import tpu as pltpu
from jax.sharding import PartitionSpec as P

F32 = jnp.float32
BF16 = jnp.bfloat16
MESH = pl.DeviceIdType.MESH
LANE, SUB, SUB2, PART, QUAD, WIDTH = 128, 8, 16, 32, 4, 160
NO = None
BOTH, THREE = pl.ds(0, 2), pl.ds(0, 3)

D = 1280
ROWS_IN, COLS_IN = WIDTH, 4480
ROWS_OUT, COLS_OUT = 800, 640
RAW_OUT = 3200
STEPS = 10
M_IN = ROWS_IN // STEPS // 2
M_OUT = ROWS_OUT // STEPS // 2
RAW_STEP = RAW_OUT // STEPS
TILES_OUT = RAW_OUT // LANE

GRANT = 24 << 20

SLOTS, PAIR_SLOTS = 6, 10
N_RED, N_GAT, N_EX = 6, 4, 8
(OWN, DSS, DSR, SENT, R1, R2) = range(N_RED)
(S1, S2, R_OWN, R_ON) = range(N_GAT)
(ZS, ZR, CS, CR, TS, TR, BS, BR) = range(N_EX)
PIECES, PIECE = 7, COLS_IN // 7
LEN_IN, LEN_OUT = COLS_IN + LANE, RAW_OUT + LANE

def lanes(shape):
    return lax.broadcasted_iota(jnp.int32, shape, 1)


def aligned(value, by):
    return pl.multiple_of(value, by)


def pad_lanes(row):
    return jnp.concatenate([row, jnp.zeros((1, LANE - row.shape[1]), F32)], axis=1)


def row_to_col(row):
    return jnp.broadcast_to(row, (LANE, LANE)).T


def main_kernel(n_tp, n_dp, rows_all_in, cols_all_in, rows_all_out, cols_all_out,
                w_in, w_out, g_in, g_out, m_in, m_out, r_in_hbm, c_in_hbm, r_out_hbm, c_out_hbm, lr_ref, wd_ref, b2_ref,
                win, wpk, m_in_new, m_out_new, r_in_new, c_in_new, r_out_new, c_out_new,
                own_in, raw, packed, gs_in, gs_out, w_cols, ai_out, ai_in, bj_in, vec_x, vec_y,
                col_acc, row_acc, row_peer, col_acc_out, col_peer_out, v_in, vc_in, vf_in, v_out, vc_out, vf_out,
                r_in, c_in, r_out, c_out, zr, zt_in, pt_in, ct_in, zt_out, pt_out, ct_out,
                red_sem, gat_sem, pair_sem, load_sem, ex_sem):
    tp = lax.axis_index('tp')
    q = lax.axis_index('dp')
    p, c = q // 2, q % 2
    y, x = p // 2, p % 2
    nx, ny, nc = 1 - x, 1 - y, 1 - c
    p_x, p_y, p_d = 2 * y + nx, 2 * ny + x, 2 * ny + nx
    to_x = {'dp': 2 * p_x + c}
    to_y = {'dp': 2 * p_y + c}
    to_d = {'dp': 2 * p_d + c}
    to_core = {'dp': 2 * p + nc}
    to_z = {'tp': 1 - tp}
    j = q % QUAD
    lr, wd, b2 = lr_ref[0], wd_ref[0], b2_ref[0]

    barrier = pltpu.get_barrier_semaphore()
    for dev in (to_x, to_y, to_core, to_z):
        pl.semaphore_signal(barrier, inc=1, device_id=dev, device_id_type=MESH)

    def rcopy(src, dst, send, recv, dev):
        return pltpu.make_async_remote_copy(src_ref=src, dst_ref=dst, send_sem=send, recv_sem=recv, device_id=dev, device_id_type=MESH)

    def slot_of(ph, t):
        return lax.rem(ph * STEPS + t, SLOTS)

    def spans(m, t):
        base = aligned(2 * m * t, SUB)
        return pl.ds(base, 2 * m), pl.ds(base, m), pl.ds(aligned(base + m, SUB), m)

    def first_copies(ph, w, m, t):
        _, ra, rb = spans(m, t)
        a = rcopy(w.at[BOTH, nx, ra], w.at[2, BOTH, ra], red_sem.at[SENT, slot_of(ph, t)], red_sem.at[R1, slot_of(ph, t)], to_x)
        b = rcopy(w.at[ny, BOTH, rb], w.at[2, BOTH, rb], red_sem.at[SENT, slot_of(ph, t)], red_sem.at[R1, slot_of(ph, t)], to_y)
        return a, b

    def second_copies(ph, w, m, t):
        _, ra, rb = spans(m, t)
        a = rcopy(w.at[ny, x, ra], w.at[3, 0, ra], red_sem.at[SENT, slot_of(ph, t)], red_sem.at[R2, slot_of(ph, t)], to_y)
        b = rcopy(w.at[y, nx, rb], w.at[3, 0, rb], red_sem.at[SENT, slot_of(ph, t)], red_sem.at[R2, slot_of(ph, t)], to_x)
        return a, b

    def wait_first(ph, w, m, t):
        rr, _, _ = spans(m, t)
        part = w.at[2, BOTH, rr]
        rcopy(part, part, red_sem.at[SENT, slot_of(ph, t)], red_sem.at[R1, slot_of(ph, t)], to_x).wait_recv()

    def wait_second(ph, w, m, t):
        rr, _, _ = spans(m, t)
        part = w.at[3, 0, rr]
        rcopy(part, part, red_sem.at[SENT, slot_of(ph, t)], red_sem.at[R2, slot_of(ph, t)], to_y).wait_recv()

    def wait_sent(ph, w, m, t):
        rr, _, _ = spans(m, t)
        part = w.at[THREE, 0, rr]
        rcopy(part, part, red_sem.at[SENT, slot_of(ph, t)], red_sem.at[R1, slot_of(ph, t)], to_x).wait_send()

    def pair_in(t):
        rr, _, _ = spans(M_IN, t)
        return rcopy(g_in.at[:, :, nc, rr], win.at[BOTH, :, rr], red_sem.at[DSS, slot_of(0, t)], red_sem.at[DSR, slot_of(0, t)], to_core)

    def piece_in(k):
        rows, cols = pl.ds(0, 2 * M_IN), pl.ds(PIECE * k, PIECE)
        return rcopy(g_in.at[:, :, nc, rows, cols], win.at[BOTH, :, rows, cols], red_sem.at[DSS, 0], load_sem.at[2 * QUAD + k], to_core)

    def reduce_start():
        own_load(0).wait()
        for k in range(PIECES):
            cols = pl.ds(PIECE * k, PIECE)
            piece_in(k).wait_recv()
            for yy in range(2):
                for xx in range(2):
                    win[yy, xx, 0:2 * M_IN, cols] = win[yy, xx, 0:2 * M_IN, cols] + own_in[0, yy, xx, :, cols]
            ra, rb = pl.ds(0, M_IN), pl.ds(M_IN, M_IN)
            rcopy(win.at[BOTH, nx, ra, cols], win.at[2, BOTH, ra, cols], red_sem.at[SENT, 0], red_sem.at[R1, 0], to_x).start()
            rcopy(win.at[ny, BOTH, rb, cols], win.at[2, BOTH, rb, cols], red_sem.at[SENT, 0], red_sem.at[R1, 0], to_y).start()

    def own_load(t):
        rr, _, _ = spans(M_IN, t)
        return pltpu.make_async_copy(g_in.at[:, :, c, rr], own_in.at[lax.rem(t, 3)], red_sem.at[OWN, slot_of(0, t)])

    def raw_load(t):
        return pltpu.make_async_copy(g_out.at[pl.ds(aligned(RAW_STEP * t, SUB), RAW_STEP)], raw.at[lax.rem(t, 2)], red_sem.at[OWN, slot_of(1, t)])

    def pair_out(t):
        rr, _, _ = spans(M_OUT, t)
        return rcopy(packed.at[lax.rem(t, 2), :, :, nc], wpk.at[BOTH, :, rr], red_sem.at[DSS, slot_of(1, t)], red_sem.at[DSR, slot_of(1, t)], to_core)

    def start_in(t):
        own_load(t).start()
        pair_in(t).start()

    def pack_out(t):
        raw_load(t).wait()
        slot = lax.rem(t, 2)

        @pl.when(t >= 2)
        def _():
            pair_out(t - 2).wait_send()

        def unit(u, _):
            base = aligned(PART * u, SUB)
            tiles = [[raw[slot, pl.ds(base + SUB * k, SUB), LANE * i:LANE * i + LANE] for i in range(10)] for k in range(QUAD)]
            ln = lanes((SUB, LANE))
            for s in range(SUB):
                jj, first = s % QUAD, 5 * (s // QUAD) + s % QUAD
                tail = NO
                for k in range(QUAD):
                    lo, hi = tiles[k][first], tiles[k][first + 1]
                    head = lo if jj == 0 else pltpu.roll(jnp.where(ln >= PART * jj, lo, hi), LANE - PART * jj, 1)
                    packed[slot, s // QUAD, (s // 2) % 2, s % 2, pl.ds(aligned(SUB * u, SUB), SUB), LANE * k:LANE * k + LANE] = head
                    turn = (PART * (k - jj)) % LANE
                    part = hi if turn == 0 else pltpu.roll(hi, turn, 1)
                    tail = part if tail is NO else jnp.where(ln >= PART * k, part, tail)
                packed[slot, s // QUAD, (s // 2) % 2, s % 2, pl.ds(aligned(SUB * u, SUB), SUB), 512:640] = tail
            return 0

        lax.fori_loop(0, RAW_STEP // PART, unit, 0)
        pair_out(t).start()

        @pl.when(t + 2 < STEPS)
        def _():
            raw_load(t + 2).start()

    def reduce_first(ph, w, m, t):
        rr, _, _ = spans(m, t)
        if ph == 0:
            own_load(t).wait()
            pair_in(t).wait_recv()
            slot = lax.rem(t, 3)
            for yy in range(2):
                for xx in range(2):
                    for r in range(0, 2 * m, SUB):
                        rows = pl.ds(aligned(2 * m * t + r, SUB), SUB)
                        w[yy, xx, rows] = w[yy, xx, rows] + own_in[slot, yy, xx, r:r + SUB]
        else:
            pair_out(t).wait_recv()
            slot = lax.rem(t, 2)

            def add(i, _):
                rows = pl.ds(aligned(2 * m * t + SUB2 * i, SUB), SUB2)
                for yy in range(2):
                    for xx in range(2):
                        w[yy, xx, rows] = w[yy, xx, rows] + packed[slot, yy, xx, c, pl.ds(aligned(SUB2 * i, SUB), SUB2)]
                return 0

            lax.fori_loop(0, 2 * m // SUB2, add, 0)
        for copy in first_copies(ph, w, m, t):
            copy.start()

    def reduce_second(ph, w, m, t):
        _, ra, rb = spans(m, t)
        on_y, on_x = second_copies(ph, w, m, t)
        if ph == 0:
            pair_in(t).wait_send()
        wait_first(ph, w, m, t)
        w[ny, x, ra] = w[ny, x, ra] + w[2, ny, ra]
        on_y.start()
        w[y, nx, rb] = w[y, nx, rb] + w[2, nx, rb]
        on_x.start()

    def reduce_third(ph, w, m, t, gs):
        _, ra, rb = spans(m, t)
        wait_second(ph, w, m, t)
        ga = w[y, x, ra] + w[2, y, ra] + w[3, 0, ra]
        gs[ra] = ga
        gb = w[y, x, rb] + w[2, x, rb] + w[3, 0, rb]
        gs[rb] = gb
        wait_sent(ph, w, m, t)
        if ph == 0:
            sa, sb = ga * ga + 1e-30, gb * gb + 1e-30
            col_acc[...] = col_acc[...] + (sa + sb)
            for rows, sq in ((ra, sa), (rb, sb)):
                part = sq[:, 0:LANE]
                for i in range(1, COLS_IN // LANE):
                    part = part + sq[:, LANE * i:LANE * i + LANE]
                row_acc[rows] = part

    def sems(ph, t, send, recv):
        return gat_sem.at[send, slot_of(ph, t)], gat_sem.at[recv, slot_of(ph, t)]

    def pair_sems(ph, t, send):
        return gat_sem.at[send, slot_of(ph, t)], pair_sem.at[lax.rem(ph * STEPS + t, PAIR_SLOTS)]

    def gather_first(ph, w, m, t):
        rr, _, _ = spans(m, t)
        src = w.at[p, c, rr]
        rcopy(src, src, *sems(ph, t, S1, R_OWN), to_x).start()
        rcopy(src, src, *sems(ph, t, S1, R_OWN), to_y).start()
        rcopy(src, src, *pair_sems(ph, t, S1), to_core).start()

    def gather_second(ph, w, m, t):
        rr, ra, rb = spans(m, t)
        both = w.at[BOTH, c, rr]
        rcopy(both, both, *sems(ph, t, S1, R_OWN), to_x).wait_recv()
        for other, rows, dev in ((p_x, rb, to_y), (p_y, ra, to_x)):
            rcopy(w.at[other, c, rows], w.at[other, c, rows], *sems(ph, t, S2, R_ON), dev).start()
            rcopy(w.at[other, c, rr], w.at[other, c, rr], *pair_sems(ph, t, S2), to_core).start()

    def gather_third(ph, w, m, t):
        rr, _, _ = spans(m, t)
        diag = w.at[p_d, c, rr]
        rcopy(diag, diag, *sems(ph, t, S2, R_ON), to_x).wait_recv()
        rcopy(diag, diag, *pair_sems(ph, t, S2), to_core).start()
        three = w.at[THREE, c, rr]
        rcopy(three, three, *sems(ph, t, S1, R_OWN), to_x).wait_send()

    def gather_last(ph, w, m, t):
        rr, _, _ = spans(m, t)
        four = w.at[:, nc, rr]
        rcopy(four, four, *pair_sems(ph, t, S2), to_core).wait_recv()
        rcopy(four, four, *pair_sems(ph, t, S2), to_core).wait_send()

    def z_share(src, dst, k):
        return rcopy(src, dst, ex_sem.at[k, ZS], ex_sem.at[k, ZR], to_z)

    def share(buf, k):
        copy = rcopy(buf.at[0], buf.at[1], ex_sem.at[k, CS], ex_sem.at[k, CR], to_core)
        copy.start()
        copy.wait()
        return buf[0] + buf[1]

    def to_chips(buf, k):
        for dev in (to_x, to_y, to_d):
            rcopy(buf.at[p], buf.at[p], ex_sem.at[k, TS], ex_sem.at[k, TR], dev).start()

    def from_chips(buf, k):
        three = buf.at[THREE]
        rcopy(three, three, ex_sem.at[k, TS], ex_sem.at[k, TR], to_x).wait()
        return buf[0] + buf[1] + buf[2] + buf[3]

    def halves(length):
        half = length // 2
        return pl.ds(aligned(c * half, LANE), half), pl.ds(aligned(nc * half, LANE), half)

    def vector_send(buf, chips, length):
        mine, other = halves(length)
        copy = rcopy(buf.at[0, :, other], buf.at[1, :, other], ex_sem.at[0, CS], ex_sem.at[0, CR], to_core)
        copy.start()
        copy.wait()
        chips[p] = buf[0, :, mine] + buf[1, :, mine]
        to_chips(chips, 0)

    def vector_take(chips, whole, length):
        mine, _ = halves(length)
        whole[:, mine] = from_chips(chips, 0)
        copy = rcopy(whole.at[:, mine], whole.at[:, mine], ex_sem.at[0, BS], ex_sem.at[0, BR], to_core)
        copy.start()
        copy.wait()

    def share_squares(acc, zt, pt, ct):
        zt[0] = jnp.sum(acc, axis=0, keepdims=True)
        copy = z_share(zt.at[0], zt.at[1], 1)
        copy.start()
        copy.wait()
        pt[0] = zt[0] + zt[1]
        ct[p] = share(pt, 1)
        to_chips(ct, 1)

    def scale_from(ct, count):
        mean = jnp.sum(from_chips(ct, 1), axis=1, keepdims=True) / count
        return 0.1 / jnp.maximum(1.0, jnp.sqrt(mean))

    def vec_loads():
        pairs = ((r_in_hbm, r_in), (c_in_hbm, c_in), (r_out_hbm, r_out), (c_out_hbm, c_out))
        return [pltpu.make_async_copy(src, dst, load_sem.at[QUAD + i]) for i, (src, dst) in enumerate(pairs)]

    def stats_in_send():
        for load in vec_loads():
            load.wait()
        copy = z_share(row_acc, row_peer, 0)
        copy.start()
        v_in[0, :, 0:COLS_IN] = jnp.sum(col_acc[...], axis=0, keepdims=True)
        copy.wait()
        row_mean = jnp.sum(row_acc[...] + row_peer[...], axis=1, keepdims=True) / cols_all_in
        row_mean = jnp.broadcast_to(row_mean, (ROWS_IN, LANE))
        r_old = jnp.concatenate([row_to_col(r_in[:, 0:LANE]), row_to_col(pad_lanes(r_in[:, LANE:WIDTH]))[0:PART]], axis=0)
        r_new = b2 * r_old + (1.0 - b2) * row_mean
        r_in_new[:, 0:LANE] = r_new[0:LANE].T[0:1]
        r_in_new[:, LANE:WIDTH] = jnp.concatenate([r_new[LANE:WIDTH], jnp.zeros((LANE - PART, LANE), F32)], axis=0).T[0:1, 0:PART]
        ai_in[...] = r_new
        v_in[0, :, COLS_IN:LEN_IN] = jnp.sum(r_new, axis=0, keepdims=True)
        vector_send(v_in, vc_in, LEN_IN)
        w_load_in().start()

    def w_load_in():
        return pltpu.make_async_copy(w_in.at[p, c], win.at[p, c], load_sem.at[0])

    def stats_in_norm():
        vector_take(vc_in, vf_in, LEN_IN)
        vec = vf_in[...]
        c_new = b2 * c_in[...] + (1.0 - b2) * (vec[:, 0:COLS_IN] / rows_all_in)
        c_in_new[...] = c_new
        bj_in[...] = 1.0 / jnp.sqrt(c_new)
        root_avg = jnp.sqrt(vec[:, COLS_IN:COLS_IN + 1] / rows_all_in)
        ai_in[...] = root_avg / jnp.sqrt(ai_in[...])

        def body(i, acc):
            rows = pl.ds(aligned(SUB * i, SUB), SUB)
            a = ai_in[rows]
            for k in range(COLS_IN // LANE):
                col = slice(LANE * k, LANE * k + LANE)
                u = gs_in[rows, col] * a * bj_in[:, col]
                acc = acc + u * u
            return acc

        share_squares(lax.fori_loop(0, ROWS_IN // SUB, body, jnp.zeros((SUB, LANE), F32)), zt_in, pt_in, ct_in)

    def update_in():
        scale = scale_from(ct_in, float(rows_all_in * cols_all_in))
        w_load_in().wait()
        m_load_in().wait()

        def body(i, _):
            rows = pl.ds(aligned(SUB2 * i, SUB2), SUB2)
            a = ai_in[rows] * scale
            for k in range(COLS_IN // LANE):
                col = slice(LANE * k, LANE * k + LANE)
                u = gs_in[rows, col] * a * bj_in[:, col]
                mom = (0.9 * m_in_new[rows, col].astype(F32) + u).astype(BF16)
                m_in_new[rows, col] = mom
                old = win[p, c, rows, col]
                win[p, c, rows, col] = old - lr * mom.astype(F32) - lr * wd * old
            return 0

        lax.fori_loop(0, ROWS_IN // SUB2, body, 0)

    def m_load_in():
        return pltpu.make_async_copy(m_in, m_in_new, load_sem.at[1])

    def block_out(t):
        heads, tails = [], []
        for u in range(QUAD):
            rows = pl.ds(aligned(PART * t + SUB * u, SUB), SUB)
            tail = gs_out[rows, 512:640]
            for k in range(QUAD):
                heads.append(gs_out[rows, LANE * k:LANE * k + LANE])
                tails.append(tail if k == 0 else pltpu.roll(tail, LANE - PART * k, 1))
        tails = jnp.concatenate(tails, axis=0)
        return jnp.concatenate(heads, axis=0), jnp.where(lanes((LANE, LANE)) < PART, tails, 0.0)

    def stats_out_send():
        def body(t, acc):
            head, tail = block_out(t)
            sh = head * head + 1e-30
            st = jnp.where(lanes((LANE, LANE)) < PART, tail * tail + 1e-30, 0.0)
            v_out[0, :, pl.ds(aligned(LANE * t, LANE), LANE)] = jnp.sum((sh + st).T, axis=0, keepdims=True)
            ah, at = acc
            for i in range(SUB2):
                ah = ah + sh[SUB * i:SUB * i + SUB]
                at = at + st[SUB * i:SUB * i + SUB]
            return ah, at

        zero = jnp.zeros((SUB, LANE), F32)
        ah, at = lax.fori_loop(0, TILES_OUT, body, (zero, zero))
        col_acc_out[0:SUB] = ah
        col_acc_out[SUB:SUB2] = at
        copy = z_share(col_acc_out, col_peer_out, 0)
        copy.start()
        copy.wait()
        v_out[0, :, RAW_OUT:LEN_OUT] = jnp.zeros((1, LANE), F32)
        vector_send(v_out, vc_out, LEN_OUT)

    def stats_out_norm():
        vector_take(vc_out, vf_out, LEN_OUT)
        vec = vf_out[...]
        r_new = b2 * r_out[...] + (1.0 - b2) * (vec[:, 0:RAW_OUT] / cols_all_out)
        r_out_new[...] = r_new
        part = r_new[:, 0:LANE]
        for i in range(1, TILES_OUT):
            part = part + r_new[:, LANE * i:LANE * i + LANE]
        zr[0] = part
        copy = rcopy(zr.at[0], zr.at[1], ex_sem.at[1, BS], ex_sem.at[1, BR], to_z)
        copy.start()
        copy.wait()
        root_avg = jnp.sqrt(jnp.sum(zr[0] + zr[1], axis=1, keepdims=True) / rows_all_out)
        cols = col_acc_out[...] + col_peer_out[...]
        c_new_h = b2 * c_out[:, 0:LANE] + (1.0 - b2) * (jnp.sum(cols[0:SUB], axis=0, keepdims=True) / rows_all_out)
        c_new_t = b2 * pad_lanes(c_out[:, LANE:WIDTH]) + (1.0 - b2) * (jnp.sum(cols[SUB:SUB2], axis=0, keepdims=True) / rows_all_out)
        c_out_new[:, 0:LANE] = c_new_h
        c_out_new[:, LANE:WIDTH] = c_new_t[:, 0:PART]
        vec_x[...] = jnp.broadcast_to(1.0 / jnp.sqrt(c_new_h), (SUB, LANE))
        vec_y[...] = jnp.broadcast_to(1.0 / jnp.sqrt(jnp.where(lanes((1, LANE)) < PART, c_new_t, 1.0)), (SUB, LANE))
        bh, bt = vec_x[0:1], vec_y[0:1]

        def body(t, acc):
            rows = pl.ds(aligned(LANE * t, LANE), LANE)
            a = row_to_col(root_avg / jnp.sqrt(r_out_new[:, rows]))
            ai_out[rows] = a
            head, tail = block_out(t)
            uh, ut = head * a * bh, tail * a * bt
            sq = uh * uh + ut * ut
            for i in range(SUB2):
                acc = acc + sq[SUB * i:SUB * i + SUB]
            return acc

        share_squares(lax.fori_loop(0, TILES_OUT, body, jnp.zeros((SUB, LANE), F32)), zt_out, pt_out, ct_out)

    def w_load_out():
        first = 5 * (q // QUAD) + j
        return pltpu.make_async_copy(w_out.at[:, pl.ds(aligned(LANE * first, LANE), 256)], w_cols, load_sem.at[2])

    def m_load_out():
        return pltpu.make_async_copy(m_out, m_out_new, load_sem.at[3])

    def update_out():
        scale = scale_from(ct_out, float(rows_all_out * cols_all_out))
        w_load_out().wait()
        m_load_out().wait()
        bh, bt = vec_x[0:1], vec_y[0:1]
        back = PART * ((QUAD - j) % QUAD)

        def body(t, _):
            rows = pl.ds(aligned(LANE * t, LANE), LANE)
            a = ai_out[rows] * scale
            head, tail = block_out(t)
            uh, ut = head * a * bh, tail * a * bt
            mom = m_out_new[:, rows].astype(F32)
            mh = (0.9 * mom[0:LANE].T + uh).astype(BF16).astype(F32)
            mt = (0.9 * jnp.concatenate([mom[LANE:WIDTH], jnp.zeros((96, LANE), F32)], axis=0).T + ut).astype(BF16).astype(F32)
            m_out_new[0:LANE, rows] = mh.T.astype(BF16)
            m_out_new[LANE:WIDTH, rows] = mt.T[0:PART].astype(BF16)
            lo, hi = w_cols[rows, 0:LANE], w_cols[rows, LANE:256]
            wh = pltpu.roll(jnp.where(lanes((LANE, LANE)) >= PART * j, lo, hi), back, 1)
            wt = pltpu.roll(hi, back, 1)
            wh = wh - lr * mh - lr * wd * wh
            wt = wt - lr * mt - lr * wd * wt
            ln = lanes((SUB, LANE))
            for u in range(QUAD):
                to = pl.ds(aligned(PART * t + SUB * u, SUB), SUB)
                joined = NO
                for k in range(QUAD):
                    at = PART * u + SUB * k
                    wpk[p, c, to, LANE * k:LANE * k + LANE] = wh[at:at + SUB]
                    part = wt[at:at + SUB] if k == 0 else pltpu.roll(wt[at:at + SUB], PART * k, 1)
                    joined = part if joined is NO else jnp.where(ln >= PART * k, part, joined)
                wpk[p, c, to, 512:640] = joined
            return 0

        lax.fori_loop(0, TILES_OUT, body, 0)

    col_acc[...] = jnp.zeros_like(col_acc)
    own_load(0).start()
    own_load(1).start()
    pl.semaphore_wait(barrier, QUAD)
    for k in range(PIECES):
        piece_in(k).start()
    pair_in(1).start()
    reduce_start()

    def at_step(cond, fn, *args):
        @pl.when(cond)
        def _():
            fn(*args)

    n = STEPS

    def step(s, _):
        def within(lo, hi):
            return jnp.logical_and(s >= lo, s < hi)

        at_step(s + 2 < n, start_in, s + 2)
        at_step(within(1, n), reduce_first, 0, win, M_IN, s)
        at_step(within(2, n + 2), reduce_second, 0, win, M_IN, s - 2)
        at_step(within(QUAD, n + QUAD), reduce_third, 0, win, M_IN, s - QUAD, gs_in)

        @pl.when(s == 2)
        def _():
            for copy in vec_loads():
                copy.start()
            m_load_in().start()
            m_load_out().start()
            w_load_out().start()

        @pl.when(s == n - 3)
        def _():
            raw_load(0).start()
            raw_load(1).start()

        at_step(within(n, 2 * n), reduce_first, 1, wpk, M_OUT, s - n)
        at_step(within(n - 1, 2 * n - 1), pack_out, s - n + 1)
        at_step(within(n + 2, 2 * n + 2), reduce_second, 1, wpk, M_OUT, s - n - 2)
        at_step(within(n + QUAD, 2 * n + QUAD), reduce_third, 1, wpk, M_OUT, s - n - QUAD, gs_out)
        at_step(s == n + 3, stats_in_send)
        at_step(s == n + 6, stats_in_norm)
        at_step(s == n + 9, update_in)
        at_step(within(2 * n, 3 * n), gather_first, 0, win, M_IN, s - 2 * n)
        at_step(within(2 * n + 2, 3 * n + 2), gather_second, 0, win, M_IN, s - 2 * n - 2)
        at_step(within(2 * n + QUAD, 3 * n + QUAD), gather_third, 0, win, M_IN, s - 2 * n - QUAD)
        at_step(s == 2 * n + 3, stats_out_send)
        at_step(s == 2 * n + 6, stats_out_norm)
        at_step(s == 2 * n + 9, update_out)
        at_step(within(3 * n, QUAD * n), gather_first, 1, wpk, M_OUT, s - 3 * n)
        at_step(within(3 * n + 2, QUAD * n + 2), gather_second, 1, wpk, M_OUT, s - 3 * n - 2)
        at_step(within(3 * n + QUAD, QUAD * n + QUAD), gather_third, 1, wpk, M_OUT, s - 3 * n - QUAD)
        at_step(within(2 * n + 6, 3 * n + 6), gather_last, 0, win, M_IN, s - 2 * n - 6)
        at_step(within(3 * n + 6, QUAD * n + 6), gather_last, 1, wpk, M_OUT, s - 3 * n - 6)
        return 0

    lax.fori_loop(0, QUAD * n + 6, step, 0)
    pair_out(n - 2).wait_send()
    pair_out(n - 1).wait_send()


def final_kernel(win, wpk, mi, mo, ri, ci, ro, co, win_o, wout_o, mi_o, mo_o, ri_o, ci_o, ro_o, co_o, stage, sem, stage_sem):
    plain = [pltpu.make_async_copy(win.at[i // 2, i % 2], win_o.at[i // 2, i % 2], sem.at[i]) for i in range(SUB)]
    for i, (src, dst) in enumerate(((mi, mi_o), (mo, mo_o), (ri, ri_o), (ci, ci_o), (ro, ro_o), (co, co_o))):
        plain.append(pltpu.make_async_copy(src, dst, sem.at[SUB + i]))
    for copy in plain:
        copy.start()

    def rows_of(t):
        return pl.ds(aligned(RAW_STEP * t, SUB), RAW_STEP)

    def put(t):
        return pltpu.make_async_copy(stage.at[rows_of(t)], wout_o.at[rows_of(t)], stage_sem.at[t])

    def chunk(t, _):
        def unit(u, _):
            ln = lanes((SUB, LANE))
            rows = pl.ds(aligned(2 * M_OUT * t + SUB * u, SUB), SUB)
            for half in range(2):
                tails = [wpk[2 * half + jj // 2, jj % 2, rows, 512:640] for jj in range(QUAD)]
                for k in range(QUAD):
                    to = pl.ds(aligned(RAW_STEP * t + PART * u + SUB * k, SUB), SUB)
                    heads = []
                    for jj in range(QUAD):
                        head = wpk[2 * half + jj // 2, jj % 2, rows, LANE * k:LANE * k + LANE]
                        heads.append(head if jj == 0 else pltpu.roll(head, PART * jj, 1))
                    ends = [tails[jj] if jj == k else pltpu.roll(tails[jj], (PART * (jj - k)) % LANE, 1) for jj in range(QUAD)]
                    for tile in range(5):
                        if tile == 0:
                            out = heads[0]
                        else:
                            out = ends[tile - 1]
                            if tile > 1:
                                out = jnp.where(ln < PART * (tile - 1), heads[tile - 1], out)
                            if tile < QUAD:
                                out = jnp.where(ln >= PART * tile, heads[tile], out)
                        at = LANE * (5 * half + tile)
                        stage[to, at:at + LANE] = out
            return 0

        lax.fori_loop(0, RAW_STEP // PART, unit, 0)
        put(t).start()
        return 0

    lax.fori_loop(0, STEPS, chunk, 0)
    for t in range(STEPS):
        put(t).wait()
    for copy in plain:
        copy.wait()


def solution(mesh):
    n_tp = mesh.shape['tp']
    n_dp = mesh.shape['dp']
    vmem = pl.BlockSpec(memory_space=pltpu.VMEM)
    hbm = pl.BlockSpec(memory_space=pltpu.HBM)
    smem = pl.BlockSpec(memory_space=pltpu.SMEM)
    dma = pltpu.SemaphoreType.DMA
    kept = (
        ((QUAD, 2, ROWS_IN, COLS_IN), F32),
        ((QUAD, 2, ROWS_OUT, COLS_OUT), F32),
        ((ROWS_IN, COLS_IN), BF16),
        ((WIDTH, RAW_OUT), BF16),
        ((1, ROWS_IN), F32),
        ((1, COLS_IN), F32),
        ((1, RAW_OUT), F32),
        ((1, WIDTH), F32),
    )
    main = pl.pallas_call(
        functools.partial(main_kernel, n_tp, n_dp, D, COLS_IN * n_tp, RAW_OUT * n_tp, D),
        out_shape=[pltpu.VMEM(shape, dtype) for shape, dtype in kept],
        in_specs=[hbm] * 6 + [hbm] * QUAD + [smem] * 3,
        out_specs=[vmem] * SUB,
        scratch_shapes=[
            pltpu.VMEM((3, 2, 2, 2 * M_IN, COLS_IN), F32),
            pltpu.VMEM((2, RAW_STEP, D), F32),
            pltpu.VMEM((2, 2, 2, 2, 2 * M_OUT, COLS_OUT), F32),
            pltpu.VMEM((ROWS_IN, COLS_IN), F32),
            pltpu.VMEM((ROWS_OUT, COLS_OUT), F32),
            pltpu.VMEM((RAW_OUT, 256), F32),
            pltpu.VMEM((RAW_OUT, LANE), F32),
            pltpu.VMEM((ROWS_IN, LANE), F32),
            pltpu.VMEM((1, COLS_IN), F32),
            pltpu.VMEM((SUB, LANE), F32),
            pltpu.VMEM((SUB, LANE), F32),
            pltpu.VMEM((SUB, COLS_IN), F32),
            pltpu.VMEM((ROWS_IN, LANE), F32),
            pltpu.VMEM((ROWS_IN, LANE), F32),
            pltpu.VMEM((SUB2, LANE), F32),
            pltpu.VMEM((SUB2, LANE), F32),
            pltpu.VMEM((2, 1, LEN_IN), F32),
            pltpu.VMEM((QUAD, 1, LEN_IN // 2), F32),
            pltpu.VMEM((1, LEN_IN), F32),
            pltpu.VMEM((2, 1, LEN_OUT), F32),
            pltpu.VMEM((QUAD, 1, LEN_OUT // 2), F32),
            pltpu.VMEM((1, LEN_OUT), F32),
            pltpu.VMEM((1, ROWS_IN), F32),
            pltpu.VMEM((1, COLS_IN), F32),
            pltpu.VMEM((1, RAW_OUT), F32),
            pltpu.VMEM((1, WIDTH), F32),
            pltpu.VMEM((2, 1, LANE), F32),
        ] + [pltpu.VMEM((i, 1, LANE), F32) for i in (2, 2, QUAD)] * 2 + [
            dma((N_RED, SLOTS)),
            dma((N_GAT, SLOTS)),
            dma((PAIR_SLOTS,)),
            dma((2 * QUAD + PIECES,)),
            dma((2, N_EX)),
        ],
        compiler_params=pltpu.CompilerParams(collective_id=0, has_side_effects=True, vmem_limit_bytes=GRANT),
    )
    final = pl.pallas_call(
        final_kernel,
        out_shape=[
            jax.ShapeDtypeStruct((QUAD, 2, ROWS_IN, COLS_IN), F32),
            jax.ShapeDtypeStruct((RAW_OUT, D), F32),
        ] + [jax.ShapeDtypeStruct(shape, dtype) for shape, dtype in kept[2:]],
        in_specs=[vmem] * SUB,
        out_specs=[hbm] * SUB,
        scratch_shapes=[pltpu.VMEM((RAW_OUT, D), F32), dma((14,)), dma((STEPS,))],
        compiler_params=pltpu.CompilerParams(vmem_limit_bytes=GRANT),
    )

    def body(w_in, w_out, g_in, g_out, m_in, m_out, r_in, c_in, r_out, c_out, learn_rate, weight_decay, beta_two):
        shards = (QUAD, 2, ROWS_IN, COLS_IN)
        got = main(
            w_in.reshape(shards), w_out[0], g_in.reshape((2, 2, 2, ROWS_IN, COLS_IN)), g_out[0, 0], m_in[0], m_out[0].T,
            r_in, c_in, r_out, c_out, learn_rate.reshape(1), weight_decay.reshape(1), beta_two.reshape(1))
        w_i, w_o, m_i, m_o, r_i, c_i, r_o, c_o = final(*[pltpu.with_memory_space_constraint(g, pltpu.VMEM) for g in got])
        return w_i.reshape((1, D, COLS_IN)), w_o[NO], m_i[NO], m_o.T[NO], r_i, c_i, r_o, c_o

    in_specs = (P(NO, NO, 'tp'), P(NO, 'tp', NO), P('dp', NO, NO, 'tp'), P('dp', NO, 'tp', NO), P(NO, 'dp', 'tp'), P(NO, 'tp', 'dp'), P(NO, 'dp'), P(NO, 'tp'), P(NO, 'tp'), P(NO, 'dp'), P(), P(), P())
    out_specs = (P(NO, NO, 'tp'), P(NO, 'tp', NO), P(NO, 'dp', 'tp'), P(NO, 'tp', 'dp'), P(NO, 'dp'), P(NO, 'tp'), P(NO, 'tp'), P(NO, 'dp'))
    return jax.shard_map(body, mesh=mesh, in_specs=in_specs, out_specs=out_specs, check_vma=False)
```

```python
import functools

import jax
import jax.numpy as jnp
from jax import lax
from jax.experimental import pallas as pl
from jax.experimental.pallas import tpu as pltpu
from jax.sharding import PartitionSpec as P

F32 = jnp.float32
BF16 = jnp.bfloat16
MESH = pl.DeviceIdType.MESH
LANE, SUB, SUB2, PART, QUAD, WIDTH = 128, 8, 16, 32, 4, 160
NO = None
BOTH, THREE = pl.ds(0, 2), pl.ds(0, 3)

D = 1280
ROWS_IN, COLS_IN = WIDTH, 4480
ROWS_OUT, COLS_OUT = 800, 640
RAW_OUT = 3200
STEPS = 10
M_IN = ROWS_IN // STEPS // 2
M_OUT = ROWS_OUT // STEPS // 2
RAW_STEP = RAW_OUT // STEPS
TILES_OUT = RAW_OUT // LANE

GRANT = 24 << 20

SLOTS, PAIR_SLOTS = 6, 10
N_RED, N_EX = 7, 8
(OWN, DSS, DSR, SENT, R1, R2, ON) = range(N_RED)
(ZS, ZR, CS, CR, TS, TR, BS, BR) = range(N_EX)
PIECES, PIECE = 7, COLS_IN // 7
LEN_IN, LEN_OUT = COLS_IN + LANE, RAW_OUT + LANE

def lanes(shape):
    return lax.broadcasted_iota(jnp.int32, shape, 1)


def aligned(value, by):
    return pl.multiple_of(value, by)


def pad_lanes(row):
    return jnp.concatenate([row, jnp.zeros((1, LANE - row.shape[1]), F32)], axis=1)


def row_to_col(row):
    return jnp.broadcast_to(row, (LANE, LANE)).T


def main_kernel(n_tp, n_dp, rows_all_in, cols_all_in, rows_all_out, cols_all_out,
                w_in, w_out, g_in, g_out, m_in, m_out, r_in_hbm, c_in_hbm, r_out_hbm, c_out_hbm, lr_ref, wd_ref, b2_ref,
                win, wpk, m_in_new, m_out_new, r_in_new, c_in_new, r_out_new, c_out_new,
                own_in, raw, packed, gs_in, gs_out, w_cols, ai_out, ai_in, bj_in, vec_x, vec_y,
                col_acc, row_acc, row_peer, col_acc_out, col_peer_out, v_in, vc_in, vf_in, v_out, vc_out, vf_out,
                r_in, c_in, r_out, c_out, zr, zt_in, pt_in, ct_in, zt_out, pt_out, ct_out,
                red_sem, pair_sem, load_sem, ex_sem):
    tp = lax.axis_index('tp')
    q = lax.axis_index('dp')
    p, c = q // 2, q % 2
    y, x = p // 2, p % 2
    nx, ny, nc = 1 - x, 1 - y, 1 - c
    p_x, p_y, p_d = 2 * y + nx, 2 * ny + x, 2 * ny + nx
    to_x = {'dp': 2 * p_x + c}
    to_y = {'dp': 2 * p_y + c}
    to_d = {'dp': 2 * p_d + c}
    to_core = {'dp': 2 * p + nc}
    to_z = {'tp': 1 - tp}
    j = q % QUAD
    lr, wd, b2 = lr_ref[0], wd_ref[0], b2_ref[0]

    barrier = pltpu.get_barrier_semaphore()
    for dev in (to_x, to_y, to_core, to_z):
        pl.semaphore_signal(barrier, inc=1, device_id=dev, device_id_type=MESH)

    def rcopy(src, dst, send, recv, dev):
        return pltpu.make_async_remote_copy(src_ref=src, dst_ref=dst, send_sem=send, recv_sem=recv, device_id=dev, device_id_type=MESH)

    def slot_of(ph, t):
        return lax.rem(ph * STEPS + t, SLOTS)

    def spans(m, t):
        base = aligned(2 * m * t, SUB)
        return pl.ds(base, 2 * m), pl.ds(base, m), pl.ds(aligned(base + m, SUB), m)

    def first_copies(ph, w, m, t):
        _, ra, rb = spans(m, t)
        a = rcopy(w.at[BOTH, nx, ra], w.at[2, BOTH, ra], red_sem.at[SENT, slot_of(ph, t)], red_sem.at[R1, slot_of(ph, t)], to_x)
        b = rcopy(w.at[ny, BOTH, rb], w.at[2, BOTH, rb], red_sem.at[SENT, slot_of(ph, t)], red_sem.at[R1, slot_of(ph, t)], to_y)
        return a, b

    def second_copies(ph, w, m, t):
        _, ra, rb = spans(m, t)
        a = rcopy(w.at[ny, x, ra], w.at[3, 0, ra], red_sem.at[SENT, slot_of(ph, t)], red_sem.at[R2, slot_of(ph, t)], to_y)
        b = rcopy(w.at[y, nx, rb], w.at[3, 0, rb], red_sem.at[SENT, slot_of(ph, t)], red_sem.at[R2, slot_of(ph, t)], to_x)
        return a, b

    def wait_first(ph, w, m, t):
        rr, _, _ = spans(m, t)
        part = w.at[2, BOTH, rr]
        rcopy(part, part, red_sem.at[SENT, slot_of(ph, t)], red_sem.at[R1, slot_of(ph, t)], to_x).wait_recv()

    def wait_second(ph, w, m, t):
        rr, _, _ = spans(m, t)
        part = w.at[3, 0, rr]
        rcopy(part, part, red_sem.at[SENT, slot_of(ph, t)], red_sem.at[R2, slot_of(ph, t)], to_y).wait_recv()

    def wait_sent(ph, w, m, t):
        rr, _, _ = spans(m, t)
        part = w.at[THREE, 0, rr]
        rcopy(part, part, red_sem.at[SENT, slot_of(ph, t)], red_sem.at[R1, slot_of(ph, t)], to_x).wait_send()

    def pair_in(t):
        rr, _, _ = spans(M_IN, t)
        return rcopy(g_in.at[:, :, nc, rr], win.at[BOTH, :, rr], red_sem.at[DSS, slot_of(0, t)], red_sem.at[DSR, slot_of(0, t)], to_core)

    def piece_in(k):
        rows, cols = pl.ds(0, 2 * M_IN), pl.ds(PIECE * k, PIECE)
        return rcopy(g_in.at[:, :, nc, rows, cols], win.at[BOTH, :, rows, cols], red_sem.at[DSS, 0], load_sem.at[k], to_core)

    def reduce_start():
        own_load(0).wait()
        for k in range(PIECES):
            cols = pl.ds(PIECE * k, PIECE)
            piece_in(k).wait_recv()
            for yy in range(2):
                for xx in range(2):
                    win[yy, xx, 0:2 * M_IN, cols] = win[yy, xx, 0:2 * M_IN, cols] + own_in[0, yy, xx, :, cols]
            ra, rb = pl.ds(0, M_IN), pl.ds(M_IN, M_IN)
            rcopy(win.at[BOTH, nx, ra, cols], win.at[2, BOTH, ra, cols], red_sem.at[SENT, 0], red_sem.at[R1, 0], to_x).start()
            rcopy(win.at[ny, BOTH, rb, cols], win.at[2, BOTH, rb, cols], red_sem.at[SENT, 0], red_sem.at[R1, 0], to_y).start()

    def own_load(t):
        rr, _, _ = spans(M_IN, t)
        return pltpu.make_async_copy(g_in.at[:, :, c, rr], own_in.at[lax.rem(t, 3)], red_sem.at[OWN, slot_of(0, t)])

    def raw_load(t):
        return pltpu.make_async_copy(g_out.at[pl.ds(aligned(RAW_STEP * t, SUB), RAW_STEP)], raw.at[lax.rem(t, 2)], red_sem.at[OWN, slot_of(1, t)])

    def pair_out(t):
        rr, _, _ = spans(M_OUT, t)
        return rcopy(packed.at[lax.rem(t, 2), :, :, nc], wpk.at[BOTH, :, rr], red_sem.at[DSS, slot_of(1, t)], red_sem.at[DSR, slot_of(1, t)], to_core)

    def start_in(t):
        own_load(t).start()
        pair_in(t).start()

    def pack_out(t):
        raw_load(t).wait()
        slot = lax.rem(t, 2)

        @pl.when(t >= 2)
        def _():
            pair_out(t - 2).wait_send()

        def unit(u, _):
            base = aligned(PART * u, SUB)
            tiles = [[raw[slot, pl.ds(base + SUB * k, SUB), LANE * i:LANE * i + LANE] for i in range(10)] for k in range(QUAD)]
            ln = lanes((SUB, LANE))
            for s in range(SUB):
                jj, first = s % QUAD, 5 * (s // QUAD) + s % QUAD
                tail = NO
                for k in range(QUAD):
                    lo, hi = tiles[k][first], tiles[k][first + 1]
                    head = lo if jj == 0 else pltpu.roll(jnp.where(ln >= PART * jj, lo, hi), LANE - PART * jj, 1)
                    packed[slot, s // QUAD, (s // 2) % 2, s % 2, pl.ds(aligned(SUB * u, SUB), SUB), LANE * k:LANE * k + LANE] = head
                    turn = (PART * (k - jj)) % LANE
                    part = hi if turn == 0 else pltpu.roll(hi, turn, 1)
                    tail = part if tail is NO else jnp.where(ln >= PART * k, part, tail)
                packed[slot, s // QUAD, (s // 2) % 2, s % 2, pl.ds(aligned(SUB * u, SUB), SUB), 512:640] = tail
            return 0

        lax.fori_loop(0, RAW_STEP // PART, unit, 0)
        pair_out(t).start()

        @pl.when(t + 2 < STEPS)
        def _():
            raw_load(t + 2).start()

    def reduce_first(ph, w, m, t):
        rr, _, _ = spans(m, t)
        if ph == 0:
            own_load(t).wait()
            pair_in(t).wait_recv()
            slot = lax.rem(t, 3)
            for yy in range(2):
                for xx in range(2):
                    for r in range(0, 2 * m, SUB):
                        rows = pl.ds(aligned(2 * m * t + r, SUB), SUB)
                        w[yy, xx, rows] = w[yy, xx, rows] + own_in[slot, yy, xx, r:r + SUB]
        else:
            pair_out(t).wait_recv()
            slot = lax.rem(t, 2)

            def add(i, _):
                rows = pl.ds(aligned(2 * m * t + SUB2 * i, SUB), SUB2)
                for yy in range(2):
                    for xx in range(2):
                        w[yy, xx, rows] = w[yy, xx, rows] + packed[slot, yy, xx, c, pl.ds(aligned(SUB2 * i, SUB), SUB2)]
                return 0

            lax.fori_loop(0, 2 * m // SUB2, add, 0)
        for copy in first_copies(ph, w, m, t):
            copy.start()

    def reduce_second(ph, w, m, t):
        _, ra, rb = spans(m, t)
        on_y, on_x = second_copies(ph, w, m, t)
        if ph == 0:
            pair_in(t).wait_send()
        wait_first(ph, w, m, t)
        w[ny, x, ra] = w[ny, x, ra] + w[2, ny, ra]
        on_y.start()
        w[y, nx, rb] = w[y, nx, rb] + w[2, nx, rb]
        on_x.start()

    def reduce_third(ph, w, m, t, gs):
        _, ra, rb = spans(m, t)
        wait_second(ph, w, m, t)
        ga = w[y, x, ra] + w[2, y, ra] + w[3, 0, ra]
        gs[ra] = ga
        gb = w[y, x, rb] + w[2, x, rb] + w[3, 0, rb]
        gs[rb] = gb
        wait_sent(ph, w, m, t)
        if ph == 0:
            sa, sb = ga * ga + 1e-30, gb * gb + 1e-30
            col_acc[...] = col_acc[...] + (sa + sb)
            for rows, sq in ((ra, sa), (rb, sb)):
                part = sq[:, 0:LANE]
                for i in range(1, COLS_IN // LANE):
                    part = part + sq[:, LANE * i:LANE * i + LANE]
                row_acc[rows] = part

    def sems(ph, t, send, recv):
        return red_sem.at[send, slot_of(2 + ph, t)], red_sem.at[recv, slot_of(2 + ph, t)]

    def pair_sems(ph, t, send):
        return red_sem.at[send, slot_of(2 + ph, t)], pair_sem.at[lax.rem(ph * STEPS + t, PAIR_SLOTS)]

    def gather_first(ph, w, m, t):
        rr, _, _ = spans(m, t)
        src = w.at[p, c, rr]
        rcopy(src, src, *sems(ph, t, SENT, R1), to_x).start()
        rcopy(src, src, *sems(ph, t, SENT, R1), to_y).start()
        rcopy(src, src, *pair_sems(ph, t, SENT), to_core).start()

    def gather_second(ph, w, m, t):
        rr, ra, rb = spans(m, t)
        both = w.at[BOTH, c, rr]
        rcopy(both, both, *sems(ph, t, SENT, R1), to_x).wait_recv()
        for other, rows, dev in ((p_x, rb, to_y), (p_y, ra, to_x)):
            rcopy(w.at[other, c, rows], w.at[other, c, rows], *sems(ph, t, ON, R2), dev).start()
            rcopy(w.at[other, c, rr], w.at[other, c, rr], *pair_sems(ph, t, ON), to_core).start()

    def gather_third(ph, w, m, t):
        rr, _, _ = spans(m, t)
        diag = w.at[p_d, c, rr]
        rcopy(diag, diag, *sems(ph, t, ON, R2), to_x).wait_recv()
        rcopy(diag, diag, *pair_sems(ph, t, ON), to_core).start()
        three = w.at[THREE, c, rr]
        rcopy(three, three, *sems(ph, t, SENT, R1), to_x).wait_send()

    def gather_last(ph, w, m, t):
        rr, _, _ = spans(m, t)
        four = w.at[:, nc, rr]
        rcopy(four, four, *pair_sems(ph, t, ON), to_core).wait_recv()
        rcopy(four, four, *pair_sems(ph, t, ON), to_core).wait_send()

    def z_share(src, dst, k):
        return rcopy(src, dst, ex_sem.at[k, ZS], ex_sem.at[k, ZR], to_z)

    def share(buf, k):
        copy = rcopy(buf.at[0], buf.at[1], ex_sem.at[k, CS], ex_sem.at[k, CR], to_core)
        copy.start()
        copy.wait()
        return buf[0] + buf[1]

    def to_chips(buf, k):
        for dev in (to_x, to_y, to_d):
            rcopy(buf.at[p], buf.at[p], ex_sem.at[k, TS], ex_sem.at[k, TR], dev).start()

    def from_chips(buf, k):
        three = buf.at[THREE]
        rcopy(three, three, ex_sem.at[k, TS], ex_sem.at[k, TR], to_x).wait()
        return buf[0] + buf[1] + buf[2] + buf[3]

    def halves(length):
        half = length // 2
        return pl.ds(aligned(c * half, LANE), half), pl.ds(aligned(nc * half, LANE), half)

    def vector_send(buf, chips, length):
        mine, other = halves(length)
        copy = rcopy(buf.at[0, :, other], buf.at[1, :, other], ex_sem.at[0, CS], ex_sem.at[0, CR], to_core)
        copy.start()
        copy.wait()
        chips[p] = buf[0, :, mine] + buf[1, :, mine]
        to_chips(chips, 0)

    def vector_take(chips, whole, length):
        mine, _ = halves(length)
        whole[:, mine] = from_chips(chips, 0)
        copy = rcopy(whole.at[:, mine], whole.at[:, mine], ex_sem.at[0, BS], ex_sem.at[0, BR], to_core)
        copy.start()
        copy.wait()

    def share_squares(acc, zt, pt, ct):
        zt[0] = jnp.sum(acc, axis=0, keepdims=True)
        copy = z_share(zt.at[0], zt.at[1], 1)
        copy.start()
        copy.wait()
        pt[0] = zt[0] + zt[1]
        ct[p] = share(pt, 1)
        to_chips(ct, 1)

    def scale_from(ct, count):
        mean = jnp.sum(from_chips(ct, 1), axis=1, keepdims=True) / count
        return 0.1 / jnp.maximum(1.0, jnp.sqrt(mean))

    def vec_loads():
        pairs = ((r_in_hbm, r_in), (c_in_hbm, c_in), (r_out_hbm, r_out), (c_out_hbm, c_out))
        return [pltpu.make_async_copy(src, dst, load_sem.at[QUAD + i]) for i, (src, dst) in enumerate(pairs)]

    def stats_in_send():
        for load in vec_loads():
            load.wait()
        copy = z_share(row_acc, row_peer, 0)
        copy.start()
        v_in[0, :, 0:COLS_IN] = jnp.sum(col_acc[...], axis=0, keepdims=True)
        copy.wait()
        row_mean = jnp.sum(row_acc[...] + row_peer[...], axis=1, keepdims=True) / cols_all_in
        row_mean = jnp.broadcast_to(row_mean, (ROWS_IN, LANE))
        r_old = jnp.concatenate([row_to_col(r_in[:, 0:LANE]), row_to_col(pad_lanes(r_in[:, LANE:WIDTH]))[0:PART]], axis=0)
        r_new = b2 * r_old + (1.0 - b2) * row_mean
        r_in_new[:, 0:LANE] = r_new[0:LANE].T[0:1]
        r_in_new[:, LANE:WIDTH] = jnp.concatenate([r_new[LANE:WIDTH], jnp.zeros((LANE - PART, LANE), F32)], axis=0).T[0:1, 0:PART]
        ai_in[...] = r_new
        v_in[0, :, COLS_IN:LEN_IN] = jnp.sum(r_new, axis=0, keepdims=True)
        vector_send(v_in, vc_in, LEN_IN)
        w_load_in().start()

    def w_load_in():
        return pltpu.make_async_copy(w_in.at[p, c], win.at[p, c], load_sem.at[0])

    def stats_in_norm():
        vector_take(vc_in, vf_in, LEN_IN)
        vec = vf_in[...]
        c_new = b2 * c_in[...] + (1.0 - b2) * (vec[:, 0:COLS_IN] / rows_all_in)
        c_in_new[...] = c_new
        bj_in[...] = 1.0 / jnp.sqrt(c_new)
        root_avg = jnp.sqrt(vec[:, COLS_IN:COLS_IN + 1] / rows_all_in)
        ai_in[...] = root_avg / jnp.sqrt(ai_in[...])

        def body(i, acc):
            rows = pl.ds(aligned(SUB * i, SUB), SUB)
            a = ai_in[rows]
            for k in range(COLS_IN // LANE):
                col = slice(LANE * k, LANE * k + LANE)
                u = gs_in[rows, col] * a * bj_in[:, col]
                acc = acc + u * u
            return acc

        share_squares(lax.fori_loop(0, ROWS_IN // SUB, body, jnp.zeros((SUB, LANE), F32)), zt_in, pt_in, ct_in)

    def update_in():
        scale = scale_from(ct_in, float(rows_all_in * cols_all_in))
        w_load_in().wait()
        m_load_in().wait()

        def body(i, _):
            rows = pl.ds(aligned(SUB2 * i, SUB2), SUB2)
            a = ai_in[rows] * scale
            for k in range(COLS_IN // LANE):
                col = slice(LANE * k, LANE * k + LANE)
                u = gs_in[rows, col] * a * bj_in[:, col]
                mom = (0.9 * m_in_new[rows, col].astype(F32) + u).astype(BF16)
                m_in_new[rows, col] = mom
                old = win[p, c, rows, col]
                win[p, c, rows, col] = old - lr * mom.astype(F32) - lr * wd * old
            return 0

        lax.fori_loop(0, ROWS_IN // SUB2, body, 0)

    def m_load_in():
        return pltpu.make_async_copy(m_in, m_in_new, load_sem.at[1])

    def block_out(t):
        heads, tails = [], []
        for u in range(QUAD):
            rows = pl.ds(aligned(PART * t + SUB * u, SUB), SUB)
            tail = gs_out[rows, 512:640]
            for k in range(QUAD):
                heads.append(gs_out[rows, LANE * k:LANE * k + LANE])
                tails.append(tail if k == 0 else pltpu.roll(tail, LANE - PART * k, 1))
        tails = jnp.concatenate(tails, axis=0)
        return jnp.concatenate(heads, axis=0), jnp.where(lanes((LANE, LANE)) < PART, tails, 0.0)

    def stats_out_send():
        def body(t, acc):
            head, tail = block_out(t)
            sh = head * head + 1e-30
            st = jnp.where(lanes((LANE, LANE)) < PART, tail * tail + 1e-30, 0.0)
            v_out[0, :, pl.ds(aligned(LANE * t, LANE), LANE)] = jnp.sum((sh + st).T, axis=0, keepdims=True)
            ah, at = acc
            for i in range(SUB2):
                ah = ah + sh[SUB * i:SUB * i + SUB]
                at = at + st[SUB * i:SUB * i + SUB]
            return ah, at

        zero = jnp.zeros((SUB, LANE), F32)
        ah, at = lax.fori_loop(0, TILES_OUT, body, (zero, zero))
        col_acc_out[0:SUB] = ah
        col_acc_out[SUB:SUB2] = at
        copy = z_share(col_acc_out, col_peer_out, 0)
        copy.start()
        copy.wait()
        v_out[0, :, RAW_OUT:LEN_OUT] = jnp.zeros((1, LANE), F32)
        vector_send(v_out, vc_out, LEN_OUT)

    def stats_out_norm():
        vector_take(vc_out, vf_out, LEN_OUT)
        vec = vf_out[...]
        r_new = b2 * r_out[...] + (1.0 - b2) * (vec[:, 0:RAW_OUT] / cols_all_out)
        r_out_new[...] = r_new
        part = r_new[:, 0:LANE]
        for i in range(1, TILES_OUT):
            part = part + r_new[:, LANE * i:LANE * i + LANE]
        zr[0] = part
        copy = rcopy(zr.at[0], zr.at[1], ex_sem.at[1, BS], ex_sem.at[1, BR], to_z)
        copy.start()
        copy.wait()
        root_avg = jnp.sqrt(jnp.sum(zr[0] + zr[1], axis=1, keepdims=True) / rows_all_out)
        cols = col_acc_out[...] + col_peer_out[...]
        c_new_h = b2 * c_out[:, 0:LANE] + (1.0 - b2) * (jnp.sum(cols[0:SUB], axis=0, keepdims=True) / rows_all_out)
        c_new_t = b2 * pad_lanes(c_out[:, LANE:WIDTH]) + (1.0 - b2) * (jnp.sum(cols[SUB:SUB2], axis=0, keepdims=True) / rows_all_out)
        c_out_new[:, 0:LANE] = c_new_h
        c_out_new[:, LANE:WIDTH] = c_new_t[:, 0:PART]
        vec_x[...] = jnp.broadcast_to(1.0 / jnp.sqrt(c_new_h), (SUB, LANE))
        vec_y[...] = jnp.broadcast_to(1.0 / jnp.sqrt(jnp.where(lanes((1, LANE)) < PART, c_new_t, 1.0)), (SUB, LANE))
        bh, bt = vec_x[0:1], vec_y[0:1]

        def body(t, acc):
            rows = pl.ds(aligned(LANE * t, LANE), LANE)
            a = row_to_col(root_avg / jnp.sqrt(r_out_new[:, rows]))
            ai_out[rows] = a
            head, tail = block_out(t)
            uh, ut = head * a * bh, tail * a * bt
            sq = uh * uh + ut * ut
            for i in range(SUB2):
                acc = acc + sq[SUB * i:SUB * i + SUB]
            return acc

        share_squares(lax.fori_loop(0, TILES_OUT, body, jnp.zeros((SUB, LANE), F32)), zt_out, pt_out, ct_out)

    def w_load_out():
        first = 5 * (q // QUAD) + j
        return pltpu.make_async_copy(w_out.at[:, pl.ds(aligned(LANE * first, LANE), 256)], w_cols, load_sem.at[2])

    def m_load_out():
        return pltpu.make_async_copy(m_out, m_out_new, load_sem.at[3])

    def update_out():
        scale = scale_from(ct_out, float(rows_all_out * cols_all_out))
        w_load_out().wait()
        m_load_out().wait()
        bh, bt = vec_x[0:1], vec_y[0:1]
        back = PART * ((QUAD - j) % QUAD)

        def body(t, _):
            rows = pl.ds(aligned(LANE * t, LANE), LANE)
            a = ai_out[rows] * scale
            head, tail = block_out(t)
            uh, ut = head * a * bh, tail * a * bt
            mom = m_out_new[:, rows].astype(F32)
            mh = (0.9 * mom[0:LANE].T + uh).astype(BF16).astype(F32)
            mt = (0.9 * jnp.concatenate([mom[LANE:WIDTH], jnp.zeros((96, LANE), F32)], axis=0).T + ut).astype(BF16).astype(F32)
            m_out_new[0:LANE, rows] = mh.T.astype(BF16)
            m_out_new[LANE:WIDTH, rows] = mt.T[0:PART].astype(BF16)
            lo, hi = w_cols[rows, 0:LANE], w_cols[rows, LANE:256]
            wh = pltpu.roll(jnp.where(lanes((LANE, LANE)) >= PART * j, lo, hi), back, 1)
            wt = pltpu.roll(hi, back, 1)
            wh = wh - lr * mh - lr * wd * wh
            wt = wt - lr * mt - lr * wd * wt
            ln = lanes((SUB, LANE))
            for u in range(QUAD):
                to = pl.ds(aligned(PART * t + SUB * u, SUB), SUB)
                joined = NO
                for k in range(QUAD):
                    at = PART * u + SUB * k
                    wpk[p, c, to, LANE * k:LANE * k + LANE] = wh[at:at + SUB]
                    part = wt[at:at + SUB] if k == 0 else pltpu.roll(wt[at:at + SUB], PART * k, 1)
                    joined = part if joined is NO else jnp.where(ln >= PART * k, part, joined)
                wpk[p, c, to, 512:640] = joined
            return 0

        lax.fori_loop(0, TILES_OUT, body, 0)

    col_acc[...] = jnp.zeros_like(col_acc)
    own_load(0).start()
    own_load(1).start()
    pl.semaphore_wait(barrier, QUAD)
    for k in range(PIECES):
        piece_in(k).start()
    pair_in(1).start()
    reduce_start()

    def at_step(cond, fn, *args):
        @pl.when(cond)
        def _():
            fn(*args)

    n = STEPS

    def step(s, _):
        def within(lo, hi):
            return jnp.logical_and(s >= lo, s < hi)

        at_step(s + 2 < n, start_in, s + 2)
        at_step(within(1, n), reduce_first, 0, win, M_IN, s)
        at_step(within(2, n + 2), reduce_second, 0, win, M_IN, s - 2)
        at_step(within(QUAD, n + QUAD), reduce_third, 0, win, M_IN, s - QUAD, gs_in)

        @pl.when(s == 2)
        def _():
            for copy in vec_loads():
                copy.start()
            m_load_in().start()
            m_load_out().start()
            w_load_out().start()

        @pl.when(s == n - 3)
        def _():
            raw_load(0).start()
            raw_load(1).start()

        at_step(within(n, 2 * n), reduce_first, 1, wpk, M_OUT, s - n)
        at_step(within(n - 1, 2 * n - 1), pack_out, s - n + 1)
        at_step(within(n + 2, 2 * n + 2), reduce_second, 1, wpk, M_OUT, s - n - 2)
        at_step(within(n + QUAD, 2 * n + QUAD), reduce_third, 1, wpk, M_OUT, s - n - QUAD, gs_out)
        at_step(s == n + 3, stats_in_send)
        at_step(s == n + 6, stats_in_norm)
        at_step(s == n + 9, update_in)
        at_step(within(2 * n, 3 * n), gather_first, 0, win, M_IN, s - 2 * n)
        at_step(within(2 * n + 2, 3 * n + 2), gather_second, 0, win, M_IN, s - 2 * n - 2)
        at_step(within(2 * n + QUAD, 3 * n + QUAD), gather_third, 0, win, M_IN, s - 2 * n - QUAD)
        at_step(s == 2 * n + 3, stats_out_send)
        at_step(s == 2 * n + 6, stats_out_norm)
        at_step(s == 2 * n + 9, update_out)
        at_step(within(3 * n, QUAD * n), gather_first, 1, wpk, M_OUT, s - 3 * n)
        at_step(within(3 * n + 2, QUAD * n + 2), gather_second, 1, wpk, M_OUT, s - 3 * n - 2)
        at_step(within(3 * n + QUAD, QUAD * n + QUAD), gather_third, 1, wpk, M_OUT, s - 3 * n - QUAD)
        at_step(within(2 * n + 6, 3 * n + 6), gather_last, 0, win, M_IN, s - 2 * n - 6)
        at_step(within(3 * n + 6, QUAD * n + 6), gather_last, 1, wpk, M_OUT, s - 3 * n - 6)
        return 0

    lax.fori_loop(0, QUAD * n + 6, step, 0)
    pair_out(n - 2).wait_send()
    pair_out(n - 1).wait_send()


def final_kernel(win, wpk, mi, mo, ri, ci, ro, co, win_o, wout_o, mi_o, mo_o, ri_o, ci_o, ro_o, co_o, stage, sem, stage_sem):
    plain = [pltpu.make_async_copy(win.at[i // 2, i % 2], win_o.at[i // 2, i % 2], sem.at[i]) for i in range(SUB)]
    for i, (src, dst) in enumerate(((mi, mi_o), (mo, mo_o), (ri, ri_o), (ci, ci_o), (ro, ro_o), (co, co_o))):
        plain.append(pltpu.make_async_copy(src, dst, sem.at[SUB + i]))
    for copy in plain:
        copy.start()

    def rows_of(t):
        return pl.ds(aligned(RAW_STEP * t, SUB), RAW_STEP)

    def put(t):
        return pltpu.make_async_copy(stage.at[rows_of(t)], wout_o.at[rows_of(t)], stage_sem.at[t])

    def chunk(t, _):
        def unit(u, _):
            ln = lanes((SUB, LANE))
            rows = pl.ds(aligned(2 * M_OUT * t + SUB * u, SUB), SUB)
            for half in range(2):
                tails = [wpk[2 * half + jj // 2, jj % 2, rows, 512:640] for jj in range(QUAD)]
                for k in range(QUAD):
                    to = pl.ds(aligned(RAW_STEP * t + PART * u + SUB * k, SUB), SUB)
                    heads = []
                    for jj in range(QUAD):
                        head = wpk[2 * half + jj // 2, jj % 2, rows, LANE * k:LANE * k + LANE]
                        heads.append(head if jj == 0 else pltpu.roll(head, PART * jj, 1))
                    ends = [tails[jj] if jj == k else pltpu.roll(tails[jj], (PART * (jj - k)) % LANE, 1) for jj in range(QUAD)]
                    for tile in range(5):
                        if tile == 0:
                            out = heads[0]
                        else:
                            out = ends[tile - 1]
                            if tile > 1:
                                out = jnp.where(ln < PART * (tile - 1), heads[tile - 1], out)
                            if tile < QUAD:
                                out = jnp.where(ln >= PART * tile, heads[tile], out)
                        at = LANE * (5 * half + tile)
                        stage[to, at:at + LANE] = out
            return 0

        lax.fori_loop(0, RAW_STEP // PART, unit, 0)
        put(t).start()
        return 0

    lax.fori_loop(0, STEPS, chunk, 0)
    for t in range(STEPS):
        put(t).wait()
    for copy in plain:
        copy.wait()


def solution(mesh):
    n_tp = mesh.shape['tp']
    n_dp = mesh.shape['dp']
    vmem = pl.BlockSpec(memory_space=pltpu.VMEM)
    hbm = pl.BlockSpec(memory_space=pltpu.HBM)
    smem = pl.BlockSpec(memory_space=pltpu.SMEM)
    dma = pltpu.SemaphoreType.DMA
    kept = (
        ((QUAD, 2, ROWS_IN, COLS_IN), F32),
        ((QUAD, 2, ROWS_OUT, COLS_OUT), F32),
        ((ROWS_IN, COLS_IN), BF16),
        ((WIDTH, RAW_OUT), BF16),
        ((1, ROWS_IN), F32),
        ((1, COLS_IN), F32),
        ((1, RAW_OUT), F32),
        ((1, WIDTH), F32),
    )
    main = pl.pallas_call(
        functools.partial(main_kernel, n_tp, n_dp, D, COLS_IN * n_tp, RAW_OUT * n_tp, D),
        out_shape=[pltpu.VMEM(shape, dtype) for shape, dtype in kept],
        in_specs=[hbm] * 6 + [hbm] * QUAD + [smem] * 3,
        out_specs=[vmem] * SUB,
        scratch_shapes=[
            pltpu.VMEM((3, 2, 2, 2 * M_IN, COLS_IN), F32),
            pltpu.VMEM((2, RAW_STEP, D), F32),
            pltpu.VMEM((2, 2, 2, 2, 2 * M_OUT, COLS_OUT), F32),
            pltpu.VMEM((ROWS_IN, COLS_IN), F32),
            pltpu.VMEM((ROWS_OUT, COLS_OUT), F32),
            pltpu.VMEM((RAW_OUT, 256), F32),
            pltpu.VMEM((RAW_OUT, LANE), F32),
            pltpu.VMEM((ROWS_IN, LANE), F32),
            pltpu.VMEM((1, COLS_IN), F32),
            pltpu.VMEM((SUB, LANE), F32),
            pltpu.VMEM((SUB, LANE), F32),
            pltpu.VMEM((SUB, COLS_IN), F32),
            pltpu.VMEM((ROWS_IN, LANE), F32),
            pltpu.VMEM((ROWS_IN, LANE), F32),
            pltpu.VMEM((SUB2, LANE), F32),
            pltpu.VMEM((SUB2, LANE), F32),
            pltpu.VMEM((2, 1, LEN_IN), F32),
            pltpu.VMEM((QUAD, 1, LEN_IN // 2), F32),
            pltpu.VMEM((1, LEN_IN), F32),
            pltpu.VMEM((2, 1, LEN_OUT), F32),
            pltpu.VMEM((QUAD, 1, LEN_OUT // 2), F32),
            pltpu.VMEM((1, LEN_OUT), F32),
            pltpu.VMEM((1, ROWS_IN), F32),
            pltpu.VMEM((1, COLS_IN), F32),
            pltpu.VMEM((1, RAW_OUT), F32),
            pltpu.VMEM((1, WIDTH), F32),
            pltpu.VMEM((2, 1, LANE), F32),
        ] + [pltpu.VMEM((i, 1, LANE), F32) for i in (2, 2, QUAD)] * 2 + [
            dma((N_RED, SLOTS)),
            dma((PAIR_SLOTS,)),
            dma((2 * QUAD,)),
            dma((2, N_EX)),
        ],
        compiler_params=pltpu.CompilerParams(collective_id=0, has_side_effects=True, vmem_limit_bytes=GRANT),
    )
    final = pl.pallas_call(
        final_kernel,
        out_shape=[
            jax.ShapeDtypeStruct((QUAD, 2, ROWS_IN, COLS_IN), F32),
            jax.ShapeDtypeStruct((RAW_OUT, D), F32),
        ] + [jax.ShapeDtypeStruct(shape, dtype) for shape, dtype in kept[2:]],
        in_specs=[vmem] * SUB,
        out_specs=[hbm] * SUB,
        scratch_shapes=[pltpu.VMEM((RAW_OUT, D), F32), dma((14,)), dma((STEPS,))],
        compiler_params=pltpu.CompilerParams(vmem_limit_bytes=GRANT),
    )

    def body(w_in, w_out, g_in, g_out, m_in, m_out, r_in, c_in, r_out, c_out, learn_rate, weight_decay, beta_two):
        shards = (QUAD, 2, ROWS_IN, COLS_IN)
        got = main(
            w_in.reshape(shards), w_out[0], g_in.reshape((2, 2, 2, ROWS_IN, COLS_IN)), g_out[0, 0], m_in[0], m_out[0].T,
            r_in, c_in, r_out, c_out, learn_rate.reshape(1), weight_decay.reshape(1), beta_two.reshape(1))
        w_i, w_o, m_i, m_o, r_i, c_i, r_o, c_o = final(*[pltpu.with_memory_space_constraint(g, pltpu.VMEM) for g in got])
        return w_i.reshape((1, D, COLS_IN)), w_o[NO], m_i[NO], m_o.T[NO], r_i, c_i, r_o, c_o

    in_specs = (P(NO, NO, 'tp'), P(NO, 'tp', NO), P('dp', NO, NO, 'tp'), P('dp', NO, 'tp', NO), P(NO, 'dp', 'tp'), P(NO, 'tp', 'dp'), P(NO, 'dp'), P(NO, 'tp'), P(NO, 'tp'), P(NO, 'dp'), P(), P(), P())
    out_specs = (P(NO, NO, 'tp'), P(NO, 'tp', NO), P(NO, 'dp', 'tp'), P(NO, 'tp', 'dp'), P(NO, 'dp'), P(NO, 'tp'), P(NO, 'tp'), P(NO, 'dp'))
    return jax.shard_map(body, mesh=mesh, in_specs=in_specs, out_specs=out_specs, check_vma=False)
```

```python
import functools

import jax
import jax.numpy as jnp
from jax import lax
from jax.experimental import pallas as pl
from jax.experimental.pallas import tpu as pltpu
from jax.sharding import PartitionSpec as P

F32 = jnp.float32
BF16 = jnp.bfloat16
MESH = pl.DeviceIdType.MESH
LANE, SUB, SUB2, PART, QUAD, WIDTH = 128, 8, 16, 32, 4, 160
NO = None
BOTH, THREE = pl.ds(0, 2), pl.ds(0, 3)

D = 1280
ROWS_IN, COLS_IN = WIDTH, 4480
ROWS_OUT, COLS_OUT = 800, 640
RAW_OUT = 3200
STEPS = 10
M_IN = ROWS_IN // STEPS // 2
M_OUT = ROWS_OUT // STEPS // 2
RAW_STEP = RAW_OUT // STEPS
TILES_OUT = RAW_OUT // LANE

GRANT = 24 << 20

SLOTS, PAIR_SLOTS = 6, 10
N_RED, N_EX = 7, 8
(OWN, DSS, DSR, SENT, R1, R2, ON) = range(N_RED)
(ZS, ZR, CS, CR, TS, TR, BS, BR) = range(N_EX)
PIECES = (0, 1, 3, 7, 13, 20, 27, COLS_IN // LANE)
LEN_IN, LEN_OUT = COLS_IN + LANE, RAW_OUT + LANE

def lanes(shape):
    return lax.broadcasted_iota(jnp.int32, shape, 1)


def aligned(value, by):
    return pl.multiple_of(value, by)


def pad_lanes(row):
    return jnp.concatenate([row, jnp.zeros((1, LANE - row.shape[1]), F32)], axis=1)


def row_to_col(row):
    return jnp.broadcast_to(row, (LANE, LANE)).T


def main_kernel(n_tp, n_dp, rows_all_in, cols_all_in, rows_all_out, cols_all_out,
                w_in, w_out, g_in, g_out, m_in, m_out, r_in_hbm, c_in_hbm, r_out_hbm, c_out_hbm, lr_ref, wd_ref, b2_ref,
                win, wpk, m_in_new, m_out_new, r_in_new, c_in_new, r_out_new, c_out_new,
                own_in, raw, packed, gs_in, gs_out, w_cols, ai_out, ai_in, bj_in, vec_x, vec_y,
                col_acc, row_acc, row_peer, col_acc_out, col_peer_out, v_in, vc_in, vf_in, v_out, vc_out, vf_out,
                r_in, c_in, r_out, c_out, zr, zt_in, pt_in, ct_in, zt_out, pt_out, ct_out,
                red_sem, pair_sem, load_sem, ex_sem):
    tp = lax.axis_index('tp')
    q = lax.axis_index('dp')
    p, c = q // 2, q % 2
    y, x = p // 2, p % 2
    nx, ny, nc = 1 - x, 1 - y, 1 - c
    p_x, p_y, p_d = 2 * y + nx, 2 * ny + x, 2 * ny + nx
    to_x = {'dp': 2 * p_x + c}
    to_y = {'dp': 2 * p_y + c}
    to_d = {'dp': 2 * p_d + c}
    to_core = {'dp': 2 * p + nc}
    to_z = {'tp': 1 - tp}
    j = q % QUAD
    lr, wd, b2 = lr_ref[0], wd_ref[0], b2_ref[0]

    barrier = pltpu.get_barrier_semaphore()
    for dev in (to_x, to_y, to_core, to_z):
        pl.semaphore_signal(barrier, inc=1, device_id=dev, device_id_type=MESH)

    def rcopy(src, dst, send, recv, dev):
        return pltpu.make_async_remote_copy(src_ref=src, dst_ref=dst, send_sem=send, recv_sem=recv, device_id=dev, device_id_type=MESH)

    def slot_of(ph, t):
        return lax.rem(ph * STEPS + t, SLOTS)

    def spans(m, t):
        base = aligned(2 * m * t, SUB)
        return pl.ds(base, 2 * m), pl.ds(base, m), pl.ds(aligned(base + m, SUB), m)

    def first_copies(ph, w, m, t):
        _, ra, rb = spans(m, t)
        a = rcopy(w.at[BOTH, nx, ra], w.at[2, BOTH, ra], red_sem.at[SENT, slot_of(ph, t)], red_sem.at[R1, slot_of(ph, t)], to_x)
        b = rcopy(w.at[ny, BOTH, rb], w.at[2, BOTH, rb], red_sem.at[SENT, slot_of(ph, t)], red_sem.at[R1, slot_of(ph, t)], to_y)
        return a, b

    def second_copies(ph, w, m, t):
        _, ra, rb = spans(m, t)
        a = rcopy(w.at[ny, x, ra], w.at[3, 0, ra], red_sem.at[SENT, slot_of(ph, t)], red_sem.at[R2, slot_of(ph, t)], to_y)
        b = rcopy(w.at[y, nx, rb], w.at[3, 0, rb], red_sem.at[SENT, slot_of(ph, t)], red_sem.at[R2, slot_of(ph, t)], to_x)
        return a, b

    def wait_first(ph, w, m, t):
        rr, _, _ = spans(m, t)
        part = w.at[2, BOTH, rr]
        rcopy(part, part, red_sem.at[SENT, slot_of(ph, t)], red_sem.at[R1, slot_of(ph, t)], to_x).wait_recv()

    def wait_second(ph, w, m, t):
        rr, _, _ = spans(m, t)
        part = w.at[3, 0, rr]
        rcopy(part, part, red_sem.at[SENT, slot_of(ph, t)], red_sem.at[R2, slot_of(ph, t)], to_y).wait_recv()

    def wait_sent(ph, w, m, t):
        rr, _, _ = spans(m, t)
        part = w.at[THREE, 0, rr]
        rcopy(part, part, red_sem.at[SENT, slot_of(ph, t)], red_sem.at[R1, slot_of(ph, t)], to_x).wait_send()

    def pair_in(t):
        rr, _, _ = spans(M_IN, t)
        return rcopy(g_in.at[:, :, nc, rr], win.at[BOTH, :, rr], red_sem.at[DSS, slot_of(0, t)], red_sem.at[DSR, slot_of(0, t)], to_core)

    def piece(k):
        return pl.ds(LANE * PIECES[k], LANE * (PIECES[k + 1] - PIECES[k]))

    def piece_in(k):
        rows, cols = pl.ds(0, 2 * M_IN), piece(k)
        return rcopy(g_in.at[:, :, nc, rows, cols], win.at[BOTH, :, rows, cols], red_sem.at[DSS, 0], load_sem.at[k], to_core)

    def reduce_start():
        own_load(0).wait()
        for k in range(len(PIECES) - 1):
            cols = piece(k)
            piece_in(k).wait_recv()
            for yy in range(2):
                for xx in range(2):
                    win[yy, xx, 0:2 * M_IN, cols] = win[yy, xx, 0:2 * M_IN, cols] + own_in[0, yy, xx, :, cols]
            ra, rb = pl.ds(0, M_IN), pl.ds(M_IN, M_IN)
            rcopy(win.at[BOTH, nx, ra, cols], win.at[2, BOTH, ra, cols], red_sem.at[SENT, 0], red_sem.at[R1, 0], to_x).start()
            rcopy(win.at[ny, BOTH, rb, cols], win.at[2, BOTH, rb, cols], red_sem.at[SENT, 0], red_sem.at[R1, 0], to_y).start()

    def own_load(t):
        rr, _, _ = spans(M_IN, t)
        return pltpu.make_async_copy(g_in.at[:, :, c, rr], own_in.at[lax.rem(t, 3)], red_sem.at[OWN, slot_of(0, t)])

    def raw_load(t):
        return pltpu.make_async_copy(g_out.at[pl.ds(aligned(RAW_STEP * t, SUB), RAW_STEP)], raw.at[lax.rem(t, 2)], red_sem.at[OWN, slot_of(1, t)])

    def pair_out(t):
        rr, _, _ = spans(M_OUT, t)
        return rcopy(packed.at[lax.rem(t, 2), :, :, nc], wpk.at[BOTH, :, rr], red_sem.at[DSS, slot_of(1, t)], red_sem.at[DSR, slot_of(1, t)], to_core)

    def start_in(t):
        own_load(t).start()
        pair_in(t).start()

    def pack_out(t):
        raw_load(t).wait()
        slot = lax.rem(t, 2)

        @pl.when(t >= 2)
        def _():
            pair_out(t - 2).wait_send()

        def unit(u, _):
            base = aligned(PART * u, SUB)
            tiles = [[raw[slot, pl.ds(base + SUB * k, SUB), LANE * i:LANE * i + LANE] for i in range(10)] for k in range(QUAD)]
            ln = lanes((SUB, LANE))
            for s in range(SUB):
                jj, first = s % QUAD, 5 * (s // QUAD) + s % QUAD
                tail = NO
                for k in range(QUAD):
                    lo, hi = tiles[k][first], tiles[k][first + 1]
                    head = lo if jj == 0 else pltpu.roll(jnp.where(ln >= PART * jj, lo, hi), LANE - PART * jj, 1)
                    packed[slot, s // QUAD, (s // 2) % 2, s % 2, pl.ds(aligned(SUB * u, SUB), SUB), LANE * k:LANE * k + LANE] = head
                    turn = (PART * (k - jj)) % LANE
                    part = hi if turn == 0 else pltpu.roll(hi, turn, 1)
                    tail = part if tail is NO else jnp.where(ln >= PART * k, part, tail)
                packed[slot, s // QUAD, (s // 2) % 2, s % 2, pl.ds(aligned(SUB * u, SUB), SUB), 512:640] = tail
            return 0

        lax.fori_loop(0, RAW_STEP // PART, unit, 0)
        pair_out(t).start()

        @pl.when(t + 2 < STEPS)
        def _():
            raw_load(t + 2).start()

    def reduce_first(ph, w, m, t):
        rr, _, _ = spans(m, t)
        if ph == 0:
            own_load(t).wait()
            pair_in(t).wait_recv()
            slot = lax.rem(t, 3)
            for yy in range(2):
                for xx in range(2):
                    for r in range(0, 2 * m, SUB):
                        rows = pl.ds(aligned(2 * m * t + r, SUB), SUB)
                        w[yy, xx, rows] = w[yy, xx, rows] + own_in[slot, yy, xx, r:r + SUB]
        else:
            pair_out(t).wait_recv()
            slot = lax.rem(t, 2)

            def add(i, _):
                rows = pl.ds(aligned(2 * m * t + SUB2 * i, SUB), SUB2)
                for yy in range(2):
                    for xx in range(2):
                        w[yy, xx, rows] = w[yy, xx, rows] + packed[slot, yy, xx, c, pl.ds(aligned(SUB2 * i, SUB), SUB2)]
                return 0

            lax.fori_loop(0, 2 * m // SUB2, add, 0)
        for copy in first_copies(ph, w, m, t):
            copy.start()

    def reduce_second(ph, w, m, t):
        _, ra, rb = spans(m, t)
        on_y, on_x = second_copies(ph, w, m, t)
        if ph == 0:
            pair_in(t).wait_send()
        wait_first(ph, w, m, t)
        w[ny, x, ra] = w[ny, x, ra] + w[2, ny, ra]
        on_y.start()
        w[y, nx, rb] = w[y, nx, rb] + w[2, nx, rb]
        on_x.start()

    def reduce_third(ph, w, m, t, gs):
        _, ra, rb = spans(m, t)
        wait_second(ph, w, m, t)
        ga = w[y, x, ra] + w[2, y, ra] + w[3, 0, ra]
        gs[ra] = ga
        gb = w[y, x, rb] + w[2, x, rb] + w[3, 0, rb]
        gs[rb] = gb
        wait_sent(ph, w, m, t)
        if ph == 0:
            sa, sb = ga * ga + 1e-30, gb * gb + 1e-30
            col_acc[...] = col_acc[...] + (sa + sb)
            for rows, sq in ((ra, sa), (rb, sb)):
                part = sq[:, 0:LANE]
                for i in range(1, COLS_IN // LANE):
                    part = part + sq[:, LANE * i:LANE * i + LANE]
                row_acc[rows] = part

    def sems(ph, t, send, recv):
        return red_sem.at[send, slot_of(2 + ph, t)], red_sem.at[recv, slot_of(2 + ph, t)]

    def pair_sems(ph, t, send):
        return red_sem.at[send, slot_of(2 + ph, t)], pair_sem.at[lax.rem(ph * STEPS + t, PAIR_SLOTS)]

    def gather_first(ph, w, m, t):
        rr, _, _ = spans(m, t)
        src = w.at[p, c, rr]
        rcopy(src, src, *sems(ph, t, SENT, R1), to_x).start()
        rcopy(src, src, *sems(ph, t, SENT, R1), to_y).start()
        rcopy(src, src, *pair_sems(ph, t, SENT), to_core).start()

    def gather_second(ph, w, m, t):
        rr, ra, rb = spans(m, t)
        both = w.at[BOTH, c, rr]
        rcopy(both, both, *sems(ph, t, SENT, R1), to_x).wait_recv()
        for other, rows, dev in ((p_x, rb, to_y), (p_y, ra, to_x)):
            rcopy(w.at[other, c, rows], w.at[other, c, rows], *sems(ph, t, ON, R2), dev).start()
            rcopy(w.at[other, c, rr], w.at[other, c, rr], *pair_sems(ph, t, ON), to_core).start()

    def gather_third(ph, w, m, t):
        rr, _, _ = spans(m, t)
        diag = w.at[p_d, c, rr]
        rcopy(diag, diag, *sems(ph, t, ON, R2), to_x).wait_recv()
        rcopy(diag, diag, *pair_sems(ph, t, ON), to_core).start()
        three = w.at[THREE, c, rr]
        rcopy(three, three, *sems(ph, t, SENT, R1), to_x).wait_send()

    def gather_last(ph, w, m, t):
        rr, _, _ = spans(m, t)
        four = w.at[:, nc, rr]
        rcopy(four, four, *pair_sems(ph, t, ON), to_core).wait_recv()
        rcopy(four, four, *pair_sems(ph, t, ON), to_core).wait_send()

    def z_share(src, dst, k):
        return rcopy(src, dst, ex_sem.at[k, ZS], ex_sem.at[k, ZR], to_z)

    def share(buf, k):
        copy = rcopy(buf.at[0], buf.at[1], ex_sem.at[k, CS], ex_sem.at[k, CR], to_core)
        copy.start()
        copy.wait()
        return buf[0] + buf[1]

    def to_chips(buf, k):
        for dev in (to_x, to_y, to_d):
            rcopy(buf.at[p], buf.at[p], ex_sem.at[k, TS], ex_sem.at[k, TR], dev).start()

    def from_chips(buf, k):
        three = buf.at[THREE]
        rcopy(three, three, ex_sem.at[k, TS], ex_sem.at[k, TR], to_x).wait()
        return buf[0] + buf[1] + buf[2] + buf[3]

    def halves(length):
        half = length // 2
        return pl.ds(aligned(c * half, LANE), half), pl.ds(aligned(nc * half, LANE), half)

    def vector_send(buf, chips, length):
        mine, other = halves(length)
        copy = rcopy(buf.at[0, :, other], buf.at[1, :, other], ex_sem.at[0, CS], ex_sem.at[0, CR], to_core)
        copy.start()
        copy.wait()
        chips[p] = buf[0, :, mine] + buf[1, :, mine]
        to_chips(chips, 0)

    def vector_take(chips, whole, length):
        mine, _ = halves(length)
        whole[:, mine] = from_chips(chips, 0)
        copy = rcopy(whole.at[:, mine], whole.at[:, mine], ex_sem.at[0, BS], ex_sem.at[0, BR], to_core)
        copy.start()
        copy.wait()

    def share_squares(acc, zt, pt, ct):
        zt[0] = jnp.sum(acc, axis=0, keepdims=True)
        copy = z_share(zt.at[0], zt.at[1], 1)
        copy.start()
        copy.wait()
        pt[0] = zt[0] + zt[1]
        ct[p] = share(pt, 1)
        to_chips(ct, 1)

    def scale_from(ct, count):
        mean = jnp.sum(from_chips(ct, 1), axis=1, keepdims=True) / count
        return 0.1 / jnp.maximum(1.0, jnp.sqrt(mean))

    def vec_loads():
        pairs = ((r_in_hbm, r_in), (c_in_hbm, c_in), (r_out_hbm, r_out), (c_out_hbm, c_out))
        return [pltpu.make_async_copy(src, dst, load_sem.at[QUAD + i]) for i, (src, dst) in enumerate(pairs)]

    def stats_in_send():
        for load in vec_loads():
            load.wait()
        copy = z_share(row_acc, row_peer, 0)
        copy.start()
        v_in[0, :, 0:COLS_IN] = jnp.sum(col_acc[...], axis=0, keepdims=True)
        copy.wait()
        row_mean = jnp.sum(row_acc[...] + row_peer[...], axis=1, keepdims=True) / cols_all_in
        row_mean = jnp.broadcast_to(row_mean, (ROWS_IN, LANE))
        r_old = jnp.concatenate([row_to_col(r_in[:, 0:LANE]), row_to_col(pad_lanes(r_in[:, LANE:WIDTH]))[0:PART]], axis=0)
        r_new = b2 * r_old + (1.0 - b2) * row_mean
        r_in_new[:, 0:LANE] = r_new[0:LANE].T[0:1]
        r_in_new[:, LANE:WIDTH] = jnp.concatenate([r_new[LANE:WIDTH], jnp.zeros((LANE - PART, LANE), F32)], axis=0).T[0:1, 0:PART]
        ai_in[...] = r_new
        v_in[0, :, COLS_IN:LEN_IN] = jnp.sum(r_new, axis=0, keepdims=True)
        vector_send(v_in, vc_in, LEN_IN)
        w_load_in().start()

    def w_load_in():
        return pltpu.make_async_copy(w_in.at[p, c], win.at[p, c], load_sem.at[0])

    def stats_in_norm():
        vector_take(vc_in, vf_in, LEN_IN)
        vec = vf_in[...]
        c_new = b2 * c_in[...] + (1.0 - b2) * (vec[:, 0:COLS_IN] / rows_all_in)
        c_in_new[...] = c_new
        bj_in[...] = 1.0 / jnp.sqrt(c_new)
        root_avg = jnp.sqrt(vec[:, COLS_IN:COLS_IN + 1] / rows_all_in)
        ai_in[...] = root_avg / jnp.sqrt(ai_in[...])

        def body(i, acc):
            rows = pl.ds(aligned(SUB * i, SUB), SUB)
            a = ai_in[rows]
            for k in range(COLS_IN // LANE):
                col = slice(LANE * k, LANE * k + LANE)
                u = gs_in[rows, col] * a * bj_in[:, col]
                acc = acc + u * u
            return acc

        share_squares(lax.fori_loop(0, ROWS_IN // SUB, body, jnp.zeros((SUB, LANE), F32)), zt_in, pt_in, ct_in)

    def update_in():
        scale = scale_from(ct_in, float(rows_all_in * cols_all_in))
        w_load_in().wait()
        m_load_in().wait()

        def body(i, _):
            rows = pl.ds(aligned(SUB2 * i, SUB2), SUB2)
            a = ai_in[rows] * scale
            for k in range(COLS_IN // LANE):
                col = slice(LANE * k, LANE * k + LANE)
                u = gs_in[rows, col] * a * bj_in[:, col]
                mom = (0.9 * m_in_new[rows, col].astype(F32) + u).astype(BF16)
                m_in_new[rows, col] = mom
                old = win[p, c, rows, col]
                win[p, c, rows, col] = old - lr * mom.astype(F32) - lr * wd * old
            return 0

        lax.fori_loop(0, ROWS_IN // SUB2, body, 0)

    def m_load_in():
        return pltpu.make_async_copy(m_in, m_in_new, load_sem.at[1])

    def block_out(t):
        heads, tails = [], []
        for u in range(QUAD):
            rows = pl.ds(aligned(PART * t + SUB * u, SUB), SUB)
            tail = gs_out[rows, 512:640]
            for k in range(QUAD):
                heads.append(gs_out[rows, LANE * k:LANE * k + LANE])
                tails.append(tail if k == 0 else pltpu.roll(tail, LANE - PART * k, 1))
        tails = jnp.concatenate(tails, axis=0)
        return jnp.concatenate(heads, axis=0), jnp.where(lanes((LANE, LANE)) < PART, tails, 0.0)

    def stats_out_send():
        def body(t, acc):
            head, tail = block_out(t)
            sh = head * head + 1e-30
            st = jnp.where(lanes((LANE, LANE)) < PART, tail * tail + 1e-30, 0.0)
            v_out[0, :, pl.ds(aligned(LANE * t, LANE), LANE)] = jnp.sum((sh + st).T, axis=0, keepdims=True)
            ah, at = acc
            for i in range(SUB2):
                ah = ah + sh[SUB * i:SUB * i + SUB]
                at = at + st[SUB * i:SUB * i + SUB]
            return ah, at

        zero = jnp.zeros((SUB, LANE), F32)
        ah, at = lax.fori_loop(0, TILES_OUT, body, (zero, zero))
        col_acc_out[0:SUB] = ah
        col_acc_out[SUB:SUB2] = at
        copy = z_share(col_acc_out, col_peer_out, 0)
        copy.start()
        copy.wait()
        v_out[0, :, RAW_OUT:LEN_OUT] = jnp.zeros((1, LANE), F32)
        vector_send(v_out, vc_out, LEN_OUT)

    def stats_out_norm():
        vector_take(vc_out, vf_out, LEN_OUT)
        vec = vf_out[...]
        r_new = b2 * r_out[...] + (1.0 - b2) * (vec[:, 0:RAW_OUT] / cols_all_out)
        r_out_new[...] = r_new
        part = r_new[:, 0:LANE]
        for i in range(1, TILES_OUT):
            part = part + r_new[:, LANE * i:LANE * i + LANE]
        zr[0] = part
        copy = rcopy(zr.at[0], zr.at[1], ex_sem.at[1, BS], ex_sem.at[1, BR], to_z)
        copy.start()
        copy.wait()
        root_avg = jnp.sqrt(jnp.sum(zr[0] + zr[1], axis=1, keepdims=True) / rows_all_out)
        cols = col_acc_out[...] + col_peer_out[...]
        c_new_h = b2 * c_out[:, 0:LANE] + (1.0 - b2) * (jnp.sum(cols[0:SUB], axis=0, keepdims=True) / rows_all_out)
        c_new_t = b2 * pad_lanes(c_out[:, LANE:WIDTH]) + (1.0 - b2) * (jnp.sum(cols[SUB:SUB2], axis=0, keepdims=True) / rows_all_out)
        c_out_new[:, 0:LANE] = c_new_h
        c_out_new[:, LANE:WIDTH] = c_new_t[:, 0:PART]
        vec_x[...] = jnp.broadcast_to(1.0 / jnp.sqrt(c_new_h), (SUB, LANE))
        vec_y[...] = jnp.broadcast_to(1.0 / jnp.sqrt(jnp.where(lanes((1, LANE)) < PART, c_new_t, 1.0)), (SUB, LANE))
        bh, bt = vec_x[0:1], vec_y[0:1]

        def body(t, acc):
            rows = pl.ds(aligned(LANE * t, LANE), LANE)
            a = row_to_col(root_avg / jnp.sqrt(r_out_new[:, rows]))
            ai_out[rows] = a
            head, tail = block_out(t)
            uh, ut = head * a * bh, tail * a * bt
            sq = uh * uh + ut * ut
            for i in range(SUB2):
                acc = acc + sq[SUB * i:SUB * i + SUB]
            return acc

        share_squares(lax.fori_loop(0, TILES_OUT, body, jnp.zeros((SUB, LANE), F32)), zt_out, pt_out, ct_out)

    def w_load_out():
        first = 5 * (q // QUAD) + j
        return pltpu.make_async_copy(w_out.at[:, pl.ds(aligned(LANE * first, LANE), 256)], w_cols, load_sem.at[2])

    def m_load_out():
        return pltpu.make_async_copy(m_out, m_out_new, load_sem.at[3])

    def update_out():
        scale = scale_from(ct_out, float(rows_all_out * cols_all_out))
        w_load_out().wait()
        m_load_out().wait()
        bh, bt = vec_x[0:1], vec_y[0:1]
        back = PART * ((QUAD - j) % QUAD)

        def body(t, _):
            rows = pl.ds(aligned(LANE * t, LANE), LANE)
            a = ai_out[rows] * scale
            head, tail = block_out(t)
            uh, ut = head * a * bh, tail * a * bt
            mom = m_out_new[:, rows].astype(F32)
            mh = (0.9 * mom[0:LANE].T + uh).astype(BF16).astype(F32)
            mt = (0.9 * jnp.concatenate([mom[LANE:WIDTH], jnp.zeros((96, LANE), F32)], axis=0).T + ut).astype(BF16).astype(F32)
            m_out_new[0:LANE, rows] = mh.T.astype(BF16)
            m_out_new[LANE:WIDTH, rows] = mt.T[0:PART].astype(BF16)
            lo, hi = w_cols[rows, 0:LANE], w_cols[rows, LANE:256]
            wh = pltpu.roll(jnp.where(lanes((LANE, LANE)) >= PART * j, lo, hi), back, 1)
            wt = pltpu.roll(hi, back, 1)
            wh = wh - lr * mh - lr * wd * wh
            wt = wt - lr * mt - lr * wd * wt
            ln = lanes((SUB, LANE))
            for u in range(QUAD):
                to = pl.ds(aligned(PART * t + SUB * u, SUB), SUB)
                joined = NO
                for k in range(QUAD):
                    at = PART * u + SUB * k
                    wpk[p, c, to, LANE * k:LANE * k + LANE] = wh[at:at + SUB]
                    part = wt[at:at + SUB] if k == 0 else pltpu.roll(wt[at:at + SUB], PART * k, 1)
                    joined = part if joined is NO else jnp.where(ln >= PART * k, part, joined)
                wpk[p, c, to, 512:640] = joined
            return 0

        lax.fori_loop(0, TILES_OUT, body, 0)

    col_acc[...] = jnp.zeros_like(col_acc)
    own_load(0).start()
    own_load(1).start()
    pl.semaphore_wait(barrier, QUAD)
    for k in range(len(PIECES) - 1):
        piece_in(k).start()
    pair_in(1).start()
    reduce_start()

    def at_step(cond, fn, *args):
        @pl.when(cond)
        def _():
            fn(*args)

    n = STEPS

    def step(s, _):
        def within(lo, hi):
            return jnp.logical_and(s >= lo, s < hi)

        at_step(s + 2 < n, start_in, s + 2)
        at_step(within(1, n), reduce_first, 0, win, M_IN, s)
        at_step(within(2, n + 2), reduce_second, 0, win, M_IN, s - 2)
        at_step(within(QUAD, n + QUAD), reduce_third, 0, win, M_IN, s - QUAD, gs_in)

        @pl.when(s == 2)
        def _():
            for copy in vec_loads():
                copy.start()
            m_load_in().start()
            m_load_out().start()
            w_load_out().start()

        @pl.when(s == n - 3)
        def _():
            raw_load(0).start()
            raw_load(1).start()

        at_step(within(n, 2 * n), reduce_first, 1, wpk, M_OUT, s - n)
        at_step(within(n - 1, 2 * n - 1), pack_out, s - n + 1)
        at_step(within(n + 2, 2 * n + 2), reduce_second, 1, wpk, M_OUT, s - n - 2)
        at_step(within(n + QUAD, 2 * n + QUAD), reduce_third, 1, wpk, M_OUT, s - n - QUAD, gs_out)
        at_step(s == n + 3, stats_in_send)
        at_step(s == n + 6, stats_in_norm)
        at_step(s == n + 9, update_in)
        at_step(within(2 * n, 3 * n), gather_first, 0, win, M_IN, s - 2 * n)
        at_step(within(2 * n + 2, 3 * n + 2), gather_second, 0, win, M_IN, s - 2 * n - 2)
        at_step(within(2 * n + QUAD, 3 * n + QUAD), gather_third, 0, win, M_IN, s - 2 * n - QUAD)
        at_step(s == 2 * n + 3, stats_out_send)
        at_step(s == 2 * n + 6, stats_out_norm)
        at_step(s == 2 * n + 9, update_out)
        at_step(within(3 * n, QUAD * n), gather_first, 1, wpk, M_OUT, s - 3 * n)
        at_step(within(3 * n + 2, QUAD * n + 2), gather_second, 1, wpk, M_OUT, s - 3 * n - 2)
        at_step(within(3 * n + QUAD, QUAD * n + QUAD), gather_third, 1, wpk, M_OUT, s - 3 * n - QUAD)
        at_step(within(2 * n + 6, 3 * n + 6), gather_last, 0, win, M_IN, s - 2 * n - 6)
        at_step(within(3 * n + 6, QUAD * n + 6), gather_last, 1, wpk, M_OUT, s - 3 * n - 6)
        return 0

    lax.fori_loop(0, QUAD * n + 6, step, 0)
    pair_out(n - 2).wait_send()
    pair_out(n - 1).wait_send()


def final_kernel(win, wpk, mi, mo, ri, ci, ro, co, win_o, wout_o, mi_o, mo_o, ri_o, ci_o, ro_o, co_o, stage, sem, stage_sem):
    def block(i):
        at = (i // QUAD, (i // 2) % 2, pl.ds(ROWS_IN // 2 * (i % 2), ROWS_IN // 2))
        return pltpu.make_async_copy(win.at[at], win_o.at[at], sem.at[6])

    for i in range(SUB2):
        block(i).start()
    plain = []
    for i, (src, dst) in enumerate(((mi, mi_o), (mo, mo_o), (ri, ri_o), (ci, ci_o), (ro, ro_o), (co, co_o))):
        plain.append(pltpu.make_async_copy(src, dst, sem.at[i]))
    for copy in plain:
        copy.start()

    def rows_of(t):
        return pl.ds(aligned(RAW_STEP * t, SUB), RAW_STEP)

    def put(t):
        return pltpu.make_async_copy(stage.at[rows_of(t)], wout_o.at[rows_of(t)], stage_sem)

    def chunk(t, _):
        def unit(u, _):
            ln = lanes((SUB, LANE))
            rows = pl.ds(aligned(2 * M_OUT * t + SUB * u, SUB), SUB)
            for half in range(2):
                tails = [wpk[2 * half + jj // 2, jj % 2, rows, 512:640] for jj in range(QUAD)]
                for k in range(QUAD):
                    to = pl.ds(aligned(RAW_STEP * t + PART * u + SUB * k, SUB), SUB)
                    heads = []
                    for jj in range(QUAD):
                        head = wpk[2 * half + jj // 2, jj % 2, rows, LANE * k:LANE * k + LANE]
                        heads.append(head if jj == 0 else pltpu.roll(head, PART * jj, 1))
                    ends = [tails[jj] if jj == k else pltpu.roll(tails[jj], (PART * (jj - k)) % LANE, 1) for jj in range(QUAD)]
                    for tile in range(5):
                        if tile == 0:
                            out = heads[0]
                        else:
                            out = ends[tile - 1]
                            if tile > 1:
                                out = jnp.where(ln < PART * (tile - 1), heads[tile - 1], out)
                            if tile < QUAD:
                                out = jnp.where(ln >= PART * tile, heads[tile], out)
                        at = LANE * (5 * half + tile)
                        stage[to, at:at + LANE] = out
            return 0

        lax.fori_loop(0, RAW_STEP // PART, unit, 0)
        put(t).start()
        return 0

    lax.fori_loop(0, STEPS, chunk, 0)
    pltpu.make_async_copy(stage, wout_o, stage_sem).wait()
    pltpu.make_async_copy(win, win_o, sem.at[6]).wait()
    for copy in plain:
        copy.wait()


def solution(mesh):
    n_tp = mesh.shape['tp']
    n_dp = mesh.shape['dp']
    vmem = pl.BlockSpec(memory_space=pltpu.VMEM)
    hbm = pl.BlockSpec(memory_space=pltpu.HBM)
    smem = pl.BlockSpec(memory_space=pltpu.SMEM)
    dma = pltpu.SemaphoreType.DMA
    kept = (
        ((QUAD, 2, ROWS_IN, COLS_IN), F32),
        ((QUAD, 2, ROWS_OUT, COLS_OUT), F32),
        ((ROWS_IN, COLS_IN), BF16),
        ((WIDTH, RAW_OUT), BF16),
        ((1, ROWS_IN), F32),
        ((1, COLS_IN), F32),
        ((1, RAW_OUT), F32),
        ((1, WIDTH), F32),
    )
    main = pl.pallas_call(
        functools.partial(main_kernel, n_tp, n_dp, D, COLS_IN * n_tp, RAW_OUT * n_tp, D),
        out_shape=[pltpu.VMEM(shape, dtype) for shape, dtype in kept],
        in_specs=[hbm] * 6 + [hbm] * QUAD + [smem] * 3,
        out_specs=[vmem] * SUB,
        scratch_shapes=[
            pltpu.VMEM((3, 2, 2, 2 * M_IN, COLS_IN), F32),
            pltpu.VMEM((2, RAW_STEP, D), F32),
            pltpu.VMEM((2, 2, 2, 2, 2 * M_OUT, COLS_OUT), F32),
            pltpu.VMEM((ROWS_IN, COLS_IN), F32),
            pltpu.VMEM((ROWS_OUT, COLS_OUT), F32),
            pltpu.VMEM((RAW_OUT, 256), F32),
            pltpu.VMEM((RAW_OUT, LANE), F32),
            pltpu.VMEM((ROWS_IN, LANE), F32),
            pltpu.VMEM((1, COLS_IN), F32),
            pltpu.VMEM((SUB, LANE), F32),
            pltpu.VMEM((SUB, LANE), F32),
            pltpu.VMEM((SUB, COLS_IN), F32),
            pltpu.VMEM((ROWS_IN, LANE), F32),
            pltpu.VMEM((ROWS_IN, LANE), F32),
            pltpu.VMEM((SUB2, LANE), F32),
            pltpu.VMEM((SUB2, LANE), F32),
            pltpu.VMEM((2, 1, LEN_IN), F32),
            pltpu.VMEM((QUAD, 1, LEN_IN // 2), F32),
            pltpu.VMEM((1, LEN_IN), F32),
            pltpu.VMEM((2, 1, LEN_OUT), F32),
            pltpu.VMEM((QUAD, 1, LEN_OUT // 2), F32),
            pltpu.VMEM((1, LEN_OUT), F32),
            pltpu.VMEM((1, ROWS_IN), F32),
            pltpu.VMEM((1, COLS_IN), F32),
            pltpu.VMEM((1, RAW_OUT), F32),
            pltpu.VMEM((1, WIDTH), F32),
            pltpu.VMEM((2, 1, LANE), F32),
        ] + [pltpu.VMEM((i, 1, LANE), F32) for i in (2, 2, QUAD)] * 2 + [
            dma((N_RED, SLOTS)),
            dma((PAIR_SLOTS,)),
            dma((2 * QUAD,)),
            dma((2, N_EX)),
        ],
        compiler_params=pltpu.CompilerParams(collective_id=0, has_side_effects=True, vmem_limit_bytes=GRANT),
    )
    final = pl.pallas_call(
        final_kernel,
        out_shape=[
            jax.ShapeDtypeStruct((QUAD, 2, ROWS_IN, COLS_IN), F32),
            jax.ShapeDtypeStruct((RAW_OUT, D), F32),
        ] + [jax.ShapeDtypeStruct(shape, dtype) for shape, dtype in kept[2:]],
        in_specs=[vmem] * SUB,
        out_specs=[hbm] * SUB,
        scratch_shapes=[pltpu.VMEM((RAW_OUT, D), F32), dma((7,)), dma],
        compiler_params=pltpu.CompilerParams(vmem_limit_bytes=GRANT),
    )

    def body(w_in, w_out, g_in, g_out, m_in, m_out, r_in, c_in, r_out, c_out, learn_rate, weight_decay, beta_two):
        shards = (QUAD, 2, ROWS_IN, COLS_IN)
        got = main(
            w_in.reshape(shards), w_out[0], g_in.reshape((2, 2, 2, ROWS_IN, COLS_IN)), g_out[0, 0], m_in[0], m_out[0].T,
            r_in, c_in, r_out, c_out, learn_rate.reshape(1), weight_decay.reshape(1), beta_two.reshape(1))
        w_i, w_o, m_i, m_o, r_i, c_i, r_o, c_o = final(*[pltpu.with_memory_space_constraint(g, pltpu.VMEM) for g in got])
        return w_i.reshape((1, D, COLS_IN)), w_o[NO], m_i[NO], m_o.T[NO], r_i, c_i, r_o, c_o

    in_specs = (P(NO, NO, 'tp'), P(NO, 'tp', NO), P('dp', NO, NO, 'tp'), P('dp', NO, 'tp', NO), P(NO, 'dp', 'tp'), P(NO, 'tp', 'dp'), P(NO, 'dp'), P(NO, 'tp'), P(NO, 'tp'), P(NO, 'dp'), P(), P(), P())
    out_specs = (P(NO, NO, 'tp'), P(NO, 'tp', NO), P(NO, 'dp', 'tp'), P(NO, 'tp', 'dp'), P(NO, 'dp'), P(NO, 'tp'), P(NO, 'tp'), P(NO, 'dp'))
    return jax.shard_map(body, mesh=mesh, in_specs=in_specs, out_specs=out_specs, check_vma=False)
```

```python
import functools

import jax
import jax.numpy as jnp
from jax import lax
from jax.experimental import pallas as pl
from jax.experimental.pallas import tpu as pltpu
from jax.sharding import PartitionSpec as P

F32 = jnp.float32
BF16 = jnp.bfloat16
MESH = pl.DeviceIdType.MESH
LANE, SUB, SUB2, PART, QUAD, WIDTH = 128, 8, 16, 32, 4, 160
NO = None
BOTH, THREE = pl.ds(0, 2), pl.ds(0, 3)

D = 1280
ROWS_IN, COLS_IN = WIDTH, 4480
ROWS_OUT, COLS_OUT = 800, 640
RAW_OUT = 3200
STEPS = 10
M_IN = ROWS_IN // STEPS // 2
M_OUT = ROWS_OUT // STEPS // 2
RAW_STEP = RAW_OUT // STEPS
TILES_OUT = RAW_OUT // LANE

GRANT = 24 << 20

SLOTS, PAIR_SLOTS = 6, 10
N_RED, N_EX = 6, 8
(OWN, DSS, DSR, SENT, R1, R2) = range(N_RED)
ON = DSS
(ZS, ZR, CS, CR, TS, TR, BS, BR) = range(N_EX)
PIECES = (0, 1, 3, 7, 13, 20, 27, COLS_IN // LANE)
LEN_IN, LEN_OUT = COLS_IN + LANE, RAW_OUT + LANE

def lanes(shape):
    return lax.broadcasted_iota(jnp.int32, shape, 1)


def aligned(value, by):
    return pl.multiple_of(value, by)


def pad_lanes(row):
    return jnp.concatenate([row, jnp.zeros((1, LANE - row.shape[1]), F32)], axis=1)


def row_to_col(row):
    return jnp.broadcast_to(row, (LANE, LANE)).T


def main_kernel(n_tp, n_dp, rows_all_in, cols_all_in, rows_all_out, cols_all_out,
                w_in, w_out, g_in, g_out, m_in, m_out, r_in_hbm, c_in_hbm, r_out_hbm, c_out_hbm, lr_ref, wd_ref, b2_ref,
                win, wpk, m_in_new, m_out_new, r_in_new, c_in_new, r_out_new, c_out_new,
                own_in, raw, packed, gs_in, gs_out, w_cols, ai_out, ai_in, bj_in, vec_x, vec_y,
                col_acc, row_acc, row_peer, col_acc_out, col_peer_out, v_in, vc_in, vf_in, v_out, vc_out, vf_out,
                r_in, c_in, r_out, c_out, zr, zt_in, pt_in, ct_in, zt_out, pt_out, ct_out,
                red_sem, pair_sem, load_sem, ex_sem):
    tp = lax.axis_index('tp')
    q = lax.axis_index('dp')
    p, c = q // 2, q % 2
    y, x = p // 2, p % 2
    nx, ny, nc = 1 - x, 1 - y, 1 - c
    p_x, p_y, p_d = 2 * y + nx, 2 * ny + x, 2 * ny + nx
    to_x = {'dp': 2 * p_x + c}
    to_y = {'dp': 2 * p_y + c}
    to_d = {'dp': 2 * p_d + c}
    to_core = {'dp': 2 * p + nc}
    to_z = {'tp': 1 - tp}
    j = q % QUAD
    lr, wd, b2 = lr_ref[0], wd_ref[0], b2_ref[0]

    barrier = pltpu.get_barrier_semaphore()
    for dev in (to_x, to_y, to_core, to_z):
        pl.semaphore_signal(barrier, inc=1, device_id=dev, device_id_type=MESH)

    def rcopy(src, dst, send, recv, dev):
        return pltpu.make_async_remote_copy(src_ref=src, dst_ref=dst, send_sem=send, recv_sem=recv, device_id=dev, device_id_type=MESH)

    def slot_of(ph, t):
        return lax.rem(ph * STEPS + t, SLOTS)

    def spans(m, t):
        base = aligned(2 * m * t, SUB)
        return pl.ds(base, 2 * m), pl.ds(base, m), pl.ds(aligned(base + m, SUB), m)

    def first_copies(ph, w, m, t):
        _, ra, rb = spans(m, t)
        a = rcopy(w.at[BOTH, nx, ra], w.at[2, BOTH, ra], red_sem.at[SENT, slot_of(ph, t)], red_sem.at[R1, slot_of(ph, t)], to_x)
        b = rcopy(w.at[ny, BOTH, rb], w.at[2, BOTH, rb], red_sem.at[SENT, slot_of(ph, t)], red_sem.at[R1, slot_of(ph, t)], to_y)
        return a, b

    def second_copies(ph, w, m, t):
        _, ra, rb = spans(m, t)
        a = rcopy(w.at[ny, x, ra], w.at[3, 0, ra], red_sem.at[SENT, slot_of(ph, t)], red_sem.at[R2, slot_of(ph, t)], to_y)
        b = rcopy(w.at[y, nx, rb], w.at[3, 0, rb], red_sem.at[SENT, slot_of(ph, t)], red_sem.at[R2, slot_of(ph, t)], to_x)
        return a, b

    def wait_first(ph, w, m, t):
        rr, _, _ = spans(m, t)
        part = w.at[2, BOTH, rr]
        rcopy(part, part, red_sem.at[SENT, slot_of(ph, t)], red_sem.at[R1, slot_of(ph, t)], to_x).wait_recv()

    def wait_second(ph, w, m, t):
        rr, _, _ = spans(m, t)
        part = w.at[3, 0, rr]
        rcopy(part, part, red_sem.at[SENT, slot_of(ph, t)], red_sem.at[R2, slot_of(ph, t)], to_y).wait_recv()

    def wait_sent(ph, w, m, t):
        rr, _, _ = spans(m, t)
        part = w.at[THREE, 0, rr]
        rcopy(part, part, red_sem.at[SENT, slot_of(ph, t)], red_sem.at[R1, slot_of(ph, t)], to_x).wait_send()

    def pair_in(t):
        rr, _, _ = spans(M_IN, t)
        return rcopy(g_in.at[:, :, nc, rr], win.at[BOTH, :, rr], red_sem.at[DSS, slot_of(0, t)], red_sem.at[DSR, slot_of(0, t)], to_core)

    def piece(k):
        return pl.ds(LANE * PIECES[k], LANE * (PIECES[k + 1] - PIECES[k]))

    def piece_in(k):
        rows, cols = pl.ds(0, 2 * M_IN), piece(k)
        return rcopy(g_in.at[:, :, nc, rows, cols], win.at[BOTH, :, rows, cols], red_sem.at[DSS, 0], load_sem.at[k], to_core)

    def reduce_start():
        own_load(0).wait()
        for k in range(len(PIECES) - 1):
            cols = piece(k)
            piece_in(k).wait_recv()
            for yy in range(2):
                for xx in range(2):
                    win[yy, xx, 0:2 * M_IN, cols] = win[yy, xx, 0:2 * M_IN, cols] + own_in[0, yy, xx, :, cols]
            ra, rb = pl.ds(0, M_IN), pl.ds(M_IN, M_IN)
            rcopy(win.at[BOTH, nx, ra, cols], win.at[2, BOTH, ra, cols], red_sem.at[SENT, 0], red_sem.at[R1, 0], to_x).start()
            rcopy(win.at[ny, BOTH, rb, cols], win.at[2, BOTH, rb, cols], red_sem.at[SENT, 0], red_sem.at[R1, 0], to_y).start()

    def own_load(t):
        rr, _, _ = spans(M_IN, t)
        return pltpu.make_async_copy(g_in.at[:, :, c, rr], own_in.at[lax.rem(t, 3)], red_sem.at[OWN, slot_of(0, t)])

    def raw_load(t):
        return pltpu.make_async_copy(g_out.at[pl.ds(aligned(RAW_STEP * t, SUB), RAW_STEP)], raw.at[lax.rem(t, 2)], red_sem.at[OWN, slot_of(1, t)])

    def pair_out(t):
        rr, _, _ = spans(M_OUT, t)
        return rcopy(packed.at[lax.rem(t, 2), :, :, nc], wpk.at[BOTH, :, rr], red_sem.at[DSS, slot_of(1, t)], red_sem.at[DSR, slot_of(1, t)], to_core)

    def start_in(t):
        own_load(t).start()
        pair_in(t).start()

    def pack_out(t):
        raw_load(t).wait()
        slot = lax.rem(t, 2)

        @pl.when(t >= 2)
        def _():
            pair_out(t - 2).wait_send()

        def unit(u, _):
            base = aligned(PART * u, SUB)
            tiles = [[raw[slot, pl.ds(base + SUB * k, SUB), LANE * i:LANE * i + LANE] for i in range(10)] for k in range(QUAD)]
            ln = lanes((SUB, LANE))
            for s in range(SUB):
                jj, first = s % QUAD, 5 * (s // QUAD) + s % QUAD
                tail = NO
                for k in range(QUAD):
                    lo, hi = tiles[k][first], tiles[k][first + 1]
                    head = lo if jj == 0 else pltpu.roll(jnp.where(ln >= PART * jj, lo, hi), LANE - PART * jj, 1)
                    packed[slot, s // QUAD, (s // 2) % 2, s % 2, pl.ds(aligned(SUB * u, SUB), SUB), LANE * k:LANE * k + LANE] = head
                    turn = (PART * (k - jj)) % LANE
                    part = hi if turn == 0 else pltpu.roll(hi, turn, 1)
                    tail = part if tail is NO else jnp.where(ln >= PART * k, part, tail)
                packed[slot, s // QUAD, (s // 2) % 2, s % 2, pl.ds(aligned(SUB * u, SUB), SUB), 512:640] = tail
            return 0

        lax.fori_loop(0, RAW_STEP // PART, unit, 0)
        pair_out(t).start()

        @pl.when(t + 2 < STEPS)
        def _():
            raw_load(t + 2).start()

    def reduce_first(ph, w, m, t):
        rr, _, _ = spans(m, t)
        if ph == 0:
            own_load(t).wait()
            pair_in(t).wait_recv()
            slot = lax.rem(t, 3)
            for yy in range(2):
                for xx in range(2):
                    for r in range(0, 2 * m, SUB):
                        rows = pl.ds(aligned(2 * m * t + r, SUB), SUB)
                        w[yy, xx, rows] = w[yy, xx, rows] + own_in[slot, yy, xx, r:r + SUB]
        else:
            pair_out(t).wait_recv()
            slot = lax.rem(t, 2)

            def add(i, _):
                rows = pl.ds(aligned(2 * m * t + SUB2 * i, SUB), SUB2)
                for yy in range(2):
                    for xx in range(2):
                        w[yy, xx, rows] = w[yy, xx, rows] + packed[slot, yy, xx, c, pl.ds(aligned(SUB2 * i, SUB), SUB2)]
                return 0

            lax.fori_loop(0, 2 * m // SUB2, add, 0)
        for copy in first_copies(ph, w, m, t):
            copy.start()

    def reduce_second(ph, w, m, t):
        _, ra, rb = spans(m, t)
        on_y, on_x = second_copies(ph, w, m, t)
        if ph == 0:
            pair_in(t).wait_send()
        wait_first(ph, w, m, t)
        w[ny, x, ra] = w[ny, x, ra] + w[2, ny, ra]
        on_y.start()
        w[y, nx, rb] = w[y, nx, rb] + w[2, nx, rb]
        on_x.start()

    def reduce_third(ph, w, m, t, gs):
        _, ra, rb = spans(m, t)
        wait_second(ph, w, m, t)
        ga = w[y, x, ra] + w[2, y, ra] + w[3, 0, ra]
        gs[ra] = ga
        gb = w[y, x, rb] + w[2, x, rb] + w[3, 0, rb]
        gs[rb] = gb
        wait_sent(ph, w, m, t)
        if ph == 0:
            sa, sb = ga * ga + 1e-30, gb * gb + 1e-30
            col_acc[...] = col_acc[...] + (sa + sb)
            for rows, sq in ((ra, sa), (rb, sb)):
                part = sq[:, 0:LANE]
                for i in range(1, COLS_IN // LANE):
                    part = part + sq[:, LANE * i:LANE * i + LANE]
                row_acc[rows] = part

    def sems(ph, t, send, recv):
        return red_sem.at[send, slot_of(2 + ph, t)], red_sem.at[recv, slot_of(2 + ph, t)]

    def pair_sems(ph, t, send):
        return red_sem.at[send, slot_of(2 + ph, t)], pair_sem.at[lax.rem(ph * STEPS + t, PAIR_SLOTS)]

    def gather_first(ph, w, m, t):
        rr, _, _ = spans(m, t)
        src = w.at[p, c, rr]
        rcopy(src, src, *sems(ph, t, SENT, R1), to_x).start()
        rcopy(src, src, *sems(ph, t, SENT, R1), to_y).start()
        rcopy(src, src, *pair_sems(ph, t, SENT), to_core).start()

    def gather_second(ph, w, m, t):
        rr, ra, rb = spans(m, t)
        both = w.at[BOTH, c, rr]
        rcopy(both, both, *sems(ph, t, SENT, R1), to_x).wait_recv()
        for other, rows, dev in ((p_x, rb, to_y), (p_y, ra, to_x)):
            rcopy(w.at[other, c, rows], w.at[other, c, rows], *sems(ph, t, ON, R2), dev).start()
            rcopy(w.at[other, c, rr], w.at[other, c, rr], *pair_sems(ph, t, ON), to_core).start()

    def gather_third(ph, w, m, t):
        rr, _, _ = spans(m, t)
        diag = w.at[p_d, c, rr]
        rcopy(diag, diag, *sems(ph, t, ON, R2), to_x).wait_recv()
        rcopy(diag, diag, *pair_sems(ph, t, ON), to_core).start()
        three = w.at[THREE, c, rr]
        rcopy(three, three, *sems(ph, t, SENT, R1), to_x).wait_send()

    def gather_last(ph, w, m, t):
        rr, _, _ = spans(m, t)
        four = w.at[:, nc, rr]
        rcopy(four, four, *pair_sems(ph, t, ON), to_core).wait_recv()
        rcopy(four, four, *pair_sems(ph, t, ON), to_core).wait_send()

    def z_share(src, dst, k):
        return rcopy(src, dst, ex_sem.at[k, ZS], ex_sem.at[k, ZR], to_z)

    def share(buf, k):
        copy = rcopy(buf.at[0], buf.at[1], ex_sem.at[k, CS], ex_sem.at[k, CR], to_core)
        copy.start()
        copy.wait()
        return buf[0] + buf[1]

    def to_chips(buf, k):
        for dev in (to_x, to_y, to_d):
            rcopy(buf.at[p], buf.at[p], ex_sem.at[k, TS], ex_sem.at[k, TR], dev).start()

    def from_chips(buf, k):
        three = buf.at[THREE]
        rcopy(three, three, ex_sem.at[k, TS], ex_sem.at[k, TR], to_x).wait()
        return buf[0] + buf[1] + buf[2] + buf[3]

    def halves(length):
        half = length // 2
        return pl.ds(aligned(c * half, LANE), half), pl.ds(aligned(nc * half, LANE), half)

    def vector_send(buf, chips, length):
        mine, other = halves(length)
        copy = rcopy(buf.at[0, :, other], buf.at[1, :, other], ex_sem.at[0, CS], ex_sem.at[0, CR], to_core)
        copy.start()
        copy.wait()
        chips[p] = buf[0, :, mine] + buf[1, :, mine]
        to_chips(chips, 0)

    def vector_take(chips, whole, length):
        mine, _ = halves(length)
        whole[:, mine] = from_chips(chips, 0)
        copy = rcopy(whole.at[:, mine], whole.at[:, mine], ex_sem.at[0, BS], ex_sem.at[0, BR], to_core)
        copy.start()
        copy.wait()

    def share_squares(acc, zt, pt, ct):
        zt[0] = jnp.sum(acc, axis=0, keepdims=True)
        copy = z_share(zt.at[0], zt.at[1], 1)
        copy.start()
        copy.wait()
        pt[0] = zt[0] + zt[1]
        ct[p] = share(pt, 1)
        to_chips(ct, 1)

    def scale_from(ct, count):
        mean = jnp.sum(from_chips(ct, 1), axis=1, keepdims=True) / count
        return 0.1 / jnp.maximum(1.0, jnp.sqrt(mean))

    def vec_loads():
        pairs = ((r_in_hbm, r_in), (c_in_hbm, c_in), (r_out_hbm, r_out), (c_out_hbm, c_out))
        return [pltpu.make_async_copy(src, dst, load_sem.at[QUAD + i]) for i, (src, dst) in enumerate(pairs)]

    def stats_in_send():
        for load in vec_loads():
            load.wait()
        copy = z_share(row_acc, row_peer, 0)
        copy.start()
        v_in[0, :, 0:COLS_IN] = jnp.sum(col_acc[...], axis=0, keepdims=True)
        copy.wait()
        row_mean = jnp.sum(row_acc[...] + row_peer[...], axis=1, keepdims=True) / cols_all_in
        row_mean = jnp.broadcast_to(row_mean, (ROWS_IN, LANE))
        r_old = jnp.concatenate([row_to_col(r_in[:, 0:LANE]), row_to_col(pad_lanes(r_in[:, LANE:WIDTH]))[0:PART]], axis=0)
        r_new = b2 * r_old + (1.0 - b2) * row_mean
        r_in_new[:, 0:LANE] = r_new[0:LANE].T[0:1]
        r_in_new[:, LANE:WIDTH] = jnp.concatenate([r_new[LANE:WIDTH], jnp.zeros((LANE - PART, LANE), F32)], axis=0).T[0:1, 0:PART]
        ai_in[...] = r_new
        v_in[0, :, COLS_IN:LEN_IN] = jnp.sum(r_new, axis=0, keepdims=True)
        vector_send(v_in, vc_in, LEN_IN)
        w_load_in().start()

    def w_load_in():
        return pltpu.make_async_copy(w_in.at[p, c], win.at[p, c], load_sem.at[0])

    def stats_in_norm():
        vector_take(vc_in, vf_in, LEN_IN)
        vec = vf_in[...]
        c_new = b2 * c_in[...] + (1.0 - b2) * (vec[:, 0:COLS_IN] / rows_all_in)
        c_in_new[...] = c_new
        bj_in[...] = 1.0 / jnp.sqrt(c_new)
        root_avg = jnp.sqrt(vec[:, COLS_IN:COLS_IN + 1] / rows_all_in)
        ai_in[...] = root_avg / jnp.sqrt(ai_in[...])

        def body(i, acc):
            rows = pl.ds(aligned(SUB * i, SUB), SUB)
            a = ai_in[rows]
            for k in range(COLS_IN // LANE):
                col = slice(LANE * k, LANE * k + LANE)
                u = gs_in[rows, col] * a * bj_in[:, col]
                acc = acc + u * u
            return acc

        share_squares(lax.fori_loop(0, ROWS_IN // SUB, body, jnp.zeros((SUB, LANE), F32)), zt_in, pt_in, ct_in)

    def update_in():
        scale = scale_from(ct_in, float(rows_all_in * cols_all_in))
        w_load_in().wait()
        m_load_in().wait()

        def body(i, _):
            rows = pl.ds(aligned(SUB2 * i, SUB2), SUB2)
            a = ai_in[rows] * scale
            for k in range(COLS_IN // LANE):
                col = slice(LANE * k, LANE * k + LANE)
                u = gs_in[rows, col] * a * bj_in[:, col]
                mom = (0.9 * m_in_new[rows, col].astype(F32) + u).astype(BF16)
                m_in_new[rows, col] = mom
                old = win[p, c, rows, col]
                win[p, c, rows, col] = old - lr * mom.astype(F32) - lr * wd * old
            return 0

        lax.fori_loop(0, ROWS_IN // SUB2, body, 0)

    def m_load_in():
        return pltpu.make_async_copy(m_in, m_in_new, load_sem.at[1])

    def block_out(t):
        heads, tails = [], []
        for u in range(QUAD):
            rows = pl.ds(aligned(PART * t + SUB * u, SUB), SUB)
            tail = gs_out[rows, 512:640]
            for k in range(QUAD):
                heads.append(gs_out[rows, LANE * k:LANE * k + LANE])
                tails.append(tail if k == 0 else pltpu.roll(tail, LANE - PART * k, 1))
        tails = jnp.concatenate(tails, axis=0)
        return jnp.concatenate(heads, axis=0), jnp.where(lanes((LANE, LANE)) < PART, tails, 0.0)

    def stats_out_send():
        def body(t, acc):
            head, tail = block_out(t)
            sh = head * head + 1e-30
            st = jnp.where(lanes((LANE, LANE)) < PART, tail * tail + 1e-30, 0.0)
            v_out[0, :, pl.ds(aligned(LANE * t, LANE), LANE)] = jnp.sum((sh + st).T, axis=0, keepdims=True)
            ah, at = acc
            for i in range(SUB2):
                ah = ah + sh[SUB * i:SUB * i + SUB]
                at = at + st[SUB * i:SUB * i + SUB]
            return ah, at

        zero = jnp.zeros((SUB, LANE), F32)
        ah, at = lax.fori_loop(0, TILES_OUT, body, (zero, zero))
        col_acc_out[0:SUB] = ah
        col_acc_out[SUB:SUB2] = at
        copy = z_share(col_acc_out, col_peer_out, 0)
        copy.start()
        copy.wait()
        v_out[0, :, RAW_OUT:LEN_OUT] = jnp.zeros((1, LANE), F32)
        vector_send(v_out, vc_out, LEN_OUT)

    def stats_out_norm():
        vector_take(vc_out, vf_out, LEN_OUT)
        vec = vf_out[...]
        r_new = b2 * r_out[...] + (1.0 - b2) * (vec[:, 0:RAW_OUT] / cols_all_out)
        r_out_new[...] = r_new
        part = r_new[:, 0:LANE]
        for i in range(1, TILES_OUT):
            part = part + r_new[:, LANE * i:LANE * i + LANE]
        zr[0] = part
        copy = rcopy(zr.at[0], zr.at[1], ex_sem.at[1, BS], ex_sem.at[1, BR], to_z)
        copy.start()
        copy.wait()
        root_avg = jnp.sqrt(jnp.sum(zr[0] + zr[1], axis=1, keepdims=True) / rows_all_out)
        cols = col_acc_out[...] + col_peer_out[...]
        c_new_h = b2 * c_out[:, 0:LANE] + (1.0 - b2) * (jnp.sum(cols[0:SUB], axis=0, keepdims=True) / rows_all_out)
        c_new_t = b2 * pad_lanes(c_out[:, LANE:WIDTH]) + (1.0 - b2) * (jnp.sum(cols[SUB:SUB2], axis=0, keepdims=True) / rows_all_out)
        c_out_new[:, 0:LANE] = c_new_h
        c_out_new[:, LANE:WIDTH] = c_new_t[:, 0:PART]
        vec_x[...] = jnp.broadcast_to(1.0 / jnp.sqrt(c_new_h), (SUB, LANE))
        vec_y[...] = jnp.broadcast_to(1.0 / jnp.sqrt(jnp.where(lanes((1, LANE)) < PART, c_new_t, 1.0)), (SUB, LANE))
        bh, bt = vec_x[0:1], vec_y[0:1]

        def body(t, acc):
            rows = pl.ds(aligned(LANE * t, LANE), LANE)
            a = row_to_col(root_avg / jnp.sqrt(r_out_new[:, rows]))
            ai_out[rows] = a
            head, tail = block_out(t)
            uh, ut = head * a * bh, tail * a * bt
            sq = uh * uh + ut * ut
            for i in range(SUB2):
                acc = acc + sq[SUB * i:SUB * i + SUB]
            return acc

        share_squares(lax.fori_loop(0, TILES_OUT, body, jnp.zeros((SUB, LANE), F32)), zt_out, pt_out, ct_out)

    def w_load_out():
        first = 5 * (q // QUAD) + j
        return pltpu.make_async_copy(w_out.at[:, pl.ds(aligned(LANE * first, LANE), 256)], w_cols, load_sem.at[2])

    def m_load_out():
        return pltpu.make_async_copy(m_out, m_out_new, load_sem.at[3])

    def update_out():
        scale = scale_from(ct_out, float(rows_all_out * cols_all_out))
        w_load_out().wait()
        m_load_out().wait()
        bh, bt = vec_x[0:1], vec_y[0:1]
        back = PART * ((QUAD - j) % QUAD)

        def body(t, _):
            rows = pl.ds(aligned(LANE * t, LANE), LANE)
            a = ai_out[rows] * scale
            head, tail = block_out(t)
            uh, ut = head * a * bh, tail * a * bt
            mom = m_out_new[:, rows].astype(F32)
            mh = (0.9 * mom[0:LANE].T + uh).astype(BF16).astype(F32)
            mt = (0.9 * jnp.concatenate([mom[LANE:WIDTH], jnp.zeros((96, LANE), F32)], axis=0).T + ut).astype(BF16).astype(F32)
            m_out_new[0:LANE, rows] = mh.T.astype(BF16)
            m_out_new[LANE:WIDTH, rows] = mt.T[0:PART].astype(BF16)
            lo, hi = w_cols[rows, 0:LANE], w_cols[rows, LANE:256]
            wh = pltpu.roll(jnp.where(lanes((LANE, LANE)) >= PART * j, lo, hi), back, 1)
            wt = pltpu.roll(hi, back, 1)
            wh = wh - lr * mh - lr * wd * wh
            wt = wt - lr * mt - lr * wd * wt
            ln = lanes((SUB, LANE))
            for u in range(QUAD):
                to = pl.ds(aligned(PART * t + SUB * u, SUB), SUB)
                joined = NO
                for k in range(QUAD):
                    at = PART * u + SUB * k
                    wpk[p, c, to, LANE * k:LANE * k + LANE] = wh[at:at + SUB]
                    part = wt[at:at + SUB] if k == 0 else pltpu.roll(wt[at:at + SUB], PART * k, 1)
                    joined = part if joined is NO else jnp.where(ln >= PART * k, part, joined)
                wpk[p, c, to, 512:640] = joined
            return 0

        lax.fori_loop(0, TILES_OUT, body, 0)

    col_acc[...] = jnp.zeros_like(col_acc)
    own_load(0).start()
    own_load(1).start()
    pl.semaphore_wait(barrier, QUAD)
    for k in range(len(PIECES) - 1):
        piece_in(k).start()
    pair_in(1).start()
    reduce_start()

    def at_step(cond, fn, *args):
        @pl.when(cond)
        def _():
            fn(*args)

    n = STEPS

    def step(s, _):
        def within(lo, hi):
            return jnp.logical_and(s >= lo, s < hi)

        at_step(s + 2 < n, start_in, s + 2)
        at_step(within(1, n), reduce_first, 0, win, M_IN, s)
        at_step(within(2, n + 2), reduce_second, 0, win, M_IN, s - 2)
        at_step(within(QUAD, n + QUAD), reduce_third, 0, win, M_IN, s - QUAD, gs_in)

        @pl.when(s == 2)
        def _():
            for copy in vec_loads():
                copy.start()
            m_load_in().start()
            m_load_out().start()
            w_load_out().start()

        @pl.when(s == n - 3)
        def _():
            raw_load(0).start()
            raw_load(1).start()

        at_step(within(n, 2 * n), reduce_first, 1, wpk, M_OUT, s - n)
        at_step(within(n - 1, 2 * n - 1), pack_out, s - n + 1)
        at_step(within(n + 2, 2 * n + 2), reduce_second, 1, wpk, M_OUT, s - n - 2)
        at_step(within(n + QUAD, 2 * n + QUAD), reduce_third, 1, wpk, M_OUT, s - n - QUAD, gs_out)
        at_step(within(2 * n, 2 * n + 2), lambda t: pair_out(t).wait_send(), s - n - 2)
        at_step(s == n + 3, stats_in_send)
        at_step(s == n + 6, stats_in_norm)
        at_step(s == n + 9, update_in)
        at_step(within(2 * n, 3 * n), gather_first, 0, win, M_IN, s - 2 * n)
        at_step(within(2 * n + 2, 3 * n + 2), gather_second, 0, win, M_IN, s - 2 * n - 2)
        at_step(within(2 * n + QUAD, 3 * n + QUAD), gather_third, 0, win, M_IN, s - 2 * n - QUAD)
        at_step(s == 2 * n + 3, stats_out_send)
        at_step(s == 2 * n + 6, stats_out_norm)
        at_step(s == 2 * n + 9, update_out)
        at_step(within(3 * n, QUAD * n), gather_first, 1, wpk, M_OUT, s - 3 * n)
        at_step(within(3 * n + 2, QUAD * n + 2), gather_second, 1, wpk, M_OUT, s - 3 * n - 2)
        at_step(within(3 * n + QUAD, QUAD * n + QUAD), gather_third, 1, wpk, M_OUT, s - 3 * n - QUAD)
        at_step(within(2 * n + 6, 3 * n + 6), gather_last, 0, win, M_IN, s - 2 * n - 6)
        at_step(within(3 * n + 6, QUAD * n + 6), gather_last, 1, wpk, M_OUT, s - 3 * n - 6)
        return 0

    lax.fori_loop(0, QUAD * n + 6, step, 0)


def final_kernel(win, wpk, mi, mo, ri, ci, ro, co, win_o, wout_o, mi_o, mo_o, ri_o, ci_o, ro_o, co_o, stage, sem, stage_sem):
    def block(i):
        at = (i // QUAD, (i // 2) % 2, pl.ds(ROWS_IN // 2 * (i % 2), ROWS_IN // 2))
        return pltpu.make_async_copy(win.at[at], win_o.at[at], sem.at[6])

    for i in range(SUB2):
        block(i).start()
    plain = []
    for i, (src, dst) in enumerate(((mi, mi_o), (mo, mo_o), (ri, ri_o), (ci, ci_o), (ro, ro_o), (co, co_o))):
        plain.append(pltpu.make_async_copy(src, dst, sem.at[i]))
    for copy in plain:
        copy.start()

    def rows_of(t):
        return pl.ds(aligned(RAW_STEP * t, SUB), RAW_STEP)

    def put(t):
        return pltpu.make_async_copy(stage.at[rows_of(t)], wout_o.at[rows_of(t)], stage_sem)

    def chunk(t, _):
        def unit(u, _):
            ln = lanes((SUB, LANE))
            rows = pl.ds(aligned(2 * M_OUT * t + SUB * u, SUB), SUB)
            for half in range(2):
                tails = [wpk[2 * half + jj // 2, jj % 2, rows, 512:640] for jj in range(QUAD)]
                for k in range(QUAD):
                    to = pl.ds(aligned(RAW_STEP * t + PART * u + SUB * k, SUB), SUB)
                    heads = []
                    for jj in range(QUAD):
                        head = wpk[2 * half + jj // 2, jj % 2, rows, LANE * k:LANE * k + LANE]
                        heads.append(head if jj == 0 else pltpu.roll(head, PART * jj, 1))
                    ends = [tails[jj] if jj == k else pltpu.roll(tails[jj], (PART * (jj - k)) % LANE, 1) for jj in range(QUAD)]
                    for tile in range(5):
                        if tile == 0:
                            out = heads[0]
                        else:
                            out = ends[tile - 1]
                            if tile > 1:
                                out = jnp.where(ln < PART * (tile - 1), heads[tile - 1], out)
                            if tile < QUAD:
                                out = jnp.where(ln >= PART * tile, heads[tile], out)
                        at = LANE * (5 * half + tile)
                        stage[to, at:at + LANE] = out
            return 0

        lax.fori_loop(0, RAW_STEP // PART, unit, 0)
        put(t).start()
        return 0

    lax.fori_loop(0, STEPS, chunk, 0)
    pltpu.make_async_copy(stage, wout_o, stage_sem).wait()
    pltpu.make_async_copy(win, win_o, sem.at[6]).wait()
    for copy in plain:
        copy.wait()


def solution(mesh):
    n_tp = mesh.shape['tp']
    n_dp = mesh.shape['dp']
    vmem = pl.BlockSpec(memory_space=pltpu.VMEM)
    hbm = pl.BlockSpec(memory_space=pltpu.HBM)
    smem = pl.BlockSpec(memory_space=pltpu.SMEM)
    dma = pltpu.SemaphoreType.DMA
    kept = (
        ((QUAD, 2, ROWS_IN, COLS_IN), F32),
        ((QUAD, 2, ROWS_OUT, COLS_OUT), F32),
        ((ROWS_IN, COLS_IN), BF16),
        ((WIDTH, RAW_OUT), BF16),
        ((1, ROWS_IN), F32),
        ((1, COLS_IN), F32),
        ((1, RAW_OUT), F32),
        ((1, WIDTH), F32),
    )
    main = pl.pallas_call(
        functools.partial(main_kernel, n_tp, n_dp, D, COLS_IN * n_tp, RAW_OUT * n_tp, D),
        out_shape=[pltpu.VMEM(shape, dtype) for shape, dtype in kept],
        in_specs=[hbm] * 6 + [hbm] * QUAD + [smem] * 3,
        out_specs=[vmem] * SUB,
        scratch_shapes=[
            pltpu.VMEM((3, 2, 2, 2 * M_IN, COLS_IN), F32),
            pltpu.VMEM((2, RAW_STEP, D), F32),
            pltpu.VMEM((2, 2, 2, 2, 2 * M_OUT, COLS_OUT), F32),
            pltpu.VMEM((ROWS_IN, COLS_IN), F32),
            pltpu.VMEM((ROWS_OUT, COLS_OUT), F32),
            pltpu.VMEM((RAW_OUT, 256), F32),
            pltpu.VMEM((RAW_OUT, LANE), F32),
            pltpu.VMEM((ROWS_IN, LANE), F32),
            pltpu.VMEM((1, COLS_IN), F32),
            pltpu.VMEM((SUB, LANE), F32),
            pltpu.VMEM((SUB, LANE), F32),
            pltpu.VMEM((SUB, COLS_IN), F32),
            pltpu.VMEM((ROWS_IN, LANE), F32),
            pltpu.VMEM((ROWS_IN, LANE), F32),
            pltpu.VMEM((SUB2, LANE), F32),
            pltpu.VMEM((SUB2, LANE), F32),
            pltpu.VMEM((2, 1, LEN_IN), F32),
            pltpu.VMEM((QUAD, 1, LEN_IN // 2), F32),
            pltpu.VMEM((1, LEN_IN), F32),
            pltpu.VMEM((2, 1, LEN_OUT), F32),
            pltpu.VMEM((QUAD, 1, LEN_OUT // 2), F32),
            pltpu.VMEM((1, LEN_OUT), F32),
            pltpu.VMEM((1, ROWS_IN), F32),
            pltpu.VMEM((1, COLS_IN), F32),
            pltpu.VMEM((1, RAW_OUT), F32),
            pltpu.VMEM((1, WIDTH), F32),
            pltpu.VMEM((2, 1, LANE), F32),
        ] + [pltpu.VMEM((i, 1, LANE), F32) for i in (2, 2, QUAD)] * 2 + [
            dma((N_RED, SLOTS)),
            dma((PAIR_SLOTS,)),
            dma((2 * QUAD,)),
            dma((2, N_EX)),
        ],
        compiler_params=pltpu.CompilerParams(collective_id=0, has_side_effects=True, vmem_limit_bytes=GRANT),
    )
    final = pl.pallas_call(
        final_kernel,
        out_shape=[
            jax.ShapeDtypeStruct((QUAD, 2, ROWS_IN, COLS_IN), F32),
            jax.ShapeDtypeStruct((RAW_OUT, D), F32),
        ] + [jax.ShapeDtypeStruct(shape, dtype) for shape, dtype in kept[2:]],
        in_specs=[vmem] * SUB,
        out_specs=[hbm] * SUB,
        scratch_shapes=[pltpu.VMEM((RAW_OUT, D), F32), dma((7,)), dma],
        compiler_params=pltpu.CompilerParams(vmem_limit_bytes=GRANT),
    )

    def body(w_in, w_out, g_in, g_out, m_in, m_out, r_in, c_in, r_out, c_out, learn_rate, weight_decay, beta_two):
        shards = (QUAD, 2, ROWS_IN, COLS_IN)
        got = main(
            w_in.reshape(shards), w_out[0], g_in.reshape((2, 2, 2, ROWS_IN, COLS_IN)), g_out[0, 0], m_in[0], m_out[0].T,
            r_in, c_in, r_out, c_out, learn_rate.reshape(1), weight_decay.reshape(1), beta_two.reshape(1))
        w_i, w_o, m_i, m_o, r_i, c_i, r_o, c_o = final(*[pltpu.with_memory_space_constraint(g, pltpu.VMEM) for g in got])
        return w_i.reshape((1, D, COLS_IN)), w_o[NO], m_i[NO], m_o.T[NO], r_i, c_i, r_o, c_o

    in_specs = (P(NO, NO, 'tp'), P(NO, 'tp', NO), P('dp', NO, NO, 'tp'), P('dp', NO, 'tp', NO), P(NO, 'dp', 'tp'), P(NO, 'tp', 'dp'), P(NO, 'dp'), P(NO, 'tp'), P(NO, 'tp'), P(NO, 'dp'), P(), P(), P())
    out_specs = (P(NO, NO, 'tp'), P(NO, 'tp', NO), P(NO, 'dp', 'tp'), P(NO, 'tp', 'dp'), P(NO, 'dp'), P(NO, 'tp'), P(NO, 'tp'), P(NO, 'dp'))
    return jax.shard_map(body, mesh=mesh, in_specs=in_specs, out_specs=out_specs, check_vma=False)
```
